128 devices in a mesh: sp: 4 (over x), fsdp: 32 (over z, y, core).
Axes of the slice: x: 4, y: 4, z: 4, core: 2. Of those that a mesh axis runs over, the one named last changes fastest.
Arguments:
- x: bfloat16 [32, 512, 4096], P('fsdp', 'sp')
- grad_y: bfloat16 [32, 512, 4096], P('fsdp', 'sp')
- w_q: bfloat16 [4096, 4096], P('fsdp')
- w_k: bfloat16 [4096, 4096], P('fsdp')
- w_v: bfloat16 [4096, 4096], P('fsdp')
- w_o: bfloat16 [4096, 4096], P('fsdp')
- q_norm_w: float32 [4096], P('fsdp')
- k_norm_w: float32 [4096], P('fsdp')
- post_norm_w: float32 [4096], P('fsdp')
Outputs:
- output 1: bfloat16 [32, 512, 4096], P('fsdp', 'sp')
- output 2: bfloat16 [32, 512, 4096], P('fsdp', 'sp')
- output 3: float32 [4096, 4096], P('fsdp')
- output 4: float32 [4096, 4096], P('fsdp')
- output 5: float32 [4096, 4096], P('fsdp')
- output 6: float32 [4096, 4096], P('fsdp')
- output 7: float32 [4096], P('fsdp')
- output 8: float32 [4096], P('fsdp')
- output 9: float32 [4096], P('fsdp')
All inputs are finite; a program needn't handle non-finite values.
Results may differ from the reference program's by a relative error of at most 0.02.
Values are sent between devices in bfloat16 or wider.
A program may use at most 1 GiB of HBM per device.

```python
import jax
import jax.numpy as jnp
from jax import lax

BATCH_SIZE = 32
SEQ_LEN = 512
D_MODEL = 4096
N_HEADS = 32
HEAD_DIM = 128
RMS_EPSILON = 1e-6
ROPE_THETA = 500000.0


def setup_inputs(seed: int = 0) -> dict:
    key_list = jax.random.split(jax.random.key(seed), 11)
    tok_shape = (BATCH_SIZE, SEQ_LEN, D_MODEL)
    fan_scale = D_MODEL ** -0.5
    q_scale = jnp.repeat(jnp.exp(jax.random.uniform(key_list[0], (N_HEADS,), jnp.float32, -0.7, 0.7)), HEAD_DIM)
    k_scale = jnp.repeat(jnp.exp(jax.random.uniform(key_list[1], (N_HEADS,), jnp.float32, -0.7, 0.7)), HEAD_DIM)
    x = jax.random.normal(key_list[2], tok_shape, jnp.float32)
    grad_y = jax.random.normal(key_list[3], tok_shape, jnp.float32)
    w_q = jax.random.normal(key_list[4], (D_MODEL, D_MODEL), jnp.float32) * (fan_scale * q_scale)[None, :]
    w_k = jax.random.normal(key_list[5], (D_MODEL, D_MODEL), jnp.float32) * (fan_scale * k_scale)[None, :]
    w_v = jax.random.normal(key_list[6], (D_MODEL, D_MODEL), jnp.float32) * fan_scale
    w_o = jax.random.normal(key_list[7], (D_MODEL, D_MODEL), jnp.float32) * fan_scale
    q_norm_w = jax.random.uniform(key_list[8], (D_MODEL,), jnp.float32, 0.6, 1.4)
    k_norm_w = jax.random.uniform(key_list[9], (D_MODEL,), jnp.float32, 0.6, 1.4)
    post_norm_w = jax.random.uniform(key_list[10], (D_MODEL,), jnp.float32, 0.6, 1.4)
    return {'x': x.astype(jnp.bfloat16), 'grad_y': grad_y.astype(jnp.bfloat16), 'w_q': w_q.astype(jnp.bfloat16), 'w_k': w_k.astype(jnp.bfloat16), 'w_v': w_v.astype(jnp.bfloat16), 'w_o': w_o.astype(jnp.bfloat16), 'q_norm_w': q_norm_w, 'k_norm_w': k_norm_w, 'post_norm_w': post_norm_w}


def snap_bf16(values):
    rounded = values.astype(jnp.bfloat16).astype(values.dtype)
    return values + lax.stop_gradient(rounded - values)


def rms_norm(values, gain_vec):
    inv_rms = lax.rsqrt(jnp.mean(values * values, axis=-1, keepdims=True) + RMS_EPSILON)
    return values * inv_rms * gain_vec


def rope_tables():
    half_dim = HEAD_DIM // 2
    inv_freq = ROPE_THETA ** (-jnp.arange(half_dim, dtype=jnp.float32) * (2.0 / HEAD_DIM))
    angles = jnp.arange(SEQ_LEN, dtype=jnp.float32)[:, None] * inv_freq[None, :]
    return jnp.cos(angles)[:, None, :], jnp.sin(angles)[:, None, :]


def rope_apply(heads_in, cos_tab, sin_tab):
    half_dim = HEAD_DIM // 2
    first_half = heads_in[..., :half_dim]
    second_half = heads_in[..., half_dim:]
    return jnp.concatenate([first_half * cos_tab - second_half * sin_tab, second_half * cos_tab + first_half * sin_tab], axis=-1)


def attend_sequence(triple):
    q_seq, k_seq, v_seq = triple
    scores = jnp.einsum('qhd,khd->hqk', q_seq, k_seq) * (HEAD_DIM ** -0.5)
    causal = jnp.arange(SEQ_LEN)[:, None] >= jnp.arange(SEQ_LEN)[None, :]
    scores = jnp.where(causal[None, :, :], scores, -1e30)
    attn_probs = snap_bf16(jax.nn.softmax(scores, axis=-1))
    return jnp.einsum('hqk,khd->qhd', attn_probs, v_seq)


def block_forward(x_float, w_q, w_k, w_v, w_o, q_norm_w, k_norm_w, post_norm_w):
    tokens = x_float.reshape(-1, D_MODEL)
    head_shape = (BATCH_SIZE, SEQ_LEN, N_HEADS, HEAD_DIM)
    cos_tab, sin_tab = rope_tables()
    q_lin = snap_bf16(jnp.dot(tokens, w_q, preferred_element_type=jnp.float32))
    k_lin = snap_bf16(jnp.dot(tokens, w_k, preferred_element_type=jnp.float32))
    v_lin = snap_bf16(jnp.dot(tokens, w_v, preferred_element_type=jnp.float32))
    q_rot = snap_bf16(rope_apply(rms_norm(q_lin, q_norm_w).reshape(head_shape), cos_tab, sin_tab))
    k_rot = snap_bf16(rope_apply(rms_norm(k_lin, k_norm_w).reshape(head_shape), cos_tab, sin_tab))
    v_heads = v_lin.reshape(head_shape)
    attn_out = lax.map(jax.checkpoint(attend_sequence), (q_rot, k_rot, v_heads))
    attn_tok = snap_bf16(attn_out).reshape(-1, D_MODEL)
    a_lin = snap_bf16(jnp.dot(attn_tok, w_o, preferred_element_type=jnp.float32))
    return x_float + rms_norm(a_lin, post_norm_w).reshape(x_float.shape)


def reference(x, grad_y, w_q, w_k, w_v, w_o, q_norm_w, k_norm_w, post_norm_w):
    y_value, pullback = jax.vjp(block_forward, x.astype(jnp.float32), w_q.astype(jnp.float32), w_k.astype(jnp.float32), w_v.astype(jnp.float32), w_o.astype(jnp.float32), q_norm_w, k_norm_w, post_norm_w)
    all_grads = pullback(grad_y.astype(jnp.float32))
    return (y_value.astype(jnp.bfloat16), all_grads[0].astype(jnp.bfloat16), all_grads[1], all_grads[2], all_grads[3], all_grads[4], all_grads[5], all_grads[6], all_grads[7])
```

```python
import jax
import jax.numpy as jnp
from jax import lax
from jax.experimental import pallas as pl
from jax.experimental.pallas import tpu as pltpu
from jax.sharding import Mesh, PartitionSpec as P

HEAD_DIM = 128
RMS_EPSILON = 1e-6
ROPE_THETA = 500000.0
FS = ('z', 'y', 'c')
F32 = jnp.float32
BF16 = jnp.bfloat16
MESH_ID = pl.DeviceIdType.MESH
HBM = pl.ANY
SEG = 256
NM = 4


def grads_kernel(*refs):
    parts = refs[:NM]
    gx_part, gy = refs[NM:NM + 2]
    outs = refs[NM + 2:2 * NM + 2]
    gx_out = refs[2 * NM + 2]
    (r1, r2, loc, rg, gloc, s1s, s1r, s2s, s2r, ags, agr, d2s, d2r, fws, fwr, lws, lsem, gs, gr, gsem) = refs[2 * NM + 3:]
    x, z, y, c = (lax.axis_index(n) for n in ('sp', 'z', 'y', 'c'))

    def mod4(v):
        return lax.rem(v + 8, 4)

    p1 = (1 - c) * y + c * z
    p2 = (1 - c) * z + c * y
    dirs = (1, -1)

    def axis1(d):
        return (x, mod4(z + d * c), mod4(y + d * (1 - c)), c)

    def axis2(d):
        return (x, mod4(z + d * (1 - c)), mod4(y + d * c), c)

    def xdev(d, core):
        return (mod4(x + d), z, y, core)

    partner = (x, z, y, 1 - c)
    peers = [axis1(1), axis1(-1), axis2(1), axis2(-1), xdev(1, c), xdev(-1, c), xdev(1, 1 - c), xdev(-1, 1 - c), partner]
    barrier = pltpu.get_barrier_semaphore()
    for peer in peers:
        pl.semaphore_signal(barrier, inc=1, device_id=peer, device_id_type=MESH_ID)
    pl.semaphore_wait(barrier, len(peers))

    def seg_rows(b, j):
        zz = (1 - c) * j + c * b
        yy = (1 - c) * b + c * j
        return pl.ds(pl.multiple_of(zz * 1024 + yy * SEG, SEG), SEG)

    def remote(src, dst, ss, rs, dev):
        return pltpu.make_async_remote_copy(src_ref=src, dst_ref=dst, send_sem=ss, recv_sem=rs, device_id=dev, device_id_type=MESH_ID)

    def send1(m, t, kk, jj):
        d = dirs[kk]
        if t == 0:
            rows = seg_rows(mod4(p1 - d), mod4(p2 - d * (1 + jj)))
            src = parts[m].at[rows, pl.ds(kk * SEG, SEG)]
        else:
            src = r1.at[m, kk, t - 1, jj]
        return remote(src, r1.at[m, kk, t, jj], s1s.at[m, kk, t, jj], s1r.at[m, kk, t, jj], axis1(d))

    def load(m, t, kk, jj):
        d = dirs[kk]
        par = (3 * m + t) % 2
        rows = seg_rows(mod4(p1 - d * (2 + t)), mod4(p2 - d * (1 + jj)))
        return pltpu.make_async_copy(parts[m].at[rows, pl.ds(kk * SEG, SEG)], loc.at[par, kk, jj], lsem.at[par, kk, jj])

    def send2(m, u, kk):
        return remote(r1.at[m, kk, 2, u], r2.at[m, kk, u], s2s.at[m, kk, u], s2r.at[m, kk, u], axis2(dirs[kk]))

    def out_cols(k, xs):
        return pl.ds(pl.multiple_of(k * 1024 + xs * SEG, SEG), SEG)

    def ag_send(m, kk, di, h):
        k = 2 * c + kk
        return remote(r1.at[m, kk, 2, 3, pl.ds(h * 128, 128)], outs[m].at[:, out_cols(k, x)], ags.at[m, kk, di, h], agr.at[m, di, k], xdev(dirs[di], h))

    def ag_recv(m, di, k):
        cols = out_cols(k, mod4(x - dirs[di]))
        return remote(outs[m].at[:, cols], outs[m].at[:, cols], ags.at[m, 0, di, 0], agr.at[m, di, k], xdev(dirs[di], c))

    def pair_send(m, kk):
        k = 2 * c + kk
        rows = pl.ds(pl.multiple_of((1 - c) * 128, 128), 128)
        return remote(r1.at[m, kk, 2, 3, rows], outs[m].at[:, out_cols(k, x)], d2s.at[m, kk], d2r.at[m, kk], partner)

    def own_store(m, kk):
        k = 2 * c + kk
        rows = pl.ds(pl.multiple_of(c * 128, 128), 128)
        return pltpu.make_async_copy(r1.at[m, kk, 2, 3, rows], outs[m].at[:, out_cols(k, x)], lws.at[m, kk])

    def forward(m, k):
        di = k % 2
        cols = out_cols(k, mod4(x - dirs[di]))
        return remote(outs[m].at[:, cols], outs[m].at[:, cols], fws.at[m, k], fwr.at[m, k], xdev(dirs[di], c))

    def gcols(kk, jj):
        return pl.ds(pl.multiple_of(kk * 2048 + jj * 512, 512), 512)

    def gsend(t, kk, jj):
        d = dirs[kk]
        if t == 0:
            src = gx_part.at[pl.ds(pl.multiple_of(mod4(x - d) * 128, 128), 128), gcols(kk, jj)]
        else:
            src = rg.at[kk, t - 1, jj]
        return remote(src, rg.at[kk, t, jj], gs.at[kk, t, jj], gr.at[kk, t, jj], xdev(d, c))

    def gload(t, kk, jj):
        rows = pl.ds(pl.multiple_of(mod4(x - dirs[kk] * (2 + t)) * 128, 128), 128)
        return pltpu.make_async_copy(gx_part.at[rows, gcols(kk, jj)], gloc.at[t % 2, kk, jj], gsem.at[t % 2, kk, jj])

    def each(fn):
        def step(jj, carry):
            for kk in range(2):
                fn(kk, jj)
            return carry
        lax.fori_loop(0, 4, step, 0)

    each(lambda kk, jj: send1(0, 0, kk, jj).start())
    each(lambda kk, jj: load(0, 0, kk, jj).start())
    each(lambda kk, jj: gsend(0, kk, jj).start())
    each(lambda kk, jj: gload(0, kk, jj).start())

    def phase2(m, u):
        for kk in range(2):
            send2(m, u - 1, kk).wait_recv()
            r1[m, kk, 2, u] = r1[m, kk, 2, u] + r2[m, kk, u - 1]
            if u < 3:
                send2(m, u, kk).start()
            else:
                own_store(m, kk).start()
                for di in range(2):
                    for h in range(2):
                        ag_send(m, kk, di, h).start()
                pair_send(m, kk).start()

    def do_forward(m):
        for k in range(4):
            ag_recv(m, k % 2, k).wait_recv()
            forward(m, k).start()

    def gx_step(t):
        if t < 2:
            each(lambda kk, jj: gload(t + 1, kk, jj).start())

        def item(kk, jj):
            gsend(t, kk, jj).wait_recv()
            gload(t, kk, jj).wait()
            total = rg[kk, t, jj] + gloc[t % 2, kk, jj]
            if t < 2:
                rg[kk, t, jj] = total
                gsend(t + 1, kk, jj).start()
            else:
                gx_out[:, gcols(kk, jj)] = (total + gy[:, gcols(kk, jj)].astype(F32)).astype(BF16)
        each(item)

    last = 3 * NM
    for r in range(last):
        m, t = divmod(r, 3)
        if r + 1 < last:
            mn, tn = divmod(r + 1, 3)
            each(lambda kk, jj: load(mn, tn, kk, jj).start())

        def item(kk, jj):
            send1(m, t, kk, jj).wait_recv()
            load(m, t, kk, jj).wait()
            r1[m, kk, t, jj] = r1[m, kk, t, jj] + loc[r % 2, kk, jj]
            if t < 2:
                send1(m, t + 1, kk, jj).start()
            elif m + 1 < NM:
                send1(m + 1, 0, kk, jj).start()

        each(item)
        if t == 2:
            for kk in range(2):
                send2(m, 0, kk).start()
        if m > 0 and t == 0:
            phase2(m - 1, 1)
        if m > 0 and t == 1:
            phase2(m - 1, 2)
        if m > 0 and t == 2:
            phase2(m - 1, 3)
        if m > 1 and t == 0:
            do_forward(m - 2)
        if r in (2, 4, 6):
            gx_step((r - 2) // 2)
    for u in (1, 2, 3):
        phase2(NM - 1, u)
    if NM > 1:
        do_forward(NM - 2)
    do_forward(NM - 1)

    for m in range(NM):
        for t in range(3):
            each(lambda kk, jj: send1(m, t, kk, jj).wait_send())
        for kk in range(2):
            for u in range(3):
                send2(m, u, kk).wait_send()
            for di in range(2):
                for h in range(2):
                    ag_send(m, kk, di, h).wait_send()
            pair_send(m, kk).wait()
            own_store(m, kk).wait()
        for k in range(4):
            ag_recv(m, 1 - k % 2, k).wait_recv()
            forward(m, k).wait()
    for t in range(3):
        each(lambda kk, jj: gsend(t, kk, jj).wait_send())


def reduce_grads(parts, gx_part, gy):
    nm = len(parts)
    dma = pltpu.SemaphoreType.DMA
    vmem = pl.BlockSpec(memory_space=pltpu.VMEM)
    hbm = pl.BlockSpec(memory_space=HBM)
    return pl.pallas_call(
        grads_kernel,
        out_shape=[jax.ShapeDtypeStruct((128, 4096), F32)] * nm + [jax.ShapeDtypeStruct((128, 4096), BF16)],
        in_specs=[hbm] * (nm + 1) + [vmem],
        out_specs=[hbm] * nm + [vmem],
        scratch_shapes=[
            pltpu.VMEM((nm, 2, 3, 4, SEG, SEG), F32),
            pltpu.VMEM((nm, 2, 3, SEG, SEG), F32),
            pltpu.VMEM((2, 2, 4, SEG, SEG), F32),
            pltpu.VMEM((2, 3, 4, 128, 512), F32),
            pltpu.VMEM((2, 2, 4, 128, 512), F32),
            dma((nm, 2, 3, 4)), dma((nm, 2, 3, 4)),
            dma((nm, 2, 3)), dma((nm, 2, 3)),
            dma((nm, 2, 2, 2)), dma((nm, 2, 4)),
            dma((nm, 2)), dma((nm, 2)),
            dma((nm, 4)), dma((nm, 4)),
            dma((nm, 2)), dma((2, 2, 4)),
            dma((2, 3, 4)), dma((2, 3, 4)), dma((2, 2, 4)),
        ],
        compiler_params=pltpu.CompilerParams(collective_id=4, has_side_effects=True, vmem_limit_bytes=60 * 1024 * 1024),
        cost_estimate=pl.CostEstimate(flops=10 ** 11, bytes_accessed=10 ** 8, transcendentals=0),
        name='reduce_grads',
    )(*parts, gx_part, gy)


def gather_kernel(*refs):
    nw = 3
    w_in = refs[:nw]
    x_in, gy_in = refs[nw:nw + 2]
    w_out = refs[nw + 2:2 * nw + 2]
    qkv = refs[2 * nw + 2:3 * nw + 2]
    x_full, gy_cols, stats = refs[3 * nw + 2:3 * nw + 5]
    (w, sq, st, ld, d0s, d0r, a1s, a1r, a2s, a2r, f3s, f3r, xls, xs, xr, xfs, xfr, gls, gs, gr, sts, strv, wos) = refs[3 * nw + 5:]
    x, z, y, c = (lax.axis_index(n) for n in ('sp', 'z', 'y', 'c'))

    def mod4(v):
        return lax.rem(v + 8, 4)

    p1 = (1 - c) * y + c * z
    p2 = (1 - c) * z + c * y
    dirs = (1, -1)

    def axis1(d):
        return (x, mod4(z + d * c), mod4(y + d * (1 - c)), c)

    def axis2(d):
        return (x, mod4(z + d * (1 - c)), mod4(y + d * c), c)

    def xdev(d):
        return (mod4(x + d), z, y, c)

    partner = (x, z, y, 1 - c)
    peers = [axis1(1), axis1(-1), axis2(1), axis2(-1), xdev(1), xdev(-1), xdev(2), partner]
    barrier = pltpu.get_barrier_semaphore()
    for peer in peers:
        pl.semaphore_signal(barrier, inc=1, device_id=peer, device_id_type=MESH_ID)

    def seg_rows(b, j):
        zz = (1 - c) * j + c * b
        yy = (1 - c) * b + c * j
        return pl.ds(pl.multiple_of(zz * 1024 + yy * SEG, SEG), SEG)

    def remote(src, dst, ss, rs, dev):
        return pltpu.make_async_remote_copy(src_ref=src, dst_ref=dst, send_sem=ss, recv_sem=rs, device_id=dev, device_id_type=MESH_ID)

    def each(fn, n=4):
        def step(jj, carry):
            for kk in range(2):
                fn(kk, jj)
            return carry
        lax.fori_loop(0, n, step, 0)

    my_rows = pl.ds(pl.multiple_of(z * 1024 + y * SEG + c * 128, 128), 128)

    def load(m, k):
        src = w_in[m].at[:, pl.ds(pl.multiple_of(k * 1024 + x * SEG, SEG), SEG)]
        return pltpu.make_async_copy(src, w.at[m, my_rows, pl.ds(k * SEG, SEG)], ld.at[m, k])

    def pair_send(m):
        return remote(w.at[m, my_rows], w.at[m, my_rows], d0s.at[m], d0r.at[m], partner)

    def color(kk):
        return pl.ds(pl.multiple_of((2 * c + kk) * SEG, SEG), SEG)

    def same(m, kk, rows, ss, rs, dev):
        ref = w.at[m, rows, color(kk)]
        return remote(ref, ref, ss, rs, dev)

    def send1(m, u, kk):
        d = dirs[kk]
        return same(m, kk, seg_rows(p1, mod4(p2 - d * u)), a1s.at[m, kk, u], a1r.at[m, kk, u], axis2(d))

    def fwd1(m, u, kk):
        rows = seg_rows(p1, mod4(p2 - dirs[kk] * (u + 1)))
        return same(m, kk, rows, f3s.at[m, kk, u], f3r.at[m, kk, u], partner)

    def send2(m, t, kk, jj):
        d = dirs[kk]
        rows = seg_rows(mod4(p1 - d * t), mod4(p2 - d * jj))
        return same(m, kk, rows, a2s.at[m, kk, t, jj], a2r.at[m, kk, t, jj], axis1(d))

    def fwd2(m, t, kk, jj):
        d = dirs[kk]
        rows = seg_rows(mod4(p1 - d * (t + 1)), mod4(p2 - d * jj))
        idx = 3 + t * 4 + jj
        return same(m, kk, rows, f3s.at[m, kk, idx], f3r.at[m, kk, idx], partner)

    def xseg(ref, b, g):
        rows = pl.ds(pl.multiple_of(b * 128, 128), 128)
        return ref.at[rows, pl.ds(g * 1024, 1024)]

    x_own = pltpu.make_async_copy(x_in, x_full.at[pl.ds(pl.multiple_of(x * 128, 128), 128)], xls)

    def xsend(di, g):
        ref = xseg(x_full, x, g)
        return remote(ref, ref, xs.at[di, g], xr.at[di, g], xdev(dirs[di]))

    def xfwd(g):
        d = dirs[g // 2]
        ref = xseg(x_full, mod4(x - d), g)
        return remote(ref, ref, xfs.at[g], xfr.at[g], xdev(d))

    gy_rows = pl.ds(pl.multiple_of(x * 128, 128), 128)
    gy_own = pltpu.make_async_copy(gy_in.at[x], gy_cols.at[gy_rows], gls)

    def gy_send(i):
        d = (1, -1, 2)[i]
        return remote(gy_in.at[mod4(x + d)], gy_cols.at[gy_rows], gs.at[i], gr.at[i], xdev(d))

    def st_send(i):
        d = (1, -1, 2)[i]
        return remote(st.at[0], st.at[1 + i], sts.at[i], strv.at[i], xdev(d))

    def w_store(m):
        return pltpu.make_async_copy(w.at[m], w_out[m], wos.at[m])

    st[0] = jnp.zeros((8, 512), F32)
    x_own.start()
    for m in range(nw):
        for k in range(4):
            load(m, k).start()
    gy_own.start()
    pl.semaphore_wait(barrier, len(peers))
    x_own.wait()
    for m in range(nw):
        for k in range(4):
            load(m, k).wait()
        pair_send(m).start()
        if m == 0:
            for g in range(4):
                for di in range(2):
                    xsend(di, (g + 2 * di) % 4).start()

    def stage1_first(m):
        pair_send(m).wait_recv()
        for kk in range(2):
            send1(m, 0, kk).start()
            send2(m, 0, kk, 0).start()

    def stage1_next(m, u):
        for kk in range(2):
            send1(m, u, kk).wait_recv()
            if u < 2:
                send1(m, u + 1, kk).start()
            send2(m, 0, kk, u + 1).start()
            fwd1(m, u, kk).start()

    def pair_done(m):
        def step(i, carry):
            for kk in range(2):
                ref = w.at[m, pl.ds(0, SEG), pl.ds(0, SEG)]
                remote(ref, ref, f3s.at[m, kk, i], f3r.at[m, kk, i], partner).wait_recv()
            return carry
        lax.fori_loop(0, 15, step, 0)

    def chunks(m, theirs):
        def step(i, carry):
            base = (1 - c) if theirs else c
            k = 2 * base + i
            cols = pl.ds(pl.multiple_of(k * SEG, SEG), SEG)
            acc = jnp.dot(x_full[...], w[m, :, cols], preferred_element_type=F32).astype(BF16)
            qkv[m][:, cols] = acc
            if m < 2:
                sqv = acc.astype(F32)
                sqv = sqv * sqv
                sqv = sqv[:, :128] + sqv[:, 128:]
                if theirs:
                    sq[m] = sq[m] + sqv
                else:
                    @pl.when(i == 0)
                    def _():
                        sq[m] = sqv

                    @pl.when(i == 1)
                    def _():
                        sq[m] = sq[m] + sqv
            return carry
        lax.fori_loop(0, 2, step, 0)

    def x_wait():
        for g in range(4):
            xsend(1 - g // 2, g).wait_recv()
            xfwd(g).wait_recv()

    stage1_first(0)
    for u in range(3):
        stage1_next(0, u)
    for m in range(nw):
        for t in range(3):
            def item(kk, jj):
                send2(m, t, kk, jj).wait_recv()
                if t < 2:
                    send2(m, t + 1, kk, jj).start()
                fwd2(m, t, kk, jj).start()
            each(item)
            if m + 1 < nw:
                if t == 0:
                    stage1_first(m + 1)
                    stage1_next(m + 1, 0)
                elif t == 1:
                    stage1_next(m + 1, 1)
                else:
                    stage1_next(m + 1, 2)
            if (m, t) == (0, 1):
                for g in range(4):
                    xsend(g // 2, g).wait_recv()
                    xfwd(g).start()
                for i in range(3):
                    gy_send(i).start()
            if (m, t) == (1, 1):
                x_wait()
                chunks(0, False)
            if (m, t) == (1, 2):
                pair_done(0)
                w_store(0).start()
                chunks(0, True)
            if (m, t) == (2, 0):
                chunks(1, False)
            if (m, t) == (2, 1):
                pair_done(1)
                w_store(1).start()
                chunks(1, True)
                for i in range(2):
                    st[0, i:i + 1] = jnp.sum(sq[i].T, axis=0, keepdims=True)
                for i in range(3):
                    st_send(i).start()
    chunks(2, False)
    pair_done(2)
    w_store(2).start()
    chunks(2, True)
    for i in range(3):
        st_send(i).wait()
    stats[...] = (st[0] + st[1]) + (st[2] + st[3])

    gy_own.wait()
    for i in range(3):
        gy_send(i).wait()
    for g in range(4):
        xsend(0, g).wait_send()
        xsend(1, g).wait_send()
        xfwd(g).wait_send()
    for m in range(nw):
        pair_send(m).wait_send()
        for kk in range(2):
            for u in range(3):
                send1(m, u, kk).wait_send()
                fwd1(m, u, kk).wait_send()
        for t in range(3):
            each(lambda kk, jj: send2(m, t, kk, jj).wait_send())
            each(lambda kk, jj: fwd2(m, t, kk, jj).wait_send())
        w_store(m).wait()


def gather_project(weights, x_tok, gy_split):
    nw = len(weights)
    dma = pltpu.SemaphoreType.DMA
    vmem = pl.BlockSpec(memory_space=pltpu.VMEM)
    hbm = pl.BlockSpec(memory_space=HBM)
    sds = jax.ShapeDtypeStruct
    return pl.pallas_call(
        gather_kernel,
        out_shape=[sds((4096, 1024), BF16)] * nw + [sds((512, 1024), BF16)] * nw
        + [sds((512, 4096), BF16), sds((512, 1024), BF16), sds((8, 512), F32)],
        in_specs=[hbm] * (nw + 2),
        out_specs=[hbm] * nw + [vmem] * (nw + 3),
        scratch_shapes=[
            pltpu.VMEM((nw, 4096, 1024), BF16),
            pltpu.VMEM((2, 512, 128), F32),
            pltpu.VMEM((4, 8, 512), F32),
            dma((nw, 4)), dma((nw,)), dma((nw,)),
            dma((nw, 2, 3)), dma((nw, 2, 3)),
            dma((nw, 2, 3, 4)), dma((nw, 2, 3, 4)),
            dma((nw, 2, 15)), dma((nw, 2, 15)),
            dma(()), dma((2, 4)), dma((2, 4)), dma((4,)), dma((4,)),
            dma(()), dma((3,)), dma((3,)), dma((3,)), dma((3,)), dma((nw,)),
        ],
        compiler_params=pltpu.CompilerParams(collective_id=5, has_side_effects=True, vmem_limit_bytes=60 * 1024 * 1024),
        cost_estimate=pl.CostEstimate(flops=10 ** 11, bytes_accessed=10 ** 8, transcendentals=0),
        name='gather_project',
    )(*weights, x_tok, gy_split)


def rope_angles(positions):
    half_dim = HEAD_DIM // 2
    inv_freq = ROPE_THETA ** (-jnp.arange(half_dim, dtype=jnp.float32) * (2.0 / HEAD_DIM))
    angles = positions.astype(jnp.float32)[:, None] * inv_freq[None, :]
    return jnp.cos(angles)[:, None, :], jnp.sin(angles)[:, None, :]


def rope_apply(heads_in, cos_tab, sin_tab):
    half_dim = HEAD_DIM // 2
    first_half = heads_in[..., :half_dim]
    second_half = heads_in[..., half_dim:]
    return jnp.concatenate([first_half * cos_tab - second_half * sin_tab, second_half * cos_tab + first_half * sin_tab], axis=-1)


def causal_attention(q_rot, k_rot, v_heads):
    seq_len = q_rot.shape[0]
    scores = jnp.einsum('qhd,khd->hqk', q_rot, k_rot, preferred_element_type=F32) * (HEAD_DIM ** -0.5)
    causal = jnp.arange(seq_len)[:, None] >= jnp.arange(seq_len)[None, :]
    attn_probs = jax.nn.softmax(jnp.where(causal, scores, -1e30), axis=-1).astype(BF16)
    return jnp.einsum('hqk,khd->qhd', attn_probs, v_heads, preferred_element_type=F32).astype(BF16)


def solution(mesh):
    sp_size = mesh.shape['sp']
    mesh4 = Mesh(mesh.devices.reshape(4, 4, 4, 2), ('sp', 'z', 'y', 'c'))
    tok_spec = P(FS, 'sp', None)
    row_spec = P(FS, None)
    vec_spec = P(FS)

    def local_step(x, grad_y, wq_rows, wk_rows, wv_rows, wo_rows, gq_rows, gk_rows, gpost_rows):
        _, tok_len, width = x.shape
        rows = wq_rows.shape[0]
        seq_len = tok_len * sp_size
        lw = width // sp_size
        heads = lw // HEAD_DIM
        s = lax.axis_index('sp')

        def my_cols(w):
            return lax.dynamic_index_in_dim(w.reshape(w.shape[0], 4, 4, lw // 4), s, 2, False).reshape(w.shape[0], lw)

        def gather_cols(w):
            return lax.all_gather(my_cols(w), FS, axis=0, tiled=True)

        def gather_sp(v):
            n = v.shape[0]
            return lax.all_gather(v.reshape(n, 4, 1, lw // 4), 'sp', axis=2, tiled=True).reshape(n, width)

        def to_cols(v):
            n = v.shape[0]
            return lax.all_to_all(v.reshape(n, 4, 4, lw // 4), 'sp', 2, 0, tiled=True).reshape(n * 4, lw)

        def to_tokens(v):
            n = v.shape[0]
            return lax.all_to_all(v.reshape(n, 4, 1, lw // 4), 'sp', 0, 2, tiled=True).reshape(n // 4, width)

        x_tok, gy_tok = x[0], grad_y[0]
        gy_split = gy_tok.reshape(tok_len, 4, 4, lw // 4).transpose(2, 0, 1, 3).reshape(4, tok_len, lw)
        w_q, w_k, w_v, q_lin, k_lin, v_lin, x_full, gy_cols, qk_ss = gather_project([wq_rows, wk_rows, wv_rows], x_tok, gy_split)
        w_o = gather_cols(wo_rows)
        wo_x = lax.all_to_all(wo_rows.reshape(rows, 4, lw), 'y', 1, 0, tiled=False)
        wo_mine = lax.dynamic_index_in_dim(wo_x, s, 0, False)
        wo_gath = lax.all_gather(wo_mine, FS, axis=0, tiled=False)
        wo_head = wo_gath.reshape(4, 4, 2, rows, lw).transpose(0, 2, 3, 1, 4).reshape(lw, width)

        gains = jnp.concatenate([jnp.stack([gq_rows, gk_rows, gpost_rows]), jnp.zeros((61, HEAD_DIM), F32)], axis=0)
        gains = lax.all_gather(gains, FS, axis=0, tiled=False)[:, :3]
        gains = my_cols(gains.transpose(1, 0, 2).reshape(3, width))
        gain_q, gain_k, gain_post = gains[0], gains[1], gains[2]

        q_lin, k_lin = q_lin.astype(F32), k_lin.astype(F32)
        qk_inv = lax.rsqrt(qk_ss / width + RMS_EPSILON)
        q_inv, k_inv = qk_inv[0][:, None], qk_inv[1][:, None]
        q_hat = q_lin * q_inv
        k_hat = k_lin * k_inv
        cos_tab, sin_tab = rope_angles(jnp.arange(seq_len))
        hs = (seq_len, heads, HEAD_DIM)
        q_rot = rope_apply((q_hat * gain_q).reshape(hs), cos_tab, sin_tab).astype(BF16)
        k_rot = rope_apply((k_hat * gain_k).reshape(hs), cos_tab, sin_tab).astype(BF16)
        attn, attn_pull = jax.vjp(causal_attention, q_rot, k_rot, v_lin.reshape(hs))
        o_full = gather_sp(attn.reshape(seq_len, lw))
        a_lin = jnp.dot(o_full, w_o, preferred_element_type=F32).astype(BF16).astype(F32)
        gy_cols = gy_cols.astype(F32)
        grad_hat = gy_cols * gain_post
        a_st = lax.psum(jnp.stack([jnp.sum(a_lin * a_lin, axis=1), jnp.sum(grad_hat * a_lin, axis=1)]), 'sp')
        a_inv = lax.rsqrt(a_st[0] / width + RMS_EPSILON)[:, None]
        a_mean = a_st[1][:, None] * a_inv / width
        a_hat = a_lin * a_inv
        y_cols = (my_cols(x_full).astype(F32) + a_hat * gain_post).astype(BF16)
        y = to_tokens(y_cols)
        grad_a = (a_inv * (grad_hat - a_hat * a_mean)).astype(BF16)
        post_part = jnp.sum(gy_cols * a_hat, axis=0)
        ga_full = gather_sp(grad_a)
        grad_o = lax.dot_general(ga_full, wo_head, (((1,), (1,)), ((), ())), preferred_element_type=F32).astype(BF16)

        cidx = lax.axis_index('c')

        def swap(v):
            return lax.ppermute(v, 'c', [(0, 1), (1, 0)])

        def halves(v):
            h = v.reshape(seq_len, 2, lw // 2)
            mine = lax.dynamic_index_in_dim(h, cidx, 1, False)
            theirs = swap(lax.dynamic_index_in_dim(h, 1 - cidx, 1, False))
            return jnp.concatenate([mine, theirs], axis=0)

        x_two = jnp.concatenate([x_full, swap(x_full)], axis=0)
        o_two = jnp.concatenate([o_full, swap(o_full)], axis=0)

        def weight_part(left, right):
            return lax.dot_general(left, halves(right), (((0,), (0,)), ((), ())), preferred_element_type=F32)

        po = weight_part(o_two, grad_a)
        grad_q_rot, grad_k_rot, grad_v = attn_pull(grad_o.reshape(hs))
        grad_v = grad_v.reshape(seq_len, lw)
        pv = weight_part(x_two, grad_v)
        grad_qn = rope_apply(grad_q_rot.astype(F32), cos_tab, -sin_tab).reshape(seq_len, lw)
        grad_kn = rope_apply(grad_k_rot.astype(F32), cos_tab, -sin_tab).reshape(seq_len, lw)
        gain_q_part = jnp.sum(grad_qn * q_hat, axis=0)
        gain_k_part = jnp.sum(grad_kn * k_hat, axis=0)
        grad_qh = grad_qn * gain_q
        grad_kh = grad_kn * gain_k
        pr = lax.psum(jnp.stack([jnp.sum(grad_qh * q_hat, axis=1), jnp.sum(grad_kh * k_hat, axis=1)]), 'sp') / width
        grad_q = (q_inv * (grad_qh - q_hat * pr[0][:, None])).astype(BF16)
        grad_k = (k_inv * (grad_kh - k_hat * pr[1][:, None])).astype(BF16)
        pk = weight_part(x_two, grad_k)
        pq = weight_part(x_two, grad_q)

        def back(g, w):
            return lax.dot_general(g, w, (((1,), (1,)), ((), ())), preferred_element_type=F32)

        gx_part = back(grad_q, w_q) + back(grad_k, w_k) + back(grad_v, w_v)
        dwo, dwv, dwk, dwq, grad_x = reduce_grads([po, pv, pk, pq], gx_part, gy_tok)

        parts = jnp.stack([gain_q_part, gain_k_part, post_part])
        every = lax.all_gather(parts, ('sp',) + FS, axis=0, tiled=False).reshape(4, 32, 3, 4, 2, HEAD_DIM)
        zi, yi = lax.axis_index('z'), lax.axis_index('y')
        every = lax.dynamic_slice(every, (yi, 0, 0, zi, cidx, 0), (1, 32, 3, 1, 1, HEAD_DIM))
        gn = jnp.sum(every, axis=(0, 1, 3, 4))
        return y[None], grad_x[None], dwq, dwk, dwv, dwo, gn[0], gn[1], gn[2]

    return jax.shard_map(local_step, mesh=mesh4,
                         in_specs=(tok_spec, tok_spec, row_spec, row_spec, row_spec, row_spec, vec_spec, vec_spec, vec_spec),
                         out_specs=(tok_spec, tok_spec, row_spec, row_spec, row_spec, row_spec, vec_spec, vec_spec, vec_spec),
                         check_vma=False)
```

```python
import jax
import jax.numpy as jnp
from jax import lax
from jax.experimental import pallas as pl
from jax.experimental.pallas import tpu as pltpu
from jax.sharding import Mesh, PartitionSpec as P

HEAD_DIM = 128
RMS_EPSILON = 1e-6
ROPE_THETA = 500000.0
FS = ('z', 'y', 'c')
F32 = jnp.float32
BF16 = jnp.bfloat16
MESH_ID = pl.DeviceIdType.MESH
HBM = pl.ANY
SEG = 256
NM = 4


def rope_tables(seq_len):
    half_dim = HEAD_DIM // 2
    inv_freq = ROPE_THETA ** (-jnp.arange(half_dim, dtype=F32) * (2.0 / HEAD_DIM))
    angles = jnp.arange(seq_len).astype(F32)[:, None] * inv_freq[None, :]
    cos_half, sin_half = jnp.cos(angles), jnp.sin(angles)
    return jnp.concatenate([cos_half, cos_half], axis=1), jnp.concatenate([-sin_half, sin_half], axis=1)


def coords():
    return tuple(lax.axis_index(n) for n in ('sp', 'z', 'y', 'c'))


def mod4(v):
    return lax.rem(v + 8, 4)


def remote(src, dst, ss, rs, dev):
    return pltpu.make_async_remote_copy(src_ref=src, dst_ref=dst, send_sem=ss, recv_sem=rs, device_id=dev, device_id_type=MESH_ID)


def at256(v):
    return pl.ds(pl.multiple_of(v, SEG), SEG)


def at128(v):
    return pl.ds(pl.multiple_of(v, 128), 128)


def each(fn, n=4):
    def step(jj, carry):
        for kk in range(2):
            fn(kk, jj)
        return carry
    lax.fori_loop(0, n, step, 0)


def greet(peers):
    barrier = pltpu.get_barrier_semaphore()
    for peer in peers:
        pl.semaphore_signal(barrier, inc=1, device_id=peer, device_id_type=MESH_ID)
    return lambda: pl.semaphore_wait(barrier, len(peers))


class Torus:
    def __init__(self):
        self.x, self.z, self.y, self.c = x, z, y, c = coords()
        self.p1 = (1 - c) * y + c * z
        self.p2 = (1 - c) * z + c * y
        self.partner = (x, z, y, 1 - c)

    def axis1(self, d):
        return (self.x, mod4(self.z + d * self.c), mod4(self.y + d * (1 - self.c)), self.c)

    def axis2(self, d):
        return (self.x, mod4(self.z + d * (1 - self.c)), mod4(self.y + d * self.c), self.c)

    def xdev(self, d, core=None):
        return (mod4(self.x + d), self.z, self.y, self.c if core is None else core)

    def seg_rows(self, b, j):
        zz = (1 - self.c) * j + self.c * b
        yy = (1 - self.c) * b + self.c * j
        return at256(zz * 1024 + yy * SEG)


DIRS = (1, -1)
RING_SEMS = 8


def ring_sems(nw):
    dma = pltpu.SemaphoreType.DMA
    return [dma((nw,)), dma((nw,)), dma((nw, 2, 3)), dma((nw, 2, 3)), dma((nw, 2, 3, 4)), dma((nw, 2, 3, 4)), dma((nw, 2, 15)), dma((nw, 2, 15))]


class WeightRings:
    def __init__(self, g, w, sems):
        self.g, self.w = g, w
        self.d0s, self.d0r, self.a1s, self.a1r, self.a2s, self.a2r, self.f3s, self.f3r = sems
        self.my_rows = at128(g.z * 1024 + g.y * SEG + g.c * 128)

    def pair_send(self, m):
        ref = self.w.at[m, self.my_rows]
        return remote(ref, ref, self.d0s.at[m], self.d0r.at[m], self.g.partner)

    def same(self, m, kk, rows, ss, rs, dev):
        ref = self.w.at[m, rows, at256((2 * self.g.c + kk) * SEG)]
        return remote(ref, ref, ss, rs, dev)

    def send1(self, m, u, kk):
        g, d = self.g, DIRS[kk]
        return self.same(m, kk, g.seg_rows(g.p1, mod4(g.p2 - d * u)), self.a1s.at[m, kk, u], self.a1r.at[m, kk, u], g.axis2(d))

    def fwd1(self, m, u, kk):
        g = self.g
        rows = g.seg_rows(g.p1, mod4(g.p2 - DIRS[kk] * (u + 1)))
        return self.same(m, kk, rows, self.f3s.at[m, kk, u], self.f3r.at[m, kk, u], g.partner)

    def send2(self, m, t, kk, jj):
        g, d = self.g, DIRS[kk]
        rows = g.seg_rows(mod4(g.p1 - d * t), mod4(g.p2 - d * jj))
        return self.same(m, kk, rows, self.a2s.at[m, kk, t, jj], self.a2r.at[m, kk, t, jj], g.axis1(d))

    def fwd2(self, m, t, kk, jj):
        g, d = self.g, DIRS[kk]
        rows = g.seg_rows(mod4(g.p1 - d * (t + 1)), mod4(g.p2 - d * jj))
        idx = 3 + t * 4 + jj
        return self.same(m, kk, rows, self.f3s.at[m, kk, idx], self.f3r.at[m, kk, idx], g.partner)

    def first(self, m):
        self.pair_send(m).wait_recv()
        for kk in range(2):
            self.send1(m, 0, kk).start()
            self.send2(m, 0, kk, 0).start()

    def second(self, m, u):
        for kk in range(2):
            self.send1(m, u, kk).wait_recv()
            if u < 2:
                self.send1(m, u + 1, kk).start()
            self.send2(m, 0, kk, u + 1).start()
            self.fwd1(m, u, kk).start()

    def item(self, m, t, jj):
        for kk in range(2):
            self.send2(m, t, kk, jj).wait_recv()
            if isinstance(t, int):
                if t < 2:
                    self.send2(m, t + 1, kk, jj).start()
            else:
                pl.when(t < 2)(lambda kk=kk: self.send2(m, t + 1, kk, jj).start())
            self.fwd2(m, t, kk, jj).start()

    def round(self, m, t):
        def step(jj, carry):
            self.item(m, t, jj)
            return carry
        lax.fori_loop(0, 4, step, 0)

    def pair_done(self, m):
        def step(i, carry):
            for kk in range(2):
                ref = self.w.at[m, pl.ds(0, SEG), pl.ds(0, SEG)]
                remote(ref, ref, self.f3s.at[m, kk, i], self.f3r.at[m, kk, i], self.g.partner).wait_recv()
            return carry
        lax.fori_loop(0, 15, step, 0)

    def drain(self, m):
        self.pair_send(m).wait_send()
        for kk in range(2):
            for u in range(3):
                self.send1(m, u, kk).wait_send()
                self.fwd1(m, u, kk).wait_send()
        for t in range(3):
            each(lambda kk, jj: self.send2(m, t, kk, jj).wait_send())
            each(lambda kk, jj: self.fwd2(m, t, kk, jj).wait_send())


class StatExchange:
    def __init__(self, g, st, ss, rs):
        self.g, self.st, self.ss, self.rs = g, st, ss, rs

    def copy(self, i):
        return remote(self.st.at[0], self.st.at[1 + i], self.ss.at[i], self.rs.at[i], self.g.xdev((1, -1, 2)[i]))

    def put(self, i, lanes):
        self.st[0, i:i + 1] = jnp.sum(lanes.T, axis=0, keepdims=True)

    def start(self):
        for i in range(3):
            self.copy(i).start()

    def total(self):
        for i in range(3):
            self.copy(i).wait()
        return (self.st[0] + self.st[1]) + (self.st[2] + self.st[3])


def params(cid, vmem_mib=60):
    return pltpu.CompilerParams(collective_id=cid, has_side_effects=True, vmem_limit_bytes=vmem_mib * 1024 * 1024)


COST = pl.CostEstimate(flops=10 ** 11, bytes_accessed=10 ** 8, transcendentals=0)
DMA = pltpu.SemaphoreType.DMA
IN_VMEM = pl.BlockSpec(memory_space=pltpu.VMEM)
IN_HBM = pl.BlockSpec(memory_space=pl.ANY)
SDS = jax.ShapeDtypeStruct


def gather_kernel(wq_in, wk_in, wv_in, x_in, gy_in, wq_out, wk_out, wv_out, x_two, q_out, k_out, v_out, gy_cols, stats,
                  w, x_full, sq, st, ld, xls, xs, xr, xfs, xfr, gls, gs, gr, sts, strv, wos, xps, xpr, xst, *ring):
    w_in, w_out, qkv = (wq_in, wk_in, wv_in), (wq_out, wk_out, wv_out), (q_out, k_out, v_out)
    nw = 3
    g = Torus()
    x, c = g.x, g.c
    rings = WeightRings(g, w, ring)
    ready = greet([g.axis1(1), g.axis1(-1), g.axis2(1), g.axis2(-1), g.xdev(1), g.xdev(-1), g.xdev(2), g.partner])

    def load(m, k):
        src = w_in[m].at[:, at256(k * 1024 + x * SEG)]
        return pltpu.make_async_copy(src, w.at[m, rings.my_rows, pl.ds(k * SEG, SEG)], ld.at[m, k])

    def xseg(b, s):
        return x_full.at[at128(b * 128), pl.ds(s * 1024, 1024)]

    x_own = pltpu.make_async_copy(x_in, x_full.at[at128(x * 128)], xls)

    def xsend(di, s):
        ref = xseg(x, s)
        return remote(ref, ref, xs.at[di, s], xr.at[di, s], g.xdev(DIRS[di]))

    def xfwd(s):
        d = DIRS[s // 2]
        ref = xseg(mod4(x - d), s)
        return remote(ref, ref, xfs.at[s], xfr.at[s], g.xdev(d))

    gy_rows = at128(x * 128)
    gy_own = pltpu.make_async_copy(gy_in.at[x], gy_cols.at[gy_rows], gls)

    def gy_send(i):
        d = (1, -1, 2)[i]
        return remote(gy_in.at[mod4(x + d)], gy_cols.at[gy_rows], gs.at[i], gr.at[i], g.xdev(d))

    stat = StatExchange(g, st, sts, strv)
    x_pair = remote(x_full, x_two.at[pl.ds(512, 512)], xps, xpr, g.partner)
    x_store = pltpu.make_async_copy(x_full, x_two.at[pl.ds(0, 512)], xst)

    def w_store(m):
        return pltpu.make_async_copy(w.at[m], w_out[m], wos.at[m])

    st[0] = jnp.zeros((8, 512), F32)
    x_own.start()
    for m in range(nw):
        for k in range(4):
            load(m, k).start()
    gy_own.start()
    ready()
    x_own.wait()
    for m in range(nw):
        for k in range(4):
            load(m, k).wait()
        rings.pair_send(m).start()
        if m == 0:
            for s in range(4):
                for di in range(2):
                    xsend(di, (s + 2 * di) % 4).start()

    def chunks(m, theirs):
        def step(i, carry):
            k = 2 * ((1 - c) if theirs else c) + i
            cols = at256(k * SEG)
            acc = jnp.dot(x_full[...], w[m, :, cols], preferred_element_type=F32).astype(BF16)
            qkv[m][:, cols] = acc
            if m < 2:
                sqv = acc.astype(F32)
                sqv = sqv * sqv
                sqv = sqv[:, :128] + sqv[:, 128:]
                if theirs:
                    sq[m] = sq[m] + sqv
                else:
                    @pl.when(i == 0)
                    def _():
                        sq[m] = sqv

                    @pl.when(i == 1)
                    def _():
                        sq[m] = sq[m] + sqv
            return carry
        lax.fori_loop(0, 2, step, 0)

    rings.first(0)
    for u in range(3):
        rings.second(0, u)
    for m in range(nw):
        for t in range(3):
            rings.round(m, t)
            if m + 1 < nw:
                if t == 0:
                    rings.first(m + 1)
                rings.second(m + 1, t)
            if (m, t) == (0, 1):
                for s in range(4):
                    xsend(s // 2, s).wait_recv()
                    xfwd(s).start()
                for i in range(3):
                    gy_send(i).start()
            if (m, t) == (1, 1):
                for s in range(4):
                    xsend(1 - s // 2, s).wait_recv()
                    xfwd(s).wait_recv()
                x_pair.start()
                x_store.start()
                chunks(0, False)
            if (m, t) == (1, 2):
                rings.pair_done(0)
                w_store(0).start()
                chunks(0, True)
            if (m, t) == (2, 0):
                chunks(1, False)
            if (m, t) == (2, 1):
                rings.pair_done(1)
                w_store(1).start()
                chunks(1, True)
                for i in range(2):
                    stat.put(i, sq[i])
                stat.start()
    chunks(2, False)
    rings.pair_done(2)
    w_store(2).start()
    chunks(2, True)
    stats[...] = stat.total()

    gy_own.wait()
    for i in range(3):
        gy_send(i).wait()
    for s in range(4):
        xsend(0, s).wait_send()
        xsend(1, s).wait_send()
        xfwd(s).wait_send()
    x_pair.wait()
    x_store.wait()
    for m in range(nw):
        rings.drain(m)
        w_store(m).wait()


def gather_project(w_q, w_k, w_v, x_tok, gy_split):
    return pl.pallas_call(
        gather_kernel,
        out_shape=[SDS((4096, 1024), BF16)] * 3 + [SDS((1024, 4096), BF16)] + [SDS((512, 1024), BF16)] * 4 + [SDS((8, 512), F32)],
        in_specs=[IN_HBM] * 5,
        out_specs=[IN_HBM] * 4 + [IN_VMEM] * 5,
        scratch_shapes=[
            pltpu.VMEM((3, 4096, 1024), BF16),
            pltpu.VMEM((512, 4096), BF16),
            pltpu.VMEM((2, 512, 128), F32),
            pltpu.VMEM((4, 8, 512), F32),
            DMA((3, 4)), DMA(()), DMA((2, 4)), DMA((2, 4)), DMA((4,)), DMA((4,)),
            DMA(()), DMA((3,)), DMA((3,)), DMA((3,)), DMA((3,)), DMA((3,)), DMA(()), DMA(()), DMA(()),
        ] + ring_sems(3),
        compiler_params=params(5), cost_estimate=COST, name='gather_project',
    )(w_q, w_k, w_v, x_tok, gy_split)


SCALE = HEAD_DIM ** -0.5


def rope_turn(u, cos_tab, sin_tab):
    return u * cos_tab + pltpu.roll(u, 64, 1) * sin_tab


def causal_scores(q_blk, keys, i, n):
    s = lax.dot_general(q_blk, keys, (((1,), (1,)), ((), ())), preferred_element_type=F32) * SCALE
    rows = lax.broadcasted_iota(jnp.int32, (128, n), 0) + i * 128
    return jnp.where(rows >= lax.broadcasted_iota(jnp.int32, (128, n), 1), s, -1e30)


def inv_column(total, i):
    return lax.rsqrt(total.T[:, i:i + 1] / 4096.0 + RMS_EPSILON)


def forward_kernel(q0, k0, v0, stats, gains, cos_tab, sin_tab, gy, x_two, wo_in,
                   y_out, q_rot, k_rot, o_two, ga_two, grad_o, post,
                   w, o_full, a_acc, xc, ga_all, y_cols, sa, st,
                   ld, scs, scr, xcs, osd, orv, ofs, ofr, ops, opr, ost, gsd, grv, gfs, gfr, gps, gpr, gst, ysd, yrv, yst, sts, strv, *ring):
    g = Torus()
    x, z, y, c = g.x, g.z, g.y, g.c
    rings = WeightRings(g, w, ring)
    ready = greet([g.axis1(1), g.axis1(-1), g.axis2(1), g.axis2(-1), g.xdev(1), g.xdev(-1), g.xdev(2), g.partner]
                  + [(x, z, mod4(y + d), c) for d in (1, 2, 3)])

    def load(k):
        return pltpu.make_async_copy(wo_in.at[:, at256(k * 1024 + x * SEG)], w.at[0, rings.my_rows, pl.ds(k * SEG, SEG)], ld.at[k])

    def scatter(d):
        to = mod4(y + d)
        dst = w.at[1, at128(z * 1024 + to * SEG + c * 128)]
        return remote(wo_in.at[:, pl.ds(pl.multiple_of(to * 1024, 1024), 1024)], dst, scs.at[d], scr, (x, z, to, c))

    own_rows = pltpu.make_async_copy(wo_in.at[:, pl.ds(pl.multiple_of(y * 1024, 1024), 1024)], w.at[1, rings.my_rows], scs.at[0])

    def xc_load(k):
        return pltpu.make_async_copy(x_two.at[pl.ds(0, 512), at256(k * 1024 + x * SEG)], xc.at[:, pl.ds(k * SEG, SEG)], xcs.at[k])

    for k in range(4):
        load(k).start()
        xc_load(k).start()
    pl.when(y == x)(lambda: own_rows.start())

    inv_q = inv_column(stats[...], 0)
    inv_k = inv_column(stats[...], 1)

    def heads_prep(lo, n):
        def step(h, carry):
            cols = at128(h * 128)
            for src, inv, row, dst in ((q0, inv_q, 0, q_rot), (k0, inv_k, 1, k_rot)):
                u = src[:, cols].astype(F32) * inv * gains[row:row + 1, cols]
                dst[:, cols] = rope_turn(u, cos_tab[...], sin_tab[...]).astype(BF16)
            return carry
        lax.fori_loop(lo, lo + n, step, 0)

    def oblk(k, s):
        return o_full.at[:, at256(k * 1024 + s * SEG)]

    def osend(di, k):
        ref = oblk(k, x)
        return remote(ref, ref, osd.at[di, k], orv.at[di, k], g.xdev(DIRS[di]))

    def ofwd(k):
        d = DIRS[k % 2]
        ref = oblk(k, mod4(x - d))
        return remote(ref, ref, ofs.at[k], ofr.at[k], g.xdev(d))

    o_pair = remote(o_full, o_two.at[pl.ds(512, 512)], ops, opr, g.partner)
    o_store = pltpu.make_async_copy(o_full, o_two.at[pl.ds(0, 512)], ost)

    def gblk(k, s):
        return ga_all.at[s, :, pl.ds(k * SEG, SEG)]

    def gsend(di, k):
        ref = gblk(k, x)
        return remote(ref, ref, gsd.at[di, k], grv.at[di, k], g.xdev(DIRS[di]))

    def gfwd(k):
        d = DIRS[k % 2]
        ref = gblk(k, mod4(x - d))
        return remote(ref, ref, gfs.at[k], gfr.at[k], g.xdev(d))

    half = pl.ds(pl.multiple_of((1 - c) * 512, 512), 512)
    mine = pl.ds(pl.multiple_of(c * 512, 512), 512)
    ga_pair = remote(ga_all.at[x, :, half], ga_two.at[pl.ds(512, 512)], gps, gpr, g.partner)
    ga_store = pltpu.make_async_copy(ga_all.at[x, :, mine], ga_two.at[pl.ds(0, 512)], gst)

    def ysend(i, k):
        d = (1, -1, 2)[i]
        src = y_cols.at[at128(mod4(x + d) * 128), pl.ds(k * SEG, SEG)]
        return remote(src, y_out.at[:, at256(k * 1024 + x * SEG)], ysd.at[i, k], yrv.at[i, k], g.xdev(d))

    def y_store(k):
        return pltpu.make_async_copy(y_cols.at[at128(x * 128), pl.ds(k * SEG, SEG)], y_out.at[:, at256(k * 1024 + x * SEG)], yst.at[k])

    stat = StatExchange(g, st, sts, strv)

    ready()

    @pl.when(y == x)
    def _():
        for d in (1, 3, 2):
            scatter(d).start()
    for k in range(4):
        load(k).wait()
    rings.pair_send(0).start()
    st[0] = jnp.zeros((8, 512), F32)
    heads_prep(0, 1)
    rings.first(0)
    heads_prep(1, 2)
    rings.second(0, 0)
    heads_prep(3, 2)
    rings.second(0, 1)
    heads_prep(5, 2)
    rings.second(0, 2)
    heads_prep(7, 1)

    def head_group(hb, carry):
        for ch in range(2):
            cols = at128(hb * SEG + ch * 128)
            qh, kh, vh = q_rot[:, cols], k_rot[:, cols], v0[:, cols]
            for i in range(4):
                n = (i + 1) * 128
                s = causal_scores(qh[i * 128:n], kh[:n], i, n)
                e = jnp.exp(s - jnp.max(s, axis=-1, keepdims=True))
                p = (e / jnp.sum(e, axis=-1, keepdims=True)).astype(BF16)
                o = jnp.dot(p, vh[:n], preferred_element_type=F32).astype(BF16)
                o_full[pl.ds(i * 128, 128), at128(hb * 1024 + x * SEG + ch * 128)] = o
        for di in range(2):
            osend(di, hb).start()
        for r in range(3):
            it = 3 * hb + r
            rings.item(0, it // 4, lax.rem(it, 4))
        return carry
    lax.fori_loop(0, 4, head_group, 0)

    @pl.when(y == x)
    def _():
        own_rows.wait()

    @pl.when(y != x)
    def _():
        ref = w.at[1, rings.my_rows]
        remote(ref, ref, scs.at[1], scr, g.partner).wait_recv()
    rings.pair_send(1).start()
    rings.pair_done(0)
    rings.first(1)

    def a_part(s, init=False):
        def step(i, carry):
            cols = pl.ds(pl.multiple_of(i * 512, 512), 512)
            acc = None
            for k in range(4):
                dot = jnp.dot(o_full[:, at256(k * 1024 + s * SEG)], w[0, at256(k * 1024 + s * SEG), cols], preferred_element_type=F32)
                acc = dot if acc is None else acc + dot
            a_acc[:, cols] = acc if init else a_acc[:, cols] + acc
            return carry
        lax.fori_loop(0, 2, step, 0)

    a_part(x, True)
    rings.second(1, 0)
    for k in range(4):
        osend(k % 2, k).wait_recv()
        ofwd(k).start()
    rings.second(1, 1)
    rings.second(1, 2)
    rings.round(1, 0)
    for k in range(4):
        osend(1 - k % 2, k).wait_recv()
    a_part(mod4(x - 1))
    rings.round(1, 1)
    a_part(mod4(x + 1))
    for k in range(4):
        ofwd(k).wait_recv()
    a_part(mod4(x + 2))
    o_pair.start()
    o_store.start()
    for k in range(4):
        xc_load(k).wait()

    gpost = gains[2:3, :]

    def a_stats(h, carry):
        cols = at128(h * 128)
        a = a_acc[:, cols].astype(BF16).astype(F32)
        gh = gy[:, cols].astype(F32) * gains[2:3, cols]
        first = h == 0
        for i, v in ((0, a * a), (1, gh * a)):
            sa[i] = jnp.where(first, v, sa[i] + v)
        return carry
    sa[...] = jnp.zeros((2, 512, 128), F32)
    lax.fori_loop(0, 8, a_stats, 0)
    for i in range(2):
        stat.put(i, sa[i])
    stat.start()
    rings.round(1, 2)
    total = stat.total()
    inv_a = inv_column(total, 0)
    mean_a = total.T[:, 1:2] * inv_a / 4096.0

    for k in range(4):
        cols = pl.ds(k * SEG, SEG)
        a_hat = a_acc[:, cols].astype(BF16).astype(F32) * inv_a
        gyv = gy[:, cols].astype(F32)
        ga_all[x, :, cols] = (inv_a * (gyv * gpost[:, k * SEG:(k + 1) * SEG] - a_hat * mean_a)).astype(BF16)
        for di in range(2):
            gsend(di, k).start()
    ga_pair.start()
    ga_store.start()
    rings.pair_done(1)

    def go_part(s, init=False):
        def step(zi, carry):
            cols = at256(zi * SEG)
            acc = None
            for k in range(4):
                dot = lax.dot_general(ga_all[s, :, k * SEG:(k + 1) * SEG], w[1, at256(zi * 1024 + k * SEG), at256(s * SEG)],
                                      (((1,), (1,)), ((), ())), preferred_element_type=F32)
                acc = dot if acc is None else acc + dot
            a_acc[:, cols] = acc if init else a_acc[:, cols] + acc
            return carry
        lax.fori_loop(0, 4, step, 0)

    for k in range(4):
        cols = pl.ds(k * SEG, SEG)
        a_hat = a_acc[:, cols].astype(BF16).astype(F32) * inv_a
        y_cols[:, cols] = (xc[:, cols].astype(F32) + a_hat * gpost[:, k * SEG:(k + 1) * SEG]).astype(BF16)
        post[0:1, cols] = jnp.sum(gy[:, cols].astype(F32) * a_hat, axis=0, keepdims=True)
    go_part(x, True)
    for k in range(4):
        gsend(k % 2, k).wait_recv()
        gfwd(k).start()
    for i in range(3):
        for k in range(4):
            ysend(i, k).start()
    for k in range(4):
        y_store(k).start()
    for k in range(4):
        gsend(1 - k % 2, k).wait_recv()
    go_part(mod4(x - 1))
    go_part(mod4(x + 1))
    for k in range(4):
        gfwd(k).wait_recv()
    go_part(mod4(x + 2))
    grad_o[...] = a_acc[...].astype(BF16)

    @pl.when(y == x)
    def _():
        for d in (1, 2, 3):
            scatter(d).wait_send()
    for k in range(4):
        for di in range(2):
            osend(di, k).wait_send()
            gsend(di, k).wait_send()
        ofwd(k).wait_send()
        gfwd(k).wait_send()
        for i in range(3):
            ysend(i, k).wait()
        y_store(k).wait()
    o_pair.wait()
    o_store.wait()
    ga_pair.wait()
    ga_store.wait()
    for m in range(2):
        rings.drain(m)


def attention_forward(q0, k0, v0, stats, gains, cos_tab, sin_tab, gy_cols, x_two, wo_rows):
    act = SDS((512, 1024), BF16)
    return pl.pallas_call(
        forward_kernel,
        out_shape=[SDS((128, 4096), BF16), act, act, SDS((1024, 4096), BF16), SDS((1024, 512), BF16), act, SDS((1, 1024), F32)],
        in_specs=[IN_VMEM] * 8 + [IN_HBM] * 2,
        out_specs=[IN_HBM, IN_VMEM, IN_VMEM, IN_HBM, IN_HBM, IN_VMEM, IN_VMEM],
        scratch_shapes=[
            pltpu.VMEM((2, 4096, 1024), BF16),
            pltpu.VMEM((512, 4096), BF16),
            pltpu.VMEM((512, 1024), F32),
            pltpu.VMEM((512, 1024), BF16),
            pltpu.VMEM((4, 512, 1024), BF16),
            pltpu.VMEM((512, 1024), BF16),
            pltpu.VMEM((2, 512, 128), F32),
            pltpu.VMEM((4, 8, 512), F32),
            DMA((4,)), DMA((4,)), DMA(()), DMA((4,)), DMA((2, 4)), DMA((2, 4)), DMA((4,)), DMA((4,)), DMA(()), DMA(()), DMA(()),
            DMA((2, 4)), DMA((2, 4)), DMA((4,)), DMA((4,)), DMA(()), DMA(()), DMA(()),
            DMA((3, 4)), DMA((3, 4)), DMA((4,)), DMA((3,)), DMA((3,)),
        ] + ring_sems(2),
        compiler_params=params(6), cost_estimate=COST, name='attention_forward',
    )(q0, k0, v0, stats, gains, cos_tab, sin_tab, gy_cols, x_two, wo_rows)


def backward_kernel(q0, k0, v0, q_rot, k_rot, stats, gains, cos_tab, sin_tab, grad_o,
                    dq_out, dk_out, dv_out, d_two, gain_parts,
                    ghs, dkv, lanes, st, sts, strv, dps, dpr, dst):
    g = Torus()
    c = g.c
    ready = greet([g.xdev(1), g.xdev(-1), g.xdev(2), g.partner])
    stat = StatExchange(g, st, sts, strv)
    outs = (dv_out, dk_out, dq_out)
    half = pl.ds(pl.multiple_of((1 - c) * 512, 512), 512)
    mine = pl.ds(pl.multiple_of(c * 512, 512), 512)

    def pair(m):
        return remote(outs[m].at[:, half], d_two.at[m, pl.ds(512, 512)], dps.at[m], dpr.at[m], g.partner)

    def store(m):
        return pltpu.make_async_copy(outs[m].at[:, mine], d_two.at[m, pl.ds(0, 512)], dst.at[m])

    inv_q = inv_column(stats[...], 0)
    inv_k = inv_column(stats[...], 1)
    lanes[...] = jnp.zeros((2, 512, 128), F32)
    st[0] = jnp.zeros((8, 512), F32)
    tn = (((0,), (0,)), ((), ()))
    nt = (((1,), (1,)), ((), ()))

    def head(h, carry):
        cols = at128(h * 128)
        qh, kh, vh, do = q_rot[:, cols], k_rot[:, cols], v0[:, cols], grad_o[:, cols]
        dkv[...] = jnp.zeros((3, 512, 128), F32)
        for i in range(4):
            n = (i + 1) * 128
            s = causal_scores(qh[i * 128:n], kh[:n], i, n)
            e = jnp.exp(s - jnp.max(s, axis=-1, keepdims=True))
            p = e / jnp.sum(e, axis=-1, keepdims=True)
            do_i = do[i * 128:n]
            dp = lax.dot_general(do_i, vh[:n], nt, preferred_element_type=F32)
            ds = (p * (dp - jnp.sum(p * dp, axis=-1, keepdims=True)) * SCALE).astype(BF16)
            dkv[0, pl.ds(i * 128, 128)] = jnp.dot(ds, kh[:n], preferred_element_type=F32)
            dkv[1, pl.ds(0, n)] = dkv[1, pl.ds(0, n)] + lax.dot_general(ds, qh[i * 128:n], tn, preferred_element_type=F32)
            dkv[2, pl.ds(0, n)] = dkv[2, pl.ds(0, n)] + lax.dot_general(p.astype(BF16), do_i, tn, preferred_element_type=F32)
        dv_out[:, cols] = dkv[2].astype(BF16)
        for i, src, inv in ((0, q0, inv_q), (1, k0, inv_k)):
            gn = rope_turn(dkv[i], cos_tab[...], -sin_tab[...])
            hat = src[:, cols].astype(F32) * inv
            prod = gn * hat
            gain_parts[i:i + 1, cols] = jnp.sum(prod, axis=0, keepdims=True)
            gain = gains[i:i + 1, cols]
            ghs[i, :, cols] = gn * gain
            lanes[i] = lanes[i] + prod * gain
        return carry
    lax.fori_loop(0, 8, head, 0)
    for i in range(2):
        stat.put(i, lanes[i])
    ready()
    stat.start()
    pair(0).start()
    store(0).start()
    total = stat.total().T / 4096.0
    for i, m, src, inv in ((1, 1, k0, inv_k), (0, 2, q0, inv_q)):
        proj = total[:, i:i + 1]

        def finish(h, carry):
            cols = at128(h * 128)
            hat = src[:, cols].astype(F32) * inv
            outs[m][:, cols] = (inv * (ghs[i, :, cols] - hat * proj)).astype(BF16)
            return carry
        lax.fori_loop(0, 8, finish, 0)
        pair(m).start()
        store(m).start()
    for m in range(3):
        pair(m).wait()
        store(m).wait()


def attention_backward(q0, k0, v0, q_rot, k_rot, stats, gains, cos_tab, sin_tab, grad_o):
    act = SDS((512, 1024), BF16)
    return pl.pallas_call(
        backward_kernel,
        out_shape=[act, act, act, SDS((3, 1024, 512), BF16), SDS((2, 1024), F32)],
        in_specs=[IN_VMEM] * 10,
        out_specs=[IN_VMEM, IN_VMEM, IN_VMEM, IN_HBM, IN_VMEM],
        scratch_shapes=[
            pltpu.VMEM((2, 512, 1024), F32),
            pltpu.VMEM((3, 512, 128), F32),
            pltpu.VMEM((2, 512, 128), F32),
            pltpu.VMEM((4, 8, 512), F32),
            DMA((3,)), DMA((3,)), DMA((3,)), DMA((3,)), DMA((3,)),
        ],
        compiler_params=params(7), cost_estimate=COST, name='attention_backward',
    )(q0, k0, v0, q_rot, k_rot, stats, gains, cos_tab, sin_tab, grad_o)


def grads_kernel(*refs):
    parts = refs[:NM]
    gx_part, gy = refs[NM:NM + 2]
    outs = refs[NM + 2:2 * NM + 2]
    gx_out = refs[2 * NM + 2]
    (r1, r2, loc, rg, gloc, s1s, s1r, s2s, s2r, ags, agr, d2s, d2r, fws, fwr, lws, lsem, gs, gr, gsem) = refs[2 * NM + 3:]
    x, z, y, c = (lax.axis_index(n) for n in ('sp', 'z', 'y', 'c'))

    def mod4(v):
        return lax.rem(v + 8, 4)

    p1 = (1 - c) * y + c * z
    p2 = (1 - c) * z + c * y
    dirs = (1, -1)

    def axis1(d):
        return (x, mod4(z + d * c), mod4(y + d * (1 - c)), c)

    def axis2(d):
        return (x, mod4(z + d * (1 - c)), mod4(y + d * c), c)

    def xdev(d, core):
        return (mod4(x + d), z, y, core)

    partner = (x, z, y, 1 - c)
    peers = [axis1(1), axis1(-1), axis2(1), axis2(-1), xdev(1, c), xdev(-1, c), xdev(1, 1 - c), xdev(-1, 1 - c), partner]
    barrier = pltpu.get_barrier_semaphore()
    for peer in peers:
        pl.semaphore_signal(barrier, inc=1, device_id=peer, device_id_type=MESH_ID)
    pl.semaphore_wait(barrier, len(peers))

    def seg_rows(b, j):
        zz = (1 - c) * j + c * b
        yy = (1 - c) * b + c * j
        return pl.ds(pl.multiple_of(zz * 1024 + yy * SEG, SEG), SEG)

    def remote(src, dst, ss, rs, dev):
        return pltpu.make_async_remote_copy(src_ref=src, dst_ref=dst, send_sem=ss, recv_sem=rs, device_id=dev, device_id_type=MESH_ID)

    def send1(m, t, kk, jj):
        d = dirs[kk]
        if t == 0:
            rows = seg_rows(mod4(p1 - d), mod4(p2 - d * (1 + jj)))
            src = parts[m].at[rows, pl.ds(kk * SEG, SEG)]
        else:
            src = r1.at[m, kk, t - 1, jj]
        return remote(src, r1.at[m, kk, t, jj], s1s.at[m, kk, t, jj], s1r.at[m, kk, t, jj], axis1(d))

    def load(m, t, kk, jj):
        d = dirs[kk]
        par = (3 * m + t) % 2
        rows = seg_rows(mod4(p1 - d * (2 + t)), mod4(p2 - d * (1 + jj)))
        return pltpu.make_async_copy(parts[m].at[rows, pl.ds(kk * SEG, SEG)], loc.at[par, kk, jj], lsem.at[par, kk, jj])

    def send2(m, u, kk):
        return remote(r1.at[m, kk, 2, u], r2.at[m, kk, u], s2s.at[m, kk, u], s2r.at[m, kk, u], axis2(dirs[kk]))

    def out_cols(k, xs):
        return pl.ds(pl.multiple_of(k * 1024 + xs * SEG, SEG), SEG)

    def ag_send(m, kk, di, h):
        k = 2 * c + kk
        return remote(r1.at[m, kk, 2, 3, pl.ds(h * 128, 128)], outs[m].at[:, out_cols(k, x)], ags.at[m, kk, di, h], agr.at[m, di, k], xdev(dirs[di], h))

    def ag_recv(m, di, k):
        cols = out_cols(k, mod4(x - dirs[di]))
        return remote(outs[m].at[:, cols], outs[m].at[:, cols], ags.at[m, 0, di, 0], agr.at[m, di, k], xdev(dirs[di], c))

    def pair_send(m, kk):
        k = 2 * c + kk
        rows = pl.ds(pl.multiple_of((1 - c) * 128, 128), 128)
        return remote(r1.at[m, kk, 2, 3, rows], outs[m].at[:, out_cols(k, x)], d2s.at[m, kk], d2r.at[m, kk], partner)

    def own_store(m, kk):
        k = 2 * c + kk
        rows = pl.ds(pl.multiple_of(c * 128, 128), 128)
        return pltpu.make_async_copy(r1.at[m, kk, 2, 3, rows], outs[m].at[:, out_cols(k, x)], lws.at[m, kk])

    def forward(m, k):
        di = k % 2
        cols = out_cols(k, mod4(x - dirs[di]))
        return remote(outs[m].at[:, cols], outs[m].at[:, cols], fws.at[m, k], fwr.at[m, k], xdev(dirs[di], c))

    def gcols(kk, jj):
        return pl.ds(pl.multiple_of(kk * 2048 + jj * 512, 512), 512)

    def gsend(t, kk, jj):
        d = dirs[kk]
        if t == 0:
            src = gx_part.at[pl.ds(pl.multiple_of(mod4(x - d) * 128, 128), 128), gcols(kk, jj)]
        else:
            src = rg.at[kk, t - 1, jj]
        return remote(src, rg.at[kk, t, jj], gs.at[kk, t, jj], gr.at[kk, t, jj], xdev(d, c))

    def gload(t, kk, jj):
        rows = pl.ds(pl.multiple_of(mod4(x - dirs[kk] * (2 + t)) * 128, 128), 128)
        return pltpu.make_async_copy(gx_part.at[rows, gcols(kk, jj)], gloc.at[t % 2, kk, jj], gsem.at[t % 2, kk, jj])

    def each(fn):
        def step(jj, carry):
            for kk in range(2):
                fn(kk, jj)
            return carry
        lax.fori_loop(0, 4, step, 0)

    each(lambda kk, jj: send1(0, 0, kk, jj).start())
    each(lambda kk, jj: load(0, 0, kk, jj).start())
    each(lambda kk, jj: gsend(0, kk, jj).start())
    each(lambda kk, jj: gload(0, kk, jj).start())

    def phase2(m, u):
        for kk in range(2):
            send2(m, u - 1, kk).wait_recv()
            r1[m, kk, 2, u] = r1[m, kk, 2, u] + r2[m, kk, u - 1]
            if u < 3:
                send2(m, u, kk).start()
            else:
                own_store(m, kk).start()
                for di in range(2):
                    for h in range(2):
                        ag_send(m, kk, di, h).start()
                pair_send(m, kk).start()

    def do_forward(m):
        for k in range(4):
            ag_recv(m, k % 2, k).wait_recv()
            forward(m, k).start()

    def gx_step(t):
        if t < 2:
            each(lambda kk, jj: gload(t + 1, kk, jj).start())

        def item(kk, jj):
            gsend(t, kk, jj).wait_recv()
            gload(t, kk, jj).wait()
            total = rg[kk, t, jj] + gloc[t % 2, kk, jj]
            if t < 2:
                rg[kk, t, jj] = total
                gsend(t + 1, kk, jj).start()
            else:
                gx_out[:, gcols(kk, jj)] = (total + gy[:, gcols(kk, jj)].astype(F32)).astype(BF16)
        each(item)

    last = 3 * NM
    for r in range(last):
        m, t = divmod(r, 3)
        if r + 1 < last:
            mn, tn = divmod(r + 1, 3)
            each(lambda kk, jj: load(mn, tn, kk, jj).start())

        def item(kk, jj):
            send1(m, t, kk, jj).wait_recv()
            load(m, t, kk, jj).wait()
            r1[m, kk, t, jj] = r1[m, kk, t, jj] + loc[r % 2, kk, jj]
            if t < 2:
                send1(m, t + 1, kk, jj).start()
            elif m + 1 < NM:
                send1(m + 1, 0, kk, jj).start()

        each(item)
        if t == 2:
            for kk in range(2):
                send2(m, 0, kk).start()
        if m > 0 and t == 0:
            phase2(m - 1, 1)
        if m > 0 and t == 1:
            phase2(m - 1, 2)
        if m > 0 and t == 2:
            phase2(m - 1, 3)
        if m > 1 and t == 0:
            do_forward(m - 2)
        if r in (2, 4, 6):
            gx_step((r - 2) // 2)
    for u in (1, 2, 3):
        phase2(NM - 1, u)
    if NM > 1:
        do_forward(NM - 2)
    do_forward(NM - 1)

    for m in range(NM):
        for t in range(3):
            each(lambda kk, jj: send1(m, t, kk, jj).wait_send())
        for kk in range(2):
            for u in range(3):
                send2(m, u, kk).wait_send()
            for di in range(2):
                for h in range(2):
                    ag_send(m, kk, di, h).wait_send()
            pair_send(m, kk).wait()
            own_store(m, kk).wait()
        for k in range(4):
            ag_recv(m, 1 - k % 2, k).wait_recv()
            forward(m, k).wait()
    for t in range(3):
        each(lambda kk, jj: gsend(t, kk, jj).wait_send())


def reduce_grads(parts, gx_part, gy):
    nm = len(parts)
    dma = pltpu.SemaphoreType.DMA
    vmem = pl.BlockSpec(memory_space=pltpu.VMEM)
    hbm = pl.BlockSpec(memory_space=HBM)
    return pl.pallas_call(
        grads_kernel,
        out_shape=[jax.ShapeDtypeStruct((128, 4096), F32)] * nm + [jax.ShapeDtypeStruct((128, 4096), BF16)],
        in_specs=[hbm] * (nm + 1) + [vmem],
        out_specs=[hbm] * nm + [vmem],
        scratch_shapes=[
            pltpu.VMEM((nm, 2, 3, 4, SEG, SEG), F32),
            pltpu.VMEM((nm, 2, 3, SEG, SEG), F32),
            pltpu.VMEM((2, 2, 4, SEG, SEG), F32),
            pltpu.VMEM((2, 3, 4, 128, 512), F32),
            pltpu.VMEM((2, 2, 4, 128, 512), F32),
            dma((nm, 2, 3, 4)), dma((nm, 2, 3, 4)),
            dma((nm, 2, 3)), dma((nm, 2, 3)),
            dma((nm, 2, 2, 2)), dma((nm, 2, 4)),
            dma((nm, 2)), dma((nm, 2)),
            dma((nm, 4)), dma((nm, 4)),
            dma((nm, 2)), dma((2, 2, 4)),
            dma((2, 3, 4)), dma((2, 3, 4)), dma((2, 2, 4)),
        ],
        compiler_params=pltpu.CompilerParams(collective_id=4, has_side_effects=True, vmem_limit_bytes=60 * 1024 * 1024),
        cost_estimate=pl.CostEstimate(flops=10 ** 11, bytes_accessed=10 ** 8, transcendentals=0),
        name='reduce_grads',
    )(*parts, gx_part, gy)


def solution(mesh):
    mesh4 = Mesh(mesh.devices.reshape(4, 4, 4, 2), ('sp', 'z', 'y', 'c'))
    tok_spec = P(FS, 'sp', None)
    row_spec = P(FS, None)
    vec_spec = P(FS)

    def local_step(x, grad_y, wq_rows, wk_rows, wv_rows, wo_rows, gq_rows, gk_rows, gpost_rows):
        _, tok_len, width = x.shape
        lw = width // 4
        s, zi, yi, ci = coords()
        x_tok, gy_tok = x[0], grad_y[0]

        gains = jnp.concatenate([jnp.stack([gq_rows, gk_rows, gpost_rows]), jnp.zeros((61, HEAD_DIM), F32)], axis=0)
        gains = lax.all_gather(gains, FS, axis=0, tiled=False)[:, :3].reshape(4, 4, 2, 3, HEAD_DIM)
        gains = lax.dynamic_index_in_dim(gains, s, 1, False).transpose(2, 0, 1, 3).reshape(3, lw)
        cos_tab, sin_tab = rope_tables(4 * tok_len)

        gy_split = gy_tok.reshape(tok_len, 4, 4, lw // 4).transpose(2, 0, 1, 3).reshape(4, tok_len, lw)
        w_q, w_k, w_v, x_two, q0, k0, v0, gy_cols, stats = gather_project(wq_rows, wk_rows, wv_rows, x_tok, gy_split)
        y, q_rot, k_rot, o_two, ga_two, grad_o, post = attention_forward(
            q0, k0, v0, stats, gains, cos_tab, sin_tab, gy_cols, x_two, wo_rows)
        dq, dk, dv, d_two, gain_parts = attention_backward(q0, k0, v0, q_rot, k_rot, stats, gains, cos_tab, sin_tab, grad_o)

        def weight_part(left, right):
            return lax.dot_general(left, right, (((0,), (0,)), ((), ())), preferred_element_type=F32)

        def back(g, w):
            return lax.dot_general(g, w, (((1,), (1,)), ((), ())), preferred_element_type=F32)

        po = weight_part(o_two, ga_two)
        pv, pk, pq = (weight_part(x_two, d_two[m]) for m in range(3))
        gx_part = back(dq, w_q) + back(dk, w_k) + back(dv, w_v)
        dwo, dwv, dwk, dwq, grad_x = reduce_grads([po, pv, pk, pq], gx_part, gy_tok)

        parts = jnp.concatenate([gain_parts, post], axis=0)
        every = lax.all_gather(parts, ('sp',) + FS, axis=0, tiled=False).reshape(4, 32, 3, 4, 2, HEAD_DIM)
        every = lax.dynamic_slice(every, (yi, 0, 0, zi, ci, 0), (1, 32, 3, 1, 1, HEAD_DIM))
        gn = jnp.sum(every, axis=(0, 1, 3, 4))
        return y[None], grad_x[None], dwq, dwk, dwv, dwo, gn[0], gn[1], gn[2]

    return jax.shard_map(local_step, mesh=mesh4,
                         in_specs=(tok_spec, tok_spec, row_spec, row_spec, row_spec, row_spec, vec_spec, vec_spec, vec_spec),
                         out_specs=(tok_spec, tok_spec, row_spec, row_spec, row_spec, row_spec, vec_spec, vec_spec, vec_spec),
                         check_vma=False)
```

```python
import jax
import jax.numpy as jnp
import numpy as np
from jax import lax
from jax.experimental import pallas as pl
from jax.experimental.pallas import tpu as pltpu
from jax.sharding import Mesh, PartitionSpec as P

HEAD_DIM = 128
RMS_EPSILON = 1e-6
ROPE_THETA = 500000.0
FS = ('z', 'y', 'c')
F32 = jnp.float32
BF16 = jnp.bfloat16
MESH_ID = pl.DeviceIdType.MESH
HBM = pl.ANY
SEG = 256


def rope_tables(seq_len):
    half_dim = HEAD_DIM // 2
    angles = np.arange(seq_len)[:, None] * ROPE_THETA ** (-np.arange(half_dim) * (2.0 / HEAD_DIM))[None, :]
    cos_half, sin_half = np.cos(angles), np.sin(angles)
    tables = np.concatenate([cos_half, cos_half], axis=1), np.concatenate([-sin_half, sin_half], axis=1)
    return tuple(jnp.asarray(t, F32) for t in tables)


def coords():
    return tuple(lax.axis_index(n) for n in ('sp', 'z', 'y', 'c'))


def mod4(v):
    return lax.rem(v + 8, 4)


def remote(src, dst, ss, rs, dev):
    return pltpu.make_async_remote_copy(src_ref=src, dst_ref=dst, send_sem=ss, recv_sem=rs, device_id=dev, device_id_type=MESH_ID)


def at256(v):
    return pl.ds(pl.multiple_of(v, SEG), SEG)


def at128(v):
    return pl.ds(pl.multiple_of(v, 128), 128)


def each(fn, n=4):
    def step(jj, carry):
        for kk in range(2):
            fn(kk, jj)
        return carry
    lax.fori_loop(0, n, step, 0)


def loop(lo, hi, fn):
    def step(n, carry):
        fn(n)
        return carry
    lax.fori_loop(lo, hi, step, 0)


def greet(peers):
    barrier = pltpu.get_barrier_semaphore()
    for peer in peers:
        pl.semaphore_signal(barrier, inc=1, device_id=peer, device_id_type=MESH_ID)
    return lambda: pl.semaphore_wait(barrier, len(peers))


class Torus:
    def __init__(self):
        self.x, self.z, self.y, self.c = x, z, y, c = coords()
        self.p1 = (1 - c) * y + c * z
        self.p2 = (1 - c) * z + c * y
        self.partner = (x, z, y, 1 - c)

    def axis1(self, d):
        return (self.x, mod4(self.z + d * self.c), mod4(self.y + d * (1 - self.c)), self.c)

    def axis2(self, d):
        return (self.x, mod4(self.z + d * (1 - self.c)), mod4(self.y + d * self.c), self.c)

    def xdev(self, d, core=None):
        return (mod4(self.x + d), self.z, self.y, self.c if core is None else core)

    def seg_rows(self, b, j):
        zz = (1 - self.c) * j + self.c * b
        yy = (1 - self.c) * b + self.c * j
        return at256(zz * 1024 + yy * SEG)


DIRS = (1, -1)
RING_SEMS = 8


def ring_sems(nw):
    dma = pltpu.SemaphoreType.DMA
    return [dma((nw,)), dma((nw,)), dma((nw,)), dma((nw, 3)), dma((nw,)), dma((nw, 3, 4)), dma((nw,)), dma((nw,))]


class WeightRings:
    def __init__(self, g, w, slots, sems):
        self.g, self.w, self.slots = g, w, slots
        self.d0s, self.d0r, self.a1s, self.a1r, self.a2s, self.a2r, self.f3s, self.f3r = sems
        self.my_rows = at128(g.z * 1024 + g.y * SEG + g.c * 128)

    def pair_send(self, m):
        ref = self.w.at[self.slots[m], self.my_rows]
        return remote(ref, ref, self.d0s.at[m], self.d0r.at[m], self.g.partner)

    def same(self, m, kk, rows, ss, rs, dev):
        ref = self.w.at[self.slots[m], rows, at256((2 * self.g.c + kk) * SEG)]
        return remote(ref, ref, ss, rs, dev)

    def bulk(self, m, n, ss, rs):
        ref = self.w.at[self.slots[m], pl.ds(0, n * 128), pl.ds(0, 512)]
        return remote(ref, ref, ss, rs, self.g.partner)

    def send1(self, m, u, kk):
        g, d = self.g, DIRS[kk]
        return self.same(m, kk, g.seg_rows(g.p1, mod4(g.p2 - d * u)), self.a1s.at[m], self.a1r.at[m, u], g.axis2(d))

    def far1(self, m, e, kk):
        g = self.g
        rows = g.seg_rows(g.p1, g.p2)
        return self.same(m, kk, rows, self.a1s.at[m], self.a1r.at[m, e - 1], g.axis2(DIRS[kk] * e))

    def fwd1(self, m, u, kk):
        g = self.g
        rows = g.seg_rows(g.p1, mod4(g.p2 - DIRS[kk] * (u + 1)))
        return self.same(m, kk, rows, self.f3s.at[m], self.f3r.at[m], g.partner)

    def send2(self, m, t, kk, jj):
        g, d = self.g, DIRS[kk]
        rows = g.seg_rows(mod4(g.p1 - d * t), mod4(g.p2 - d * jj))
        return self.same(m, kk, rows, self.a2s.at[m], self.a2r.at[m, t, jj], g.axis1(d))

    def fwd2(self, m, t, kk, jj):
        g, d = self.g, DIRS[kk]
        rows = g.seg_rows(mod4(g.p1 - d * (t + 1)), mod4(g.p2 - d * jj))
        return self.same(m, kk, rows, self.f3s.at[m], self.f3r.at[m], g.partner)

    def first(self, m, far=False):
        self.pair_send(m).wait_recv()
        for kk in range(2):
            if far:
                for e in (1, 2, 3):
                    self.far1(m, e, kk).start()
            else:
                self.send1(m, 0, kk).start()
            self.send2(m, 0, kk, 0).start()

    def second(self, m, u, far=False):
        self.bulk(m, 2, self.a1s.at[m], self.a1r.at[m, u]).wait_recv()
        for kk in range(2):
            if u < 2 and not far:
                self.send1(m, u + 1, kk).start()
            self.send2(m, 0, kk, u + 1).start()
            self.fwd1(m, u, kk).start()

    def item(self, m, t, jj):
        self.bulk(m, 2, self.a2s.at[m], self.a2r.at[m, t, jj]).wait_recv()

        def pass_on():
            for kk in range(2):
                self.send2(m, t + 1, kk, jj).start()
        if isinstance(t, int):
            if t < 2:
                pass_on()
        else:
            pl.when(t < 2)(pass_on)
        for kk in range(2):
            self.fwd2(m, t, kk, jj).start()

    def round(self, m, t, extra=None):
        def step(jj):
            self.item(m, t, jj)
            if extra is not None:
                extra(jj)
        loop(0, 4, step)

    def pair_done(self, m):
        self.bulk(m, 30, self.f3s.at[m], self.f3r.at[m]).wait_recv()

    def drain(self, m):
        self.pair_send(m).wait_send()
        for sems, n in ((self.a1s, 6), (self.a2s, 24), (self.f3s, 30)):
            self.bulk(m, n, sems.at[m], self.f3r.at[m]).wait_send()


class StatExchange:
    def __init__(self, g, st, ss, rs):
        self.g, self.st, self.ss, self.rs = g, st, ss, rs

    def copy(self, i):
        return remote(self.st.at[0], self.st.at[1 + i], self.ss.at[i], self.rs.at[i], self.g.xdev((1, -1, 2)[i]))

    def put(self, i, lanes):
        self.st[0, i:i + 1] = jnp.sum(lanes.T, axis=0, keepdims=True)

    def start(self):
        for i in range(3):
            self.copy(i).start()

    def total(self):
        for i in range(3):
            self.copy(i).wait()
        return (self.st[0] + self.st[1]) + (self.st[2] + self.st[3])


def params(cid, vmem_mib=60.0):
    return pltpu.CompilerParams(collective_id=cid, has_side_effects=True, vmem_limit_bytes=int(vmem_mib * 1024 * 1024))


COST = pl.CostEstimate(flops=10 ** 11, bytes_accessed=10 ** 8, transcendentals=0)
DMA = pltpu.SemaphoreType.DMA
IN_VMEM = pl.BlockSpec(memory_space=pltpu.VMEM)
IN_HBM = pl.BlockSpec(memory_space=pl.ANY)
SDS = jax.ShapeDtypeStruct


SCALE = HEAD_DIM ** -0.5
TN = (((0,), (0,)), ((), ()))
NT = (((1,), (1,)), ((), ()))
W_SLOTS = (0, 1, 2, 0, 1)


def rope_turn(u, cos_tab, sin_tab):
    return u * cos_tab + pltpu.roll(u, 64, 1) * sin_tab


def causal_scores(q_blk, keys, i, n):
    s = lax.dot_general(q_blk, keys, NT, preferred_element_type=F32) * SCALE
    rows = lax.broadcasted_iota(jnp.int32, (128, n), 0) + i * 128
    return jnp.where(rows >= lax.broadcasted_iota(jnp.int32, (128, n), 1), s, -1e30)


def inv_column(total, i):
    return lax.rsqrt(total.T[:, i:i + 1] / 4096.0 + RMS_EPSILON)


def forward_kernel(wq_in, wk_in, wv_in, wo_in, x_in, gy_in, gq_in, gk_in, gp_in, cos_tab, sin_tab,
                   wq_out, wk_out, wv_out, x_t, q_out, k_out, v_out, qr_out, kr_out, y_out, a_out, p_out, go_out, gains, stats, post,
                   w, x_full, xt, gyc, xcv, qkv, gains_in, a_acc, o_full, ga_all, gtw, sq, st, st2, r1, s0, a_seg, stage,
                   ld, xls, xs, xr, xfs, xfr, gls, gys, gyr, sts, strv, sts2, strv2, wos, xps, xpr, xst, outs,
                   g1s, g1r, g2s, g2r, g3s, g3r, free,
                   scs, scr, osd, orv, ofs, ofr, ops, opr, gsd, grv, gfs, gfr, gps, gpr, s1s, s1r, sgs, *ring):
    w_in, w_out, qkv_out = (wq_in, wk_in, wv_in, wo_in), (wq_out, wk_out, wv_out), (q_out, k_out, v_out)
    nw = 3
    cols_m, rows_m = 3, 4
    g = Torus()
    x, z, y, c, p1, p2 = g.x, g.z, g.y, g.c, g.p1, g.p2
    rings = WeightRings(g, w, W_SLOTS, ring)
    plane = [(x, mod4(z + d), y, c) for d in (1, 2, 3)] + [(x, z, mod4(y + d), c) for d in (1, 2, 3)] + [g.partner]
    ready = greet(plane + [g.xdev(1), g.xdev(-1), g.xdev(2)])

    def load(m, k):
        src = w_in[m].at[:, at256(k * 1024 + x * SEG)]
        return pltpu.make_async_copy(src, w.at[W_SLOTS[m], rings.my_rows, pl.ds(k * SEG, SEG)], ld.at[m])

    def load_wait(m):
        ref = w.at[W_SLOTS[m], rings.my_rows]
        pltpu.make_async_copy(ref, ref, ld.at[m]).wait()

    def xseg(b, s):
        return x_full.at[at128(b * 128), pl.ds(s * 1024, 1024)]

    x_own = pltpu.make_async_copy(x_in, x_full.at[at128(x * 128)], xls)

    def xsend(di, s):
        ref = xseg(x, s)
        return remote(ref, ref, xs, xr.at[di, s], g.xdev(DIRS[di]))

    def xfwd(s):
        d = DIRS[s // 2]
        ref = xseg(mod4(x - d), s)
        return remote(ref, ref, xfs, xfr.at[s], g.xdev(d))

    gy_rows = at128(x * 128)

    def gy_own(k):
        return pltpu.make_async_copy(gy_in.at[:, at256(k * 1024 + x * SEG)], gyc.at[gy_rows, pl.ds(k * SEG, SEG)], gls)

    def gy_send(i, k):
        d = (1, -1, 2)[i]
        src = gy_in.at[:, at256(k * 1024 + mod4(x + d) * SEG)]
        return remote(src, gyc.at[gy_rows, pl.ds(k * SEG, SEG)], gys, gyr, g.xdev(d))

    def gblock(zh, ch):
        return gains.at[:, at128(zh * SEG + ch * 128)]

    def gain1(d):
        return remote(gains_in, gblock(z, c), g1s, g1r, (x, z, mod4(y + d), c))

    def gain2(d):
        ref = gblock(z, c)
        return remote(ref, ref, g2s, g2r, (x, mod4(z + d), y, c))

    def gain3(zh):
        ref = gblock(zh, c)
        return remote(ref, ref, g3s, g3r, g.partner)

    stat = StatExchange(g, st, sts, strv)
    stat2 = StatExchange(g, st2, sts2, strv2)

    def xt_pair(b):
        return remote(xt.at[lax.rem(b, 2)], x_t.at[pl.ds(pl.multiple_of(b * 1024, 1024), 1024), pl.ds(512, 512)], xps.at[b], xpr.at[b], g.partner)

    def xt_store(b):
        return pltpu.make_async_copy(xt.at[lax.rem(b, 2)], x_t.at[pl.ds(pl.multiple_of(b * 1024, 1024), 1024), pl.ds(0, 512)], xst.at[b])

    def turn(b):
        @pl.when(b >= 2)
        def _():
            xt_pair(b - 2).wait_send()
            xt_store(b - 2).wait()

        def step(i):
            xt[lax.rem(b, 2), at256(i * SEG), :] = x_full[:, at256(b * 1024 + i * SEG)].T
        loop(0, 4, step)
        xt_pair(b).start()
        xt_store(b).start()

    def w_store(m, theirs):
        cols = pl.ds(pl.multiple_of(((1 - c) if theirs else c) * 512, 512), 512)
        return pltpu.make_async_copy(w.at[m, :, cols], w_out[m].at[:, cols], wos.at[m, int(theirs)])

    def qkv_store(m):
        return pltpu.make_async_copy(qkv.at[m], qkv_out[m], outs.at[m])

    rot_store = [pltpu.make_async_copy(qkv.at[0], qr_out, outs.at[3]), pltpu.make_async_copy(qkv.at[1], kr_out, outs.at[4])]
    y_store = pltpu.make_async_copy(xcv, y_out, outs.at[5])
    a_store = pltpu.make_async_copy(a_seg, a_out, outs.at[6])
    go_store = pltpu.make_async_copy(qkv.at[0], go_out, outs.at[7])

    st[0] = jnp.zeros((8, 512), F32)
    st2[0] = jnp.zeros((8, 512), F32)
    sq[...] = jnp.zeros((2, 512, 128), F32)
    gains_in[...] = jnp.concatenate([gq_in[...], gk_in[...], gp_in[...], jnp.zeros((5, 128), F32)], axis=0)
    for k in range(4):
        load(0, k).start()
    x_own.start()
    for m in range(1, nw):
        for k in range(4):
            load(m, k).start()
    for k in range(4):
        gy_own(k).start()
    ready()
    for m in range(nw):
        load_wait(m)
        rings.pair_send(m).start()
        if m == 0:
            x_own.wait()
            for s in range(4):
                for di in range(2):
                    xsend(di, (s + 2 * di) % 4).start()

    @pl.when(y == x)
    def _():
        gains[:, at128(z * SEG + c * 128)] = gains_in[...]
        for d in (1, 2, 3):
            gain1(d).start()

    def chunk(m, theirs, i):
        cols = at256((2 * ((1 - c) if theirs else c) + i) * SEG)
        acc_ref = a_acc.at[:, pl.ds(0, SEG)]

        def accumulate(kc):
            rows = pl.ds(pl.multiple_of(kc * 2048, 2048), 2048)
            acc_ref[...] = acc_ref[...] + jnp.dot(x_full[:, rows], w[m, rows, cols], preferred_element_type=F32)
        acc_ref[...] = jnp.zeros((512, SEG), F32)
        loop(0, 2, accumulate)
        acc = acc_ref[...].astype(BF16)
        qkv[m, :, cols] = acc
        if m < 2:
            sqv = acc.astype(F32)
            sqv = sqv * sqv
            sq[m] = sq[m] + (sqv[:, :128] + sqv[:, 128:])

    def chunk_beside(m, theirs):
        return lambda jj: pl.when(lax.rem(jj, 2) == 1)(lambda: chunk(m, theirs, jj // 2))

    rings.first(0, True)
    rings.first(1)
    for u in range(3):
        rings.second(0, u, True)

    def beside(m, t):
        if (m, t) == (1, 1):
            own = chunk_beside(0, False)

            def both(jj):
                turn(jj)
                own(jj)
            return both
        return {(1, 2): chunk_beside(0, True), (2, 0): chunk_beside(1, False), (2, 1): chunk_beside(1, True)}.get((m, t))

    for m in range(nw):
        for t in range(3):
            if (m, t) == (2, 1):
                rings.pair_done(1)
                w_store(1, True).start()
            rings.round(m, t, beside(m, t))
            if m + 1 < nw:
                rings.second(m + 1, t)
            if (m, t) == (0, 0):
                @pl.when(y != x)
                def _():
                    remote(gains_in, gblock(z, c), g1s, g1r, g.partner).wait_recv()
                for d in (1, 2, 3):
                    gain2(d).start()
            if (m, t) == (0, 1):
                rings.first(2)
                for s in range(4):
                    xsend(s // 2, s).wait_recv()
                    xfwd(s).start()
                for k in range(4):
                    for i in range(3):
                        gy_send(i, k).start()
            if (m, t) == (0, 2):
                w_store(0, False).start()
                gain_rest = gains.at[:, pl.ds(0, 384)]
                remote(gain_rest, gain_rest, g2s, g2r, g.partner).wait()
                for zh in range(4):
                    gain3(zh).start()
            if (m, t) == (1, 0):
                rings.pair_done(0)
                w_store(0, True).start()
                for s in range(4):
                    xsend(1 - s // 2, s).wait_recv()
                    xfwd(s).wait_recv()
            if (m, t) == (1, 2):
                w_store(1, False).start()
                qkv_store(0).start()
                for k in range(4):
                    xcv[:, pl.ds(k * SEG, SEG)] = x_full[:, at256(k * 1024 + x * SEG)]
                rings.drain(0)
                w_store(0, False).wait()
                w_store(0, True).wait()
                for k in range(4):
                    load(cols_m, k).start()
            if (m, t) == (2, 1):
                qkv_store(1).start()
                for i in range(2):
                    stat.put(i, sq[i])
                stat.start()
                rings.drain(1)
                w_store(1, False).wait()
                w_store(1, True).wait()
                half_x, quarter_x = x_full.at[:, pl.ds(0, 2048)], x_full.at[:, pl.ds(0, 1024)]
                remote(half_x, half_x, xs, xr.at[0, 0], g.partner).wait_send()
                remote(quarter_x, quarter_x, xfs, xr.at[0, 0], g.partner).wait_send()
                for peer in plane:
                    pl.semaphore_signal(free, inc=1, device_id=peer, device_id_type=MESH_ID)
                qkv_store(0).wait()

    load_wait(cols_m)
    pl.semaphore_wait(free, len(plane))
    rings.pair_send(cols_m).start()

    def scatter(d):
        to = mod4(y + d)
        dst = w.at[1, at128(z * 1024 + to * SEG + c * 128)]
        return remote(wo_in.at[:, pl.ds(pl.multiple_of(to * 1024, 1024), 1024)], dst, scs.at[d], scr, (x, z, to, c))

    own_rows = pltpu.make_async_copy(wo_in.at[:, pl.ds(pl.multiple_of(y * 1024, 1024), 1024)], w.at[1, rings.my_rows], scs.at[0])

    @pl.when(y == x)
    def _():
        own_rows.start()
        for d in (1, 3, 2):
            scatter(d).start()
    w_store(2, False).start()
    total = stat.total()
    stats[...] = total
    inv_q, inv_k = inv_column(total, 0), inv_column(total, 1)
    loop(0, 2, lambda i: chunk(2, False, i))
    rings.first(cols_m, True)
    gain_half = gains.at[:, pl.ds(0, 512)]
    remote(gain_half, gain_half, g3s, g3r, g.partner).wait()
    qkv_store(1).wait()

    def heads_prep(base):
        def step(i):
            cols = at128((base + i) * 128)
            for j, inv in ((0, inv_q), (1, inv_k)):
                u = qkv[j, :, cols].astype(F32) * inv * gains[j:j + 1, cols]
                qkv[j, :, cols] = rope_turn(u, cos_tab[...], sin_tab[...]).astype(BF16)
        loop(0, 4, step)

    def oblk(k, s):
        return o_full.at[:, at256(k * 1024 + s * SEG)]

    def osend(di, k):
        ref = oblk(k, x)
        return remote(ref, ref, osd, orv.at[di, k], g.xdev(DIRS[di]))

    def ofwd(k, di):
        d = DIRS[di]
        ref = oblk(k, mod4(x - d))
        return remote(ref, ref, ofs, ofr.at[k], g.xdev(d))

    def attend(k):
        for ch in range(2):
            cols = at128(k * SEG + ch * 128)
            qh, kh, vh = qkv[0, :, cols], qkv[1, :, cols], qkv[2, :, cols]
            for i in range(4):
                n = (i + 1) * 128
                s = causal_scores(qh[i * 128:n], kh[:n], i, n)
                e = jnp.exp(s - jnp.max(s, axis=-1, keepdims=True))
                p = (e * (1.0 / jnp.sum(e, axis=-1, keepdims=True))).astype(BF16)
                o = jnp.dot(p, vh[:n], preferred_element_type=F32).astype(BF16)
                o_full[pl.ds(i * 128, 128), at128(k * 1024 + x * SEG + ch * 128)] = o
        for di in range(2):
            osend(di, k).start()

    def cols_items(lo, hi):
        loop(lo, hi, lambda it: rings.item(cols_m, it // 4, lax.rem(it, 4)))

    def o_forward(base):
        for i in range(2):
            osend(i, base + i).wait_recv()
            ofwd(base + i, i).start()

    own_k, pair_k = 2 * c, 2 * (1 - c)

    def groups(half):
        @pl.when(half == 1)
        def _():
            rings.pair_done(2)
            w_store(2, True).start()
            loop(0, 2, lambda i: chunk(2, True, i))
            qkv_store(2).start()
        base = own_k + half * (pair_k - own_k)
        heads_prep(2 * base)

        def one(i):
            attend(base + i)

            @pl.when(half == 0)
            def _():
                @pl.when(i == 0)
                def _():
                    for u in range(3):
                        rings.second(cols_m, u, True)

            @pl.when(half == 1)
            def _():
                for r in range(2):
                    it = 2 * i + r
                    rings.item(cols_m, it // 4, lax.rem(it, 4))
        loop(0, 2, one)
    loop(0, 2, groups)
    rot_store[0].start()
    rot_store[1].start()
    cols_items(4, 8)
    o_forward(own_k)

    @pl.when(y == x)
    def _():
        own_rows.wait()

    @pl.when(y != x)
    def _():
        ref = w.at[1, rings.my_rows]
        remote(ref, ref, scs.at[1], scr, g.partner).wait_recv()
    rings.pair_send(rows_m).start()
    cols_items(8, 12)
    rings.first(rows_m, True)
    o_forward(pair_k)
    rings.pair_done(cols_m)

    def a_part(s, init=False):
        def step(i):
            cols = pl.ds(pl.multiple_of(i * 512, 512), 512)
            acc = None
            for k in range(4):
                dot = jnp.dot(o_full[:, at256(k * 1024 + s * SEG)], w[0, at256(k * 1024 + s * SEG), cols], preferred_element_type=F32)
                acc = dot if acc is None else acc + dot
            a_acc[:, cols] = acc if init else a_acc[:, cols] + acc
        loop(0, 2, step)

    a_part(x, True)
    for k in range(4):
        osend(1 - k % 2, k).wait_recv()
    loop(0, 2, lambda i: a_part(mod4(x + 2 * i - 1)))
    for u in range(3):
        rings.second(rows_m, u, True)
    for k in range(4):
        ofwd(k, k % 2).wait_recv()
    a_part(mod4(x + 2))
    o_oth = x_full
    o_pair = remote(o_full, o_oth, ops, opr, g.partner)
    o_pair.start()
    gy_mine, gy_rest = gyc.at[pl.ds(0, 128)], gyc.at[pl.ds(0, 384)]
    pltpu.make_async_copy(gy_mine, gy_mine, gls).wait()
    remote(gy_rest, gy_rest, gys, gyr, g.partner).wait()

    gpost = gains[2:3, :]
    sq[...] = jnp.zeros((2, 512, 128), F32)

    def a_stats(h):
        cols = at128(h * 128)
        a = a_acc[:, cols].astype(BF16).astype(F32)
        gh = gyc[:, cols].astype(F32) * gains[2:3, cols]
        sq[0] = sq[0] + a * a
        sq[1] = sq[1] + gh * a
    loop(0, 8, a_stats)
    for i in range(2):
        stat2.put(i, sq[i])
    stat2.start()
    rings.round(rows_m, 0)
    total2 = stat2.total()
    inv_a = inv_column(total2, 0)
    mean_a = total2.T[:, 1:2] * inv_a / 4096.0

    def gblk(k, s):
        return ga_all.at[s, :, pl.ds(k * SEG, SEG)]

    def gsend(di, k):
        ref = gblk(k, x)
        return remote(ref, ref, gsd, grv.at[di, k], g.xdev(DIRS[di]))

    def gfwd(k):
        d = DIRS[k % 2]
        ref = gblk(k, mod4(x - d))
        return remote(ref, ref, gfs, gfr.at[k], g.xdev(d))

    theirs = pl.ds(pl.multiple_of((1 - c) * 512, 512), 512)
    mine = pl.ds(pl.multiple_of(c * 512, 512), 512)
    ga_pair = remote(ga_all.at[x, :, theirs], gtw.at[pl.ds(512, 512)], gps, gpr, g.partner)

    for k in range(4):
        cols = pl.ds(k * SEG, SEG)
        a_hat = a_acc[:, cols].astype(BF16).astype(F32) * inv_a
        gyv = gyc[:, cols].astype(F32)
        ga_all[x, :, cols] = (inv_a * (gyv * gpost[:, k * SEG:(k + 1) * SEG] - a_hat * mean_a)).astype(BF16)
        for di in range(2):
            gsend(di, k).start()
    ga_pair.start()
    gtw[0:512] = ga_all[x, :, mine]
    for k in range(4):
        cols = pl.ds(k * SEG, SEG)
        a_hat = a_acc[:, cols].astype(BF16).astype(F32) * inv_a
        xcv[:, cols] = (xcv[:, cols].astype(F32) + a_hat * gpost[:, k * SEG:(k + 1) * SEG]).astype(BF16)
        post[0:1, cols] = jnp.sum(gyc[:, cols].astype(F32) * a_hat, axis=0, keepdims=True)
    y_store.start()
    o_pair.wait_recv()
    ga_pair.wait_recv()

    def slot(kk, t, jj):
        return a_seg.at[kk, jj] if t == 2 else r1.at[kk, t, jj]

    def send1(t, kk, jj):
        src = s0.at[kk, jj] if t == 0 else slot(kk, t - 1, jj)
        return remote(src, slot(kk, t, jj), s1s.at[t], s1r.at[t, jj], g.axis1(1 - 2 * kk))

    def p_store(kk, tt, jj):
        d = 1 - 2 * kk
        rows = g.seg_rows(mod4(p1 - d * (1 + tt)), mod4(p2 - d * (1 + jj)))
        par = lax.rem(jj, 2)
        return pltpu.make_async_copy(stage.at[kk, par], p_out.at[rows, at128(kk * 128)], sgs.at[par])

    def p_wait(par):
        pltpu.make_async_copy(stage.at[pl.ds(0, 2), par], stage.at[pl.ds(0, 2), par], sgs.at[par]).wait()

    def tile(kk, tt, jj):
        d = 1 - 2 * kk
        cols = g.seg_rows(mod4(p1 - d * (1 + tt)), mod4(p2 - d * (1 + jj)))
        right = at256(kk * SEG)
        full = (lax.dot_general(o_full[:, cols], gtw[0:512, right], TN, preferred_element_type=F32)
                + lax.dot_general(o_oth[:, cols], gtw[512:1024, right], TN, preferred_element_type=F32))
        stage[kk, lax.rem(jj, 2)] = full[:, 128:]
        p_store(kk, tt, jj).start()
        return full[:, :128]

    def start_item(jj):
        pl.when(jj >= 2)(lambda: p_wait(lax.rem(jj, 2)))

        def color(kk):
            s0[kk, jj] = tile(kk, 0, jj)
            send1(0, kk, jj).start()
        loop(0, 2, color)

    def ring_item(t, jj):
        p_wait(lax.rem(jj, 2))
        ref = a_seg.at[0, pl.ds(0, 2)]
        remote(ref, ref, s1s.at[t], s1r.at[t, jj], g.partner).wait_recv()

        def color(kk):
            dst = slot(kk, t, jj)
            dst[...] = dst[...] + tile(kk, t + 1, jj)
            if t < 2:
                send1(t + 1, kk, jj).start()
        loop(0, 2, color)

    loop(0, 4, start_item)
    rings.round(rows_m, 1)
    loop(0, 4, lambda jj: ring_item(0, jj))
    rings.round(rows_m, 2)

    def g_forward(lo):
        for k in (lo, lo + 1):
            gsend(k % 2, k).wait_recv()
            gfwd(k).start()

    g_forward(0)
    rings.pair_done(rows_m)
    g_forward(2)

    def go_part(s, init=False):
        def step(zi):
            cols = at256(zi * SEG)
            acc = None
            for k in range(4):
                dot = lax.dot_general(ga_all[s, :, k * SEG:(k + 1) * SEG], w[1, at256(zi * 1024 + k * SEG), at256(s * SEG)],
                                      NT, preferred_element_type=F32)
                acc = dot if acc is None else acc + dot
            a_acc[:, cols] = acc if init else a_acc[:, cols] + acc
        loop(0, 4, step)

    go_part(x, True)
    loop(0, 4, lambda jj: ring_item(1, jj))
    for k in range(4):
        gsend(1 - k % 2, k).wait_recv()
    loop(0, 2, lambda i: go_part(mod4(x + 2 * i - 1)))
    loop(0, 4, lambda jj: ring_item(2, jj))
    a_store.start()
    @pl.when(y == x)
    def _():
        remote(gain_rest, gain_rest, g1s, g1r, g.partner).wait_send()
        for d in (1, 2, 3):
            scatter(d).wait_send()
    for b in range(4):
        if b >= 2:
            xt_pair(b).wait_send()
            xt_store(b).wait()
        xt_pair(b).wait_recv()
    w_store(2, False).wait()
    w_store(2, True).wait()
    qkv_store(2).wait()
    rot_store[0].wait()
    rot_store[1].wait()
    y_store.wait()
    o_pair.wait_send()
    ga_pair.wait_send()
    both = ga_all.at[pl.ds(0, 2)]
    one = ga_all.at[0]
    remote(both, both, osd, opr, g.partner).wait_send()
    remote(both, both, gsd, opr, g.partner).wait_send()
    remote(one, one, ofs, opr, g.partner).wait_send()
    for m in (2, cols_m, rows_m):
        rings.drain(m)
    for k in range(4):
        gfwd(k).wait_recv()
    go_part(mod4(x + 2))
    qkv[0] = a_acc[...].astype(BF16)
    go_store.start()

    a_store.wait()
    remote(one, one, gfs, opr, g.partner).wait_send()
    for t in range(3):
        remote(a_seg, a_seg, s1s.at[t], opr, g.partner).wait_send()
    p_wait(0)
    p_wait(1)
    go_store.wait()


def forward_pass(w_q, w_k, w_v, w_o, x_tok, gy_tok, gq, gk, gp, cos_tab, sin_tab):
    act = SDS((512, 1024), BF16)
    return pl.pallas_call(
        forward_kernel,
        out_shape=[SDS((4096, 1024), BF16)] * 4 + [act] * 6 + [SDS((2, 4, SEG, 128), F32), SDS((4096, SEG), F32), act]
        + [SDS((8, 1024), F32), SDS((8, 512), F32), SDS((1, 1024), F32)],
        in_specs=[IN_HBM] * 6 + [IN_VMEM] * 5,
        out_specs=[IN_HBM] * 13 + [IN_VMEM] * 3,
        scratch_shapes=[
            pltpu.VMEM((3, 4096, 1024), BF16),
            pltpu.VMEM((512, 4096), BF16),
            pltpu.VMEM((2, 1024, 512), BF16),
            pltpu.VMEM((512, 1024), BF16),
            pltpu.VMEM((512, 1024), BF16),
            pltpu.VMEM((3, 512, 1024), BF16),
            pltpu.VMEM((8, 128), F32),
            pltpu.VMEM((512, 1024), F32),
            pltpu.VMEM((512, 4096), BF16),
            pltpu.VMEM((4, 512, 1024), BF16),
            pltpu.VMEM((1024, 512), BF16),
            pltpu.VMEM((2, 512, 128), F32),
            pltpu.VMEM((4, 8, 512), F32),
            pltpu.VMEM((4, 8, 512), F32),
            pltpu.VMEM((2, 2, 4, SEG, 128), F32),
            pltpu.VMEM((2, 4, SEG, 128), F32),
            pltpu.VMEM((2, 4, SEG, 128), F32),
            pltpu.VMEM((2, 2, SEG, 128), F32),
            DMA((4,)), DMA(()), DMA(()), DMA((2, 4)), DMA(()), DMA((4,)),
            DMA(()), DMA(()), DMA(()), DMA((3,)), DMA((3,)), DMA((3,)), DMA((3,)),
            DMA((3, 2)), DMA((4,)), DMA((4,)), DMA((4,)), DMA((8,)),
            DMA(()), DMA(()), DMA(()), DMA(()), DMA(()), DMA(()), pltpu.SemaphoreType.REGULAR,
            DMA((4,)), DMA(()), DMA(()), DMA((2, 4)), DMA(()), DMA((4,)), DMA(()), DMA(()),
            DMA(()), DMA((2, 4)), DMA(()), DMA((4,)), DMA(()), DMA(()),
            DMA((3,)), DMA((3, 4)), DMA((2,)),
        ] + ring_sems(5),
        compiler_params=params(5, 63.5), cost_estimate=COST, name='forward_pass',
    )(w_q, w_k, w_v, w_o, x_tok, gy_tok, gq, gk, gp, cos_tab, sin_tab)


NU = 4
WOA, WOB = 4, 5


def backward_kernel(q0_in, k0_in, v0_in, q_rot_in, k_rot_in, grad_o_in, stats, gains, cos_tab, sin_tab, gy, post, y_in, aseg_in, p_in,
                    x_t, wq, wk, wv,
                    dwv, dwk, dwq, dwo, y_out, gx_part, gx_out, gain_out,
                    r1, r1h, r2, r2h, r2w, s0, aseg, rg, buf, acts, dall, rt, lt, gxc, p_all, ds_all, lanes, st, ge,
                    s1s, s1t, s1r, s2s, s2r, ags, agr, agx, d2s, d2r, fws, fwr, lws, lts, pls, gs, gr, gls, wls, gxs, acs, ass, dps, dpr, sts, strv,
                    ysd, yrv, yst, e1s, e1r, e2s, e2r, e3s, e3r, e4s, e4r):
    outs = (dwv, dwk, dwq, dwq, dwo, dwo)
    widths = (SEG, SEG, 128, 128, 128, 128)
    shifts = (0, 0, 0, 128, 0, 128)
    weights = (wv, wk, wq)
    g = Torus()
    x, z, y, c, p1, p2 = g.x, g.z, g.y, g.c, g.p1, g.p2
    ready = greet([(x, mod4(z + d), y, c) for d in (1, 2, 3)] + [(x, z, mod4(y + d), c) for d in (1, 2, 3)]
                  + [g.partner, g.xdev(2)] + [g.xdev(d, h) for d in DIRS for h in (0, 1)])

    def block(kk, tt, jj):
        d = 1 - 2 * kk
        return g.seg_rows(mod4(p1 - d * (1 + tt)), mod4(p2 - d * (1 + jj)))

    def aload(n, kk):
        par = lax.rem(n, 2)
        return pltpu.make_async_copy(x_t.at[block(kk, 1 + n // 4, lax.rem(n, 4))], lt.at[0, par, kk], lts.at[0, par])

    def bload(jj, kk):
        par = lax.rem(jj, 2)
        return pltpu.make_async_copy(x_t.at[block(kk, 0, jj)], lt.at[1, par, kk], lts.at[1, par])

    def load_wait(kind, par):
        pltpu.make_async_copy(lt.at[kind, par], lt.at[kind, par], lts.at[kind, par]).wait()

    def tile(kind, m, par, kk):
        cols = pl.ds(pl.multiple_of(kk * SEG + shifts[m], 128), widths[m])
        return jnp.dot(lt[kind, par, kk], rt[min(m, 2), :, cols], preferred_element_type=F32)

    def slot(m, kk, t, jj):
        if m == WOA:
            return aseg.at[kk, jj]
        return r1.at[m, kk, t, jj] if m < 2 else r1h.at[0 if m == 2 else 1, kk, t, jj]

    def slot2(m, kk, u):
        return r2.at[m, kk, u] if m < 2 else r2w.at[kk, u] if m == WOA else r2h.at[0 if m == 2 else 1, kk, u]

    def first_slot(m, kk, jj):
        return s0.at[kk, jj, :, pl.ds(shifts[m], widths[m])]

    def send1(m, t, kk, jj, first=False):
        if m == WOB and first:
            src = p_in.at[block(kk, 0, jj), at128(kk * 128)]
        else:
            src = first_slot(m, kk, jj) if first else slot(m, kk, t - 1, jj)
        ss = s1s.at[m, jj] if first and m < 2 else s1t.at[m if m < NU else NU]
        return remote(src, slot(m, kk, t, jj), ss, s1r.at[m if m < NU else NU, t, jj], g.axis1(1 - 2 * kk))

    def recv1(m, t, jj):
        ref = r1.at[0, 0, 0, pl.ds(0, 2)] if m < 2 else r1h.at[0, 0, 0, pl.ds(0, 2)]
        remote(ref, ref, s1t.at[0], s1r.at[m if m < NU else NU, t, jj], g.partner).wait_recv()

    def send2(m, u, kk):
        return remote(slot(m, kk, 2, u), slot2(m, kk, u), s2s.at[m], s2r.at[m, u], g.axis2(DIRS[kk]))

    def start_item(m, jj):
        load_wait(1, lax.rem(jj, 2))
        if m in (1, 2):
            ref = s0.at[0, pl.ds(0, 2)]
            remote(ref, ref, s1s.at[m - 1, jj], s2r.at[0, 0], g.partner).wait_send()

        def color(kk):
            first_slot(m, kk, jj)[...] = tile(1, m, lax.rem(jj, 2), kk)
            send1(m, 0, kk, jj, True).start()
        loop(0, 2, color)
        for kk in range(2):
            pl.when(jj < 2)(lambda: bload(jj + 2, kk).start())
            if m + 1 < NU:
                pl.when(jj >= 2)(lambda: bload(jj - 2, kk).start())

    def ring_item(m, n):
        t, jj = n // 4, lax.rem(n, 4)
        load_wait(0, lax.rem(n, 2))
        recv1(m, t, jj)

        def color(kk):
            ref = slot(m, kk, t, jj)
            ref[...] = ref[...] + tile(0, m, lax.rem(n, 2), kk)
            pl.when(t < 2)(lambda: send1(m, t + 1, kk, jj).start())
        loop(0, 2, color)
        for kk in range(2):
            pl.when(n < 10)(lambda: aload(n + 2, kk).start())
            if m + 1 < NU:
                pl.when(n >= 10)(lambda: aload(n - 10, kk).start())

    def p_block(n, kk):
        i = lax.rem(n, 4)
        return gxc.at[kk, at256(i // 2 * SEG), at128(SEG + lax.rem(i, 2) * 128)]

    def pload(n, kk):
        src = p_in.at[block(kk, 1 + n // 4, lax.rem(n, 4)), at128(kk * 128)]
        return pltpu.make_async_copy(src, p_block(n, kk), pls.at[lax.rem(n, 4)])

    def wo_item(n):
        t, jj = n // 4, lax.rem(n, 4)
        ref = aseg.at[0, pl.ds(0, 2)]
        pltpu.make_async_copy(ref, ref, pls.at[jj]).wait()
        recv1(WOB, t, jj)

        def color(kk):
            dst = slot(WOB, kk, t, jj)
            dst[...] = dst[...] + p_block(n, kk)[...]
            pl.when(t < 2)(lambda: send1(WOB, t + 1, kk, jj).start())
            pl.when(n < 8)(lambda: pload(n + 4, kk).start())
        loop(0, 2, color)

    def out_cols(k, xs, m=0):
        return pl.ds(pl.multiple_of(k * 1024 + xs * SEG + shifts[m], 128), widths[m])

    def ag_send(m, kk, di, h):
        k = 2 * c + kk
        return remote(slot(m, kk, 2, 3).at[pl.ds(h * 128, 128)], outs[m].at[:, out_cols(k, x, m)], ags.at[m],
                      agr.at[m, di] if di == kk else agx.at[m],
                      g.xdev(DIRS[di], h))

    def pair_send(m, kk):
        src = slot(m, kk, 2, 3).at[at128((1 - c) * 128)]
        return remote(src, outs[m].at[:, out_cols(2 * c + kk, x, m)], d2s.at[m], d2r.at[m], g.partner)

    def own_store(m, kk):
        return pltpu.make_async_copy(slot(m, kk, 2, 3).at[at128(c * 128)], outs[m].at[:, out_cols(2 * c + kk, x, m)], lws.at[m])

    def forward(m, k):
        di = k % 2
        ref = outs[m].at[:, out_cols(k, mod4(x - DIRS[di]), m)]
        return remote(ref, ref, fws.at[m], fwr.at[m], g.xdev(DIRS[di]))

    def phase2(m, u):
        if u > 0:
            ref = r2.at[0, 0, pl.ds(0, 2)] if m < 2 else r2w.at[0, pl.ds(0, 2)]
            remote(ref, ref, s2s.at[m], s2r.at[m, u - 1], g.partner).wait_recv()
        for kk in range(2):
            if u > 0:
                ref = slot(m, kk, 2, u)
                ref[...] = ref[...] + slot2(m, kk, u - 1)[...]
            if u < 3:
                send2(m, u, kk).start()
            else:
                own_store(m, kk).start()
                for di in range(2):
                    for h in range(2):
                        ag_send(m, kk, di, h).start()
                pair_send(m, kk).start()

    def do_forward(m):
        for di in range(2):
            ref = outs[m].at[:, pl.ds(0, 2 * widths[m])]
            remote(ref, ref, ags.at[m], agr.at[m, di], g.partner).wait_recv()
            for k in (di, di + 2):
                forward(m, k).start()

    def bytes_of(m, n, ss, rs):
        ref = outs[m].at[:, pl.ds(0, n * widths[m])]
        return remote(ref, ref, ss, rs, g.partner)

    def drain_slots(m):
        if m != WOA:
            ref = r1.at[m, pl.ds(0, 2), pl.ds(0, 2)] if m < 2 else r1h.at[0]
            remote(ref, ref, s1t.at[m if m < NU else NU], d2r.at[m], g.partner).wait_send()
        bytes_of(m, 12, s2s.at[m], d2r.at[m]).wait_send()
        bytes_of(m, 8, ags.at[m], agx.at[m]).wait_send()
        bytes_of(m, 2, d2s.at[m], d2r.at[m]).wait_send()
        ref = outs[m].at[:, pl.ds(0, 2 * widths[m])]
        pltpu.make_async_copy(ref, ref, lws.at[m]).wait()

    def drain_unit(m):
        if m != WOB:
            drain_slots(m)
        bytes_of(m, 4, ags.at[m], agx.at[m]).wait_recv()
        bytes_of(m, 2, d2s.at[m], d2r.at[m]).wait_recv()
        bytes_of(m, 4, fws.at[m], fwr.at[m]).wait()

    def gcols(kk, jj):
        return pl.ds(pl.multiple_of(kk * 2048 + jj * 512, 512), 512)

    def gsend(t, kk, jj):
        d = DIRS[kk]
        if t == 0:
            src = gx_part.at[at128(mod4(x - d) * 128), gcols(kk, jj)]
        else:
            src = rg.at[kk, t - 1, jj]
        return remote(src, rg.at[kk, t, jj], gs, gr.at[t, jj], g.xdev(d))

    def gbuf(t, kk, jj):
        return (t % 2, at128(jj * 128), pl.ds(kk * 512, 512))

    def gload(t, kk, jj):
        src = gx_part.at[at128(mod4(x - DIRS[kk] * (2 + t)) * 128), gcols(kk, jj)]
        return pltpu.make_async_copy(src, buf.at[gbuf(t, kk, jj)], gls.at[t % 2, jj])

    def gloads(t):
        each(lambda kk, jj: gload(t, kk, jj).start())

    def chunk_rows(e):
        return pl.ds(pl.multiple_of((lax.rem(e, 2) * 4 + e // 2) * 512, 512), 512)

    def wload(e, i):
        par = lax.rem(e, 2)
        return pltpu.make_async_copy(weights[i].at[chunk_rows(e)], acts.at[3 * par + i], wls.at[par])

    def gx_store(e):
        par = lax.rem(e, 2)
        return pltpu.make_async_copy(gxc.at[par], gx_part.at[:, chunk_rows(e)], gxs.at[par])

    def gx_ship(e, kk):
        gx_store(e).wait()
        gsend(0, kk, e // 2).start()

    def gx_chunk(e):
        par = lax.rem(e, 2)
        acc = None
        ref = acts.at[pl.ds(0, 3)]
        pltpu.make_async_copy(ref, ref, wls.at[par]).wait()
        for i in range(3):
            dot = lax.dot_general(dall[i], acts[3 * par + i], NT, preferred_element_type=F32)
            acc = dot if acc is None else acc + dot
        gxc[par] = acc
        gx_store(e).start()

        @pl.when(e < 6)
        def _():
            for i in range(3):
                wload(e + 2, i).start()
        for kk in range(2):
            pl.when(jnp.logical_and(e > 0, lax.rem(e, 2) == 1 - kk))(lambda: gx_ship(e - 1, kk))

    def gx_item(t, jj):
        ref = rg.at[0, 0, pl.ds(0, 2)]
        remote(ref, ref, gs, gr.at[t, jj], g.partner).wait_recv()
        pltpu.make_async_copy(ref, ref, gls.at[t % 2, jj]).wait()
        for kk in range(2):
            total = rg[kk, t, jj] + buf[gbuf(t, kk, jj)]
            if t < 2:
                rg[kk, t, jj] = total
                gsend(t + 1, kk, jj).start()
            else:
                gx_out[:, gcols(kk, jj)] = (total + gy[:, gcols(kk, jj)].astype(F32)).astype(BF16)

    def y_send(i, k):
        d = (1, -1, 2)[i]
        src = y_in.at[at128(mod4(x + d) * 128), pl.ds(k * SEG, SEG)]
        return remote(src, y_out.at[:, out_cols(k, x)], ysd, yrv, g.xdev(d))

    def y_own(k):
        return pltpu.make_async_copy(y_in.at[at128(x * 128), pl.ds(k * SEG, SEG)], y_out.at[:, out_cols(k, x)], yst)

    gain1 = remote(ge.at[0], ge.at[1], e1s, e1r, g.partner)

    def gain2(d):
        return remote(ge.at[8], ge.at[1 + d], e2s.at[d - 1], e2r.at[d - 1], (x, mod4(z + d), y, c))

    def gain3(d):
        return remote(ge.at[9], ge.at[4 + d], e3s.at[d - 1], e3r.at[d - 1], (x, z, mod4(y + d), c))

    my_head = at128(z * SEG + c * 128)

    def gain4(d):
        return remote(ge.at[10, :, my_head], gain_out, e4s.at[d - 1], e4r, g.xdev(d))

    def act_load(i):
        return pltpu.make_async_copy((q0_in, k0_in, v0_in, q_rot_in, k_rot_in, grad_o_in)[i], acts.at[i], acs)

    aseg_load = pltpu.make_async_copy(aseg_in, aseg, ass)
    stat = StatExchange(g, st, sts, strv)
    theirs = pl.ds(pl.multiple_of((1 - c) * 512, 512), 512)
    mine = pl.ds(pl.multiple_of(c * 512, 512), 512)

    def swap(i):
        return remote(dall.at[i, :, theirs], rt.at[i, pl.ds(512, 512)], dps.at[i], dpr.at[i], g.partner)

    def share(i):
        rt[i, 0:512] = dall[i, :, mine]
        swap(i).start()

    aseg_load.start()
    for i in (2, 3, 4, 5, 0, 1):
        act_load(i).start()
    for kk in range(2):
        for jj in range(2):
            bload(jj, kk).start()
            aload(jj, kk).start()
    inv = [gxc.at[0, :, pl.ds(i * 128, 128)] for i in range(2)]
    proj = [gxc.at[1, :, pl.ds(i * 128, 128)] for i in range(2)]
    for i in range(2):
        inv[i][...] = jnp.broadcast_to(inv_column(stats[...], i), (512, 128))
    lanes[...] = jnp.zeros((2, 512, 128), F32)
    st[0] = jnp.zeros((8, 512), F32)
    ge[0] = jnp.zeros((8, 1024), F32)
    ge[0, 2:3] = post[...]

    p_all[...] = jnp.zeros((512, 512), BF16)
    ds_all[...] = jnp.zeros((512, 512), BF16)

    def norm_back(i, src_rows, cols, gn):
        hat = acts[i, src_rows, cols].astype(F32) * inv[i][src_rows, :]
        prod = gn * hat
        gain = gains[i:i + 1, cols]
        buf[i, src_rows, cols] = gn * gain
        lanes[i, src_rows] = lanes[i, src_rows] + prod * gain
        return jnp.sum(prod, axis=0, keepdims=True)

    def head(h):
        cols = at128(h * 128)
        vh, qh, kh, do = (acts[i, :, cols] for i in (2, 3, 4, 5))
        gain_q = None
        for i in range(4):
            n = (i + 1) * 128
            rows = pl.ds(i * 128, 128)
            s = causal_scores(qh[i * 128:n], kh[:n], i, n)
            e = jnp.exp(s - jnp.max(s, axis=-1, keepdims=True))
            p = e * (1.0 / jnp.sum(e, axis=-1, keepdims=True))
            dp = lax.dot_general(do[i * 128:n], vh[:n], NT, preferred_element_type=F32)
            ds = (p * (dp - jnp.sum(p * dp, axis=-1, keepdims=True)) * SCALE).astype(BF16)
            p_all[rows, 0:n] = p.astype(BF16)
            ds_all[rows, 0:n] = ds
            dq = jnp.dot(ds, kh[:n], preferred_element_type=F32)
            part = norm_back(0, rows, cols, rope_turn(dq, cos_tab[rows, :], -sin_tab[rows, :]))
            gain_q = part if gain_q is None else gain_q + part
        ge[0, 0:1, cols] = gain_q
        dall[0, :, cols] = lax.dot_general(p_all[...], do, TN, preferred_element_type=F32).astype(BF16)
        dk = lax.dot_general(ds_all[...], qh, TN, preferred_element_type=F32)
        ge[0, 1:2, cols] = norm_back(1, pl.ds(0, 512), cols, rope_turn(dk, cos_tab[...], -sin_tab[...]))

    def finish(i, m, column):
        proj[i][...] = jnp.broadcast_to(column, (512, 128))

        def step(h):
            cols = at128(h * 128)
            scale = inv[i][...]
            hat = acts[i, :, cols].astype(F32) * scale
            dall[m, :, cols] = (scale * (buf[i, :, cols] - hat * proj[i][...])).astype(BF16)
        loop(0, 8, step)

    ready()
    for jj in range(4):
        for kk in range(2):
            send1(WOB, 0, kk, jj, True).start()
            pload(jj, kk).start()
    aseg_load.wait()
    phase2(WOA, 0)
    for k in range(4):
        for i in range(3):
            y_send(i, k).start()
        y_own(k).start()
    pltpu.make_async_copy(acts, acts, acs).wait()

    def head_step(h):
        head(h)
        wo_item(h)
        pl.when(h == 2)(lambda: phase2(WOA, 1))
        pl.when(h == 4)(lambda: phase2(WOA, 2))
    loop(0, 8, head_step)
    share(0)
    for i in range(2):
        stat.put(i, lanes[i])
    stat.start()
    gain1.start()
    phase2(WOA, 3)
    swap(0).wait_recv()

    def begin(n):
        start_item(0, n - 8)
        wo_item(n)
        pl.when(n == 8)(lambda: phase2(WOB, 0))
        pl.when(n == 10)(lambda: phase2(WOB, 1))
    loop(8, 12, begin)
    total = stat.total().T / 4096.0
    finish(1, 1, total[:, 1:2])
    share(1)
    finish(0, 2, total[:, 0:1])
    share(2)
    for e in range(2):
        for i in range(3):
            wload(e, i).start()
    do_forward(WOA)

    for m in range(NU):
        def early(n, m=m):
            ring_item(m, n)
            prev = m - 1 if m > 0 else WOB
            pl.when(n == 0)(lambda: phase2(prev, 2))
            pl.when(n == 2)(lambda: phase2(prev, 3))
            if m == 0:
                gx_chunk(n)
            elif m == 1:
                pl.when(n >= 4)(lambda: gx_item(1, n - 4))

        loop(0, 8, early)
        if m == 0:
            gx_ship(7, 1)
            gloads(0)
            gloads(1)
            do_forward(WOB)
            drain_slots(WOB)
            gain1.wait_recv()
            ge[8] = ge[0] + ge[1]
            for d in (1, 2, 3):
                gain2(d).start()
            swap(1).wait_recv()
            swap(2).wait_recv()
        if m == 1:
            for d in (1, 2, 3):
                gain2(d).wait_recv()
            ge[9] = (ge[8] + ge[2]) + (ge[3] + ge[4])
            for d in (1, 2, 3):
                gain3(d).start()
        if m == 3:
            do_forward(1)
        if m == 2:
            for d in (1, 2, 3):
                gain3(d).wait_recv()
            ge[10] = (ge[9] + ge[5]) + (ge[6] + ge[7])

            @pl.when(y == x)
            def _():
                gain_out[...] = ge[10, :, my_head]
                for d in (1, 2, 3):
                    gain4(d).start()

        def late(n, m=m):
            if m + 1 < NU:
                start_item(m + 1, n - 8)
            ring_item(m, n)
            pl.when(n == 8)(lambda: phase2(m, 0))
            pl.when(n == 10)(lambda: phase2(m, 1))
            if m in (0, 2):
                gx_item(m, n - 8)

        loop(8, 12, late)
        if m == 0:
            gloads(2)
        if m == 1:
            do_forward(0)
        if m == 3:
            do_forward(2)
    for u in (2, 3):
        phase2(NU - 1, u)
    do_forward(NU - 1)

    @pl.when(y == x)
    def _():
        for d in (1, 2, 3):
            gain4(d).wait_send()

    @pl.when(y != x)
    def _():
        gain4(1).wait_recv()
    gain1.wait_send()
    for d in (1, 2, 3):
        gain2(d).wait_send()
        gain3(d).wait_send()
    y_all, y_mine = y_out.at[:, pl.ds(0, 3072)], y_out.at[:, pl.ds(0, 1024)]
    remote(y_all, y_all, ysd, yrv, g.partner).wait()
    pltpu.make_async_copy(y_mine, y_mine, yst).wait()
    for m in range(NU + 2):
        drain_unit(m)
    most = gx_part.at[:, pl.ds(0, 3072)]
    remote(most, most, gs, gr.at[0, 0], g.partner).wait_send()
    for i in range(3):
        swap(i).wait_send()


def backward_pass(q0, k0, v0, q_rot, k_rot, grad_o, stats, gains, cos_tab, sin_tab, gy, post, y_cols, a_seg, p_rest, x_t, w_q, w_k, w_v):
    return pl.pallas_call(
        backward_kernel,
        out_shape=[SDS((128, 4096), F32)] * 4 + [SDS((128, 4096), BF16), SDS((512, 4096), F32), SDS((128, 4096), BF16), SDS((8, 128), F32)],
        in_specs=[IN_HBM] * 6 + [IN_VMEM] * 6 + [IN_HBM] * 7,
        out_specs=[IN_HBM] * 6 + [IN_VMEM] * 2,
        scratch_shapes=[
            pltpu.VMEM((2, 2, 3, 4, SEG, SEG), F32),
            pltpu.VMEM((2, 2, 3, 4, SEG, 128), F32),
            pltpu.VMEM((2, 2, 3, SEG, SEG), F32),
            pltpu.VMEM((2, 2, 3, SEG, 128), F32),
            pltpu.VMEM((2, 3, SEG, 128), F32),
            pltpu.VMEM((2, 4, SEG, SEG), F32),
            pltpu.VMEM((2, 4, SEG, 128), F32),
            pltpu.VMEM((2, 3, 4, 128, 512), F32),
            pltpu.VMEM((2, 512, 1024), F32),
            pltpu.VMEM((6, 512, 1024), BF16),
            pltpu.VMEM((3, 512, 1024), BF16),
            pltpu.VMEM((3, 1024, 512), BF16),
            pltpu.VMEM((2, 2, 2, SEG, 1024), BF16),
            pltpu.VMEM((2, 512, 512), F32),
            pltpu.VMEM((512, 512), BF16),
            pltpu.VMEM((512, 512), BF16),
            pltpu.VMEM((2, 512, 128), F32),
            pltpu.VMEM((4, 8, 512), F32),
            pltpu.VMEM((11, 8, 1024), F32),
            DMA((2, 4)), DMA((NU + 1,)), DMA((NU + 1, 3, 4)), DMA((NU + 2,)), DMA((NU + 2, 3)),
            DMA((NU + 2,)), DMA((NU + 2, 2)), DMA((NU + 2,)), DMA((NU + 2,)), DMA((NU + 2,)), DMA((NU + 2,)), DMA((NU + 2,)), DMA((NU + 2,)),
            DMA((2, 2)), DMA((4,)), DMA(()), DMA((3, 4)), DMA((2, 4)), DMA((2,)), DMA((2,)), DMA(()), DMA(()),
            DMA((3,)), DMA((3,)), DMA((3,)), DMA((3,)),
            DMA(()), DMA(()), DMA(()), DMA(()), DMA(()), DMA((3,)), DMA((3,)), DMA((3,)), DMA((3,)), DMA((3,)), DMA(()),
        ],
        compiler_params=params(7, 63.9), cost_estimate=COST, name='backward_pass',
    )(q0, k0, v0, q_rot, k_rot, grad_o, stats, gains, cos_tab, sin_tab, gy, post, y_cols, a_seg, p_rest, x_t, w_q, w_k, w_v)


def copy_kernel(*refs):
    n = (len(refs) - 7) // 5
    gain_src, gain_dst, gain_buf, gain_sems = refs[n], refs[2 * n + 1:2 * n + 4], refs[3 * n + 4], refs[5 * n + 5:]
    srcs, dsts, bufs = refs[:n], refs[n + 1:2 * n + 1], refs[2 * n + 4:3 * n + 4]
    loads, stores = refs[3 * n + 5:4 * n + 5], refs[4 * n + 5:5 * n + 5]
    parts = 4

    def rows(i, p):
        step = srcs[i].shape[0] // parts
        return pl.ds(p * step, step)

    def load(i, p):
        return pltpu.make_async_copy(srcs[i].at[rows(i, p)], bufs[i].at[rows(i, p)], loads[i].at[p])

    def store(i, p):
        return pltpu.make_async_copy(bufs[i].at[rows(i, p)], dsts[i].at[rows(i, p)], stores[i].at[p])

    gain_load = pltpu.make_async_copy(gain_src, gain_buf, gain_sems[0])
    gain_stores = [pltpu.make_async_copy(gain_buf.at[pl.ds(i, 1)], gain_dst[i], gain_sems[1].at[i]) for i in range(3)]
    order = [(i, p) for i in range(n) for p in range(parts)]
    gain_load.start()
    for i, p in order:
        load(i, p).start()
    gain_load.wait()
    for copy in gain_stores:
        copy.start()
    for i, p in order:
        load(i, p).wait()
        store(i, p).start()
    for i, p in order:
        store(i, p).wait()
    for copy in gain_stores:
        copy.wait()


def copy_out(gains, *arrays):
    n = len(arrays)
    return pl.pallas_call(
        copy_kernel,
        out_shape=[SDS(a.shape, a.dtype) for a in arrays] + [SDS((1, 128), F32)] * 3,
        in_specs=[IN_HBM] * (n + 1),
        out_specs=[IN_HBM] * (n + 3),
        scratch_shapes=[pltpu.VMEM(a.shape, a.dtype) for a in arrays] + [pltpu.VMEM((8, 128), F32)] + [DMA((4,))] * (2 * n) + [DMA(()), DMA((3,))],
        compiler_params=pltpu.CompilerParams(vmem_limit_bytes=63 * 1024 * 1024), cost_estimate=COST, name='copy_out',
    )(*arrays, gains)


def solution(mesh):
    mesh4 = Mesh(mesh.devices.reshape(4, 4, 4, 2), ('sp', 'z', 'y', 'c'))
    tok_spec = P(FS, 'sp', None)
    row_spec = P(FS, None)
    vec_spec = P(FS)

    def local_step(x, grad_y, wq_rows, wk_rows, wv_rows, wo_rows, gq_rows, gk_rows, gpost_rows):
        x_tok, gy_tok = x[0], grad_y[0]
        cos_tab, sin_tab = rope_tables(4 * x_tok.shape[0])
        w_q, w_k, w_v, x_t, q0, k0, v0, q_rot, k_rot, y_cols, a_seg, p_rest, grad_o, gains, stats, post = forward_pass(
            wq_rows, wk_rows, wv_rows, wo_rows, x_tok, gy_tok, gq_rows[None], gk_rows[None], gpost_rows[None], cos_tab, sin_tab)
        dwv, dwk, dwq, dwo, y, _, grad_x, gn = backward_pass(
            q0, k0, v0, q_rot, k_rot, grad_o, stats, gains, cos_tab, sin_tab, gy_tok, post, y_cols, a_seg, p_rest, x_t, w_q, w_k, w_v)
        dwv, dwk, dwq, dwo, y, grad_x, *gn = copy_out(gn, dwv, dwk, dwq, dwo, y, grad_x)
        return y[None], grad_x[None], dwq, dwk, dwv, dwo, gn[0][0], gn[1][0], gn[2][0]

    return jax.shard_map(local_step, mesh=mesh4,
                         in_specs=(tok_spec, tok_spec, row_spec, row_spec, row_spec, row_spec, vec_spec, vec_spec, vec_spec),
                         out_specs=(tok_spec, tok_spec, row_spec, row_spec, row_spec, row_spec, vec_spec, vec_spec, vec_spec),
                         check_vma=False)
```

```python
import jax
import jax.numpy as jnp
import numpy as np
from jax import lax
from jax.experimental import pallas as pl
from jax.experimental.pallas import tpu as pltpu
from jax.sharding import Mesh, PartitionSpec as P

HEAD_DIM = 128
RMS_EPSILON = 1e-6
ROPE_THETA = 500000.0
FS = ('z', 'y', 'c')
F32 = jnp.float32
BF16 = jnp.bfloat16
MESH_ID = pl.DeviceIdType.MESH
HBM = pl.ANY
SEG = 256


def rope_tables(seq_len):
    half_dim = HEAD_DIM // 2
    angles = np.arange(seq_len)[:, None] * ROPE_THETA ** (-np.arange(half_dim) * (2.0 / HEAD_DIM))[None, :]
    cos_half, sin_half = np.cos(angles), np.sin(angles)
    tables = np.concatenate([cos_half, cos_half], axis=1), np.concatenate([-sin_half, sin_half], axis=1)
    return tuple(jnp.asarray(t, F32) for t in tables)


def coords():
    return tuple(lax.axis_index(n) for n in ('sp', 'z', 'y', 'c'))


def mod4(v):
    return lax.rem(v + 8, 4)


def remote(src, dst, ss, rs, dev):
    return pltpu.make_async_remote_copy(src_ref=src, dst_ref=dst, send_sem=ss, recv_sem=rs, device_id=dev, device_id_type=MESH_ID)


def at256(v):
    return pl.ds(pl.multiple_of(v, SEG), SEG)


def at128(v):
    return pl.ds(pl.multiple_of(v, 128), 128)


def each(fn, n=4):
    def step(jj, carry):
        for kk in range(2):
            fn(kk, jj)
        return carry
    lax.fori_loop(0, n, step, 0)


def loop(lo, hi, fn):
    def step(n, carry):
        fn(n)
        return carry
    lax.fori_loop(lo, hi, step, 0)


def greet(peers):
    barrier = pltpu.get_barrier_semaphore()
    for peer in peers:
        pl.semaphore_signal(barrier, inc=1, device_id=peer, device_id_type=MESH_ID)
    return lambda: pl.semaphore_wait(barrier, len(peers))


class Torus:
    def __init__(self):
        self.x, self.z, self.y, self.c = x, z, y, c = coords()
        self.p1 = (1 - c) * y + c * z
        self.p2 = (1 - c) * z + c * y
        self.partner = (x, z, y, 1 - c)

    def axis1(self, d):
        return (self.x, mod4(self.z + d * self.c), mod4(self.y + d * (1 - self.c)), self.c)

    def axis2(self, d):
        return (self.x, mod4(self.z + d * (1 - self.c)), mod4(self.y + d * self.c), self.c)

    def xdev(self, d, core=None):
        return (mod4(self.x + d), self.z, self.y, self.c if core is None else core)

    def seg_rows(self, b, j):
        zz = (1 - self.c) * j + self.c * b
        yy = (1 - self.c) * b + self.c * j
        return at256(zz * 1024 + yy * SEG)


DIRS = (1, -1)
RING_SEMS = 8


def ring_sems(nw):
    dma = pltpu.SemaphoreType.DMA
    return [dma((nw,)), dma((nw,)), dma((nw,)), dma((nw, 3)), dma((nw,)), dma((nw, 3, 4)), dma((nw,)), dma((nw,))]


class WeightRings:
    def __init__(self, g, w, slots, sems):
        self.g, self.w, self.slots = g, w, slots
        self.d0s, self.d0r, self.a1s, self.a1r, self.a2s, self.a2r, self.f3s, self.f3r = sems
        self.my_rows = at128(g.z * 1024 + g.y * SEG + g.c * 128)

    def pair_send(self, m):
        ref = self.w.at[self.slots[m], self.my_rows]
        return remote(ref, ref, self.d0s.at[self.slots[m]], self.d0r.at[self.slots[m]], self.g.partner)

    def same(self, m, kk, rows, ss, rs, dev):
        ref = self.w.at[self.slots[m], rows, at256((2 * self.g.c + kk) * SEG)]
        return remote(ref, ref, ss, rs, dev)

    def bulk(self, m, n, ss, rs):
        ref = self.w.at[self.slots[m], pl.ds(0, n * 128), pl.ds(0, 512)]
        return remote(ref, ref, ss, rs, self.g.partner)

    def send1(self, m, u, kk):
        g, d = self.g, DIRS[kk]
        return self.same(m, kk, g.seg_rows(g.p1, mod4(g.p2 - d * u)), self.a1s.at[self.slots[m]], self.a1r.at[self.slots[m], u], g.axis2(d))

    def far1(self, m, e, kk):
        g = self.g
        rows = g.seg_rows(g.p1, g.p2)
        return self.same(m, kk, rows, self.a1s.at[self.slots[m]], self.a1r.at[self.slots[m], e - 1], g.axis2(DIRS[kk] * e))

    def fwd1(self, m, u, kk):
        g = self.g
        rows = g.seg_rows(g.p1, mod4(g.p2 - DIRS[kk] * (u + 1)))
        return self.same(m, kk, rows, self.f3s.at[self.slots[m]], self.f3r.at[self.slots[m]], g.partner)

    def send2(self, m, t, kk, jj):
        g, d = self.g, DIRS[kk]
        rows = g.seg_rows(mod4(g.p1 - d * t), mod4(g.p2 - d * jj))
        return self.same(m, kk, rows, self.a2s.at[self.slots[m]], self.a2r.at[self.slots[m], t, jj], g.axis1(d))

    def fwd2(self, m, t, kk, jj):
        g, d = self.g, DIRS[kk]
        rows = g.seg_rows(mod4(g.p1 - d * (t + 1)), mod4(g.p2 - d * jj))
        return self.same(m, kk, rows, self.f3s.at[self.slots[m]], self.f3r.at[self.slots[m]], g.partner)

    def first(self, m, far=False):
        self.pair_send(m).wait_recv()
        for kk in range(2):
            if far:
                for e in (1, 2, 3):
                    self.far1(m, e, kk).start()
            else:
                self.send1(m, 0, kk).start()
            self.send2(m, 0, kk, 0).start()

    def second(self, m, u, far=False):
        self.bulk(m, 2, self.a1s.at[self.slots[m]], self.a1r.at[self.slots[m], u]).wait_recv()
        for kk in range(2):
            if u < 2 and not far:
                self.send1(m, u + 1, kk).start()
            self.send2(m, 0, kk, u + 1).start()
            self.fwd1(m, u, kk).start()

    def item(self, m, t, jj):
        self.bulk(m, 2, self.a2s.at[self.slots[m]], self.a2r.at[self.slots[m], t, jj]).wait_recv()

        def pass_on():
            for kk in range(2):
                self.send2(m, t + 1, kk, jj).start()
        if isinstance(t, int):
            if t < 2:
                pass_on()
        else:
            pl.when(t < 2)(pass_on)
        for kk in range(2):
            self.fwd2(m, t, kk, jj).start()

    def round(self, m, t, extra=None):
        def step(jj):
            self.item(m, t, jj)
            if extra is not None:
                extra(jj)
        loop(0, 4, step)

    def pair_done(self, m):
        self.bulk(m, 30, self.f3s.at[self.slots[m]], self.f3r.at[self.slots[m]]).wait_recv()

    def drain(self, m):
        self.pair_send(m).wait_send()
        for sems, n in ((self.a1s, 6), (self.a2s, 24), (self.f3s, 30)):
            self.bulk(m, n, sems.at[self.slots[m]], self.f3r.at[self.slots[m]]).wait_send()


class StatExchange:
    def __init__(self, g, st, ss, rs):
        self.g, self.st, self.ss, self.rs = g, st, ss, rs

    def copy(self, i):
        return remote(self.st.at[0], self.st.at[1 + i], self.ss.at[i], self.rs.at[i], self.g.xdev((1, -1, 2)[i]))

    def put(self, i, lanes):
        self.st[0, i:i + 1] = jnp.sum(lanes.T, axis=0, keepdims=True)

    def start(self):
        for i in range(3):
            self.copy(i).start()

    def total(self):
        for i in range(3):
            self.copy(i).wait()
        return (self.st[0] + self.st[1]) + (self.st[2] + self.st[3])


def params(cid, vmem_mib=60.0):
    return pltpu.CompilerParams(collective_id=cid, has_side_effects=True, vmem_limit_bytes=int(vmem_mib * 1024 * 1024))


COST = pl.CostEstimate(flops=10 ** 11, bytes_accessed=10 ** 8, transcendentals=0)
DMA = pltpu.SemaphoreType.DMA
IN_VMEM = pl.BlockSpec(memory_space=pltpu.VMEM)
IN_HBM = pl.BlockSpec(memory_space=pl.ANY)
SDS = jax.ShapeDtypeStruct


SCALE = HEAD_DIM ** -0.5
TN = (((0,), (0,)), ((), ()))
NT = (((1,), (1,)), ((), ()))
W_SLOTS = (0, 1, 2, 0, 1)


def rope_turn(u, cos_tab, sin_tab):
    return u * cos_tab + pltpu.roll(u, 64, 1) * sin_tab


def causal_scores(keys, q_blk, i, n):
    s = lax.dot_general(keys, q_blk, NT, preferred_element_type=F32) * SCALE
    query = lax.broadcasted_iota(jnp.int32, (n, 128), 1) + i * 128
    return jnp.where(query >= lax.broadcasted_iota(jnp.int32, (n, 128), 0), s, -1e30)


def inv_column(total, i):
    return lax.rsqrt(total.T[:, i:i + 1] / 4096.0 + RMS_EPSILON)


def forward_phase(io, keep, w, x_full, xt, gyc, xcv, gains_in, a_acc, o_full, ga_all, gtw, sq, st, st2, r1, p_all, tmp,
            ld, xls, xs, xr, xfs, xfr, gls, gys, gyr, sts, strv, sts2, strv2, wos, xps, xpr, xst, yst,
            g1s, g1r, g2s, g2r, g3s, g3r, free,
            scl, sc1s, sc1r, sc2s, sc2r, osd, orv, ofs, ofr, ops, opr, gsd, grv, gfs, gfr, gps, gpr, s1s, s1r, *ring):
    (wq_in, wk_in, wv_in, wo_in, x_in, gy_in, gq_in, gk_in, gp_in, cos_tab, sin_tab, wq_out, wk_out, wv_out, x_t, y_cols) = io
    acts, gains, stats, post, wo_seg, wo_add, wor = keep
    s0 = wo_add
    w_in, w_out = (wq_in, wk_in, wv_in, wo_in), (wq_out, wk_out, wv_out)
    nw = 3
    cols_m, rows_m = 3, 4
    g = Torus()
    x, z, y, c, p1, p2 = g.x, g.z, g.y, g.c, g.p1, g.p2
    rings = WeightRings(g, w, W_SLOTS, ring)
    plane = [(x, mod4(z + d), y, c) for d in (1, 2, 3)] + [(x, z, mod4(y + d), c) for d in (1, 2, 3)] + [g.partner]
    everyone = plane + [g.xdev(1), g.xdev(-1), g.xdev(2)]
    ready = greet(everyone)

    def load(m, k):
        src = w_in[m].at[:, at256(k * 1024 + x * SEG)]
        return pltpu.make_async_copy(src, w.at[W_SLOTS[m], rings.my_rows, pl.ds(k * SEG, SEG)], ld.at[m])

    def rows_y(d):
        to = mod4(y + d)
        return remote(wo_in.at[:, at256(to * 1024 + x * SEG)], tmp.at[y], sc1s, sc1r, (x, z, to, c))

    def rows_x(d):
        return remote(tmp.at[mod4(x + d)], w.at[1, rings.my_rows, at256(x * SEG)], sc2s, sc2r, g.xdev(d))

    tmp_own = pltpu.make_async_copy(wo_in.at[:, at256(y * 1024 + x * SEG)], tmp.at[y], scl)
    tmp3 = tmp.at[pl.ds(0, 3)]

    def load_wait(m):
        ref = w.at[W_SLOTS[m], rings.my_rows]
        pltpu.make_async_copy(ref, ref, ld.at[m]).wait()

    def xseg(b, s):
        return x_full.at[at128(b * 128), pl.ds(s * 1024, 1024)]

    x_own = pltpu.make_async_copy(x_in, x_full.at[at128(x * 128)], xls)

    def xsend(di, s):
        ref = xseg(x, s)
        return remote(ref, ref, xs, xr.at[di, s], g.xdev(DIRS[di]))

    def xfwd(s):
        d = DIRS[s // 2]
        ref = xseg(mod4(x - d), s)
        return remote(ref, ref, xfs, xfr.at[s], g.xdev(d))

    gy_rows = at128(x * 128)

    def gy_own(k):
        return pltpu.make_async_copy(gy_in.at[:, at256(k * 1024 + x * SEG)], gyc.at[gy_rows, pl.ds(k * SEG, SEG)], gls)

    def gy_send(i, k):
        d = (1, -1, 2)[i]
        src = gy_in.at[:, at256(k * 1024 + mod4(x + d) * SEG)]
        return remote(src, gyc.at[gy_rows, pl.ds(k * SEG, SEG)], gys, gyr, g.xdev(d))

    def gblock(zh, ch):
        return gains.at[:, at128(zh * SEG + ch * 128)]

    def gain1(d):
        return remote(gains_in, gblock(z, c), g1s, g1r, (x, z, mod4(y + d), c))

    def gain2(d):
        ref = gblock(z, c)
        return remote(ref, ref, g2s, g2r, (x, mod4(z + d), y, c))

    def gain3(zh):
        ref = gblock(zh, c)
        return remote(ref, ref, g3s, g3r, g.partner)

    stat = StatExchange(g, st, sts, strv)
    stat2 = StatExchange(g, st2, sts2, strv2)

    def xt_pair(b):
        return remote(xt.at[lax.rem(b, 2)], x_t.at[pl.ds(pl.multiple_of(b * 1024, 1024), 1024), pl.ds(512, 512)], xps.at[b], xpr.at[b], g.partner)

    def xt_store(b):
        return pltpu.make_async_copy(xt.at[lax.rem(b, 2)], x_t.at[pl.ds(pl.multiple_of(b * 1024, 1024), 1024), pl.ds(0, 512)], xst.at[b])

    def turn(b):
        @pl.when(b >= 2)
        def _():
            xt_pair(b - 2).wait_send()
            xt_store(b - 2).wait()

        def step(i):
            xt[lax.rem(b, 2), at256(i * SEG), :] = x_full[:, at256(b * 1024 + i * SEG)].T
        loop(0, 4, step)
        xt_pair(b).start()
        xt_store(b).start()

    def w_store(m, theirs):
        cols = pl.ds(pl.multiple_of(((1 - c) if theirs else c) * 512, 512), 512)
        return pltpu.make_async_copy(w.at[m, :, cols], w_out[m].at[:, cols], wos.at[m, int(theirs)])

    y_store = pltpu.make_async_copy(xcv, y_cols, yst)

    st[0] = jnp.zeros((8, 512), F32)
    st2[0] = jnp.zeros((8, 512), F32)
    p_all[...] = jnp.zeros((512, 512), BF16)
    sq[...] = jnp.zeros((2, 512, 128), F32)
    gains_in[...] = jnp.concatenate([gq_in[...], gk_in[...], gp_in[...], jnp.zeros((5, 128), F32)], axis=0)
    for k in range(4):
        load(0, k).start()
    x_own.start()
    for m in range(1, nw):
        for k in range(4):
            load(m, k).start()
    for k in range(4):
        gy_own(k).start()
    ready()
    for m in range(nw):
        load_wait(m)
        rings.pair_send(m).start()
        if m == 0:
            x_own.wait()
            for s in range(4):
                for di in range(2):
                    xsend(di, (s + 2 * di) % 4).start()

    @pl.when(y == x)
    def _():
        gains[:, at128(z * SEG + c * 128)] = gains_in[...]
        for d in (1, 2, 3):
            gain1(d).start()

    def chunk(m, theirs, i):
        cols = at256((2 * ((1 - c) if theirs else c) + i) * SEG)
        acc_ref = a_acc.at[:, pl.ds(0, SEG)]

        def accumulate(kc):
            rows = pl.ds(pl.multiple_of(kc * 2048, 2048), 2048)
            acc_ref[...] = acc_ref[...] + jnp.dot(x_full[:, rows], w[m, rows, cols], preferred_element_type=F32)
        acc_ref[...] = jnp.zeros((512, SEG), F32)
        loop(0, 2, accumulate)
        acc = acc_ref[...].astype(BF16)
        acts[m, :, cols] = acc
        if m < 2:
            sqv = acc.astype(F32)
            sqv = sqv * sqv
            sq[m] = sq[m] + (sqv[:, :128] + sqv[:, 128:])

    def chunk_beside(m, theirs):
        return lambda jj: pl.when(lax.rem(jj, 2) == 1)(lambda: chunk(m, theirs, jj // 2))

    rings.first(0, True)
    rings.first(1)
    for u in range(3):
        rings.second(0, u, True)

    def beside(m, t):
        if (m, t) == (1, 1):
            own = chunk_beside(0, False)

            def both(jj):
                turn(jj)
                own(jj)
            return both
        return {(1, 2): chunk_beside(0, True), (2, 0): chunk_beside(1, False), (2, 1): chunk_beside(1, True)}.get((m, t))

    for m in range(nw):
        for t in range(3):
            if (m, t) == (2, 1):
                rings.pair_done(1)
                w_store(1, True).start()
            rings.round(m, t, beside(m, t))
            if m + 1 < nw:
                rings.second(m + 1, t)
            if (m, t) == (0, 0):
                @pl.when(y != x)
                def _():
                    remote(gains_in, gblock(z, c), g1s, g1r, g.partner).wait_recv()
                for d in (1, 2, 3):
                    gain2(d).start()
            if (m, t) == (0, 1):
                rings.first(2)
                for s in range(4):
                    xsend(s // 2, s).wait_recv()
                    xfwd(s).start()
                for k in range(4):
                    for i in range(3):
                        gy_send(i, k).start()
            if (m, t) == (0, 2):
                w_store(0, False).start()
                gain_rest = gains.at[:, pl.ds(0, 384)]
                remote(gain_rest, gain_rest, g2s, g2r, g.partner).wait()
                for zh in range(4):
                    gain3(zh).start()
            if (m, t) == (1, 0):
                rings.pair_done(0)
                w_store(0, True).start()
                for s in range(4):
                    xsend(1 - s // 2, s).wait_recv()
                    xfwd(s).wait_recv()
            if (m, t) == (1, 2):
                w_store(1, False).start()
                for k in range(4):
                    xcv[:, pl.ds(k * SEG, SEG)] = x_full[:, at256(k * 1024 + x * SEG)]
                rings.drain(0)
                w_store(0, False).wait()
                w_store(0, True).wait()
                for k in range(4):
                    load(cols_m, k).start()
            if (m, t) == (2, 1):
                for i in range(2):
                    stat.put(i, sq[i])
                stat.start()
                rings.drain(1)
                w_store(1, False).wait()
                w_store(1, True).wait()
                half_x, quarter_x = x_full.at[:, pl.ds(0, 2048)], x_full.at[:, pl.ds(0, 1024)]
                remote(half_x, half_x, xs, xr.at[0, 0], g.partner).wait_send()
                remote(quarter_x, quarter_x, xfs, xr.at[0, 0], g.partner).wait_send()
                tmp_own.start()
                for d in (1, 2, 3):
                    rows_y(d).start()
                for peer in everyone:
                    pl.semaphore_signal(free, inc=1, device_id=peer, device_id_type=MESH_ID)

    load_wait(cols_m)
    pl.semaphore_wait(free, len(everyone))
    rings.pair_send(cols_m).start()

    remote(tmp3, tmp3, sc1s, sc1r, g.partner).wait_recv()
    tmp_own.wait()
    for d in (1, -1, 2):
        rows_x(d).start()
    w[1, rings.my_rows, at256(x * SEG)] = tmp[x]
    w_store(2, False).start()
    total = stat.total()
    stats[...] = total
    inv_q, inv_k = inv_column(total, 0), inv_column(total, 1)
    loop(0, 2, lambda i: chunk(2, False, i))
    rings.first(cols_m, True)
    gain_half = gains.at[:, pl.ds(0, 512)]
    remote(gain_half, gain_half, g3s, g3r, g.partner).wait()

    def heads_prep(base):
        def step(i):
            cols = at128((base + i) * 128)
            for j, inv in ((0, inv_q), (1, inv_k)):
                u = acts[j, :, cols].astype(F32) * inv * gains[j:j + 1, cols]
                acts[3 + j, :, cols] = rope_turn(u, cos_tab[...], sin_tab[...]).astype(BF16)
        loop(0, 4, step)

    def oblk(k, s):
        return o_full.at[:, at256(k * 1024 + s * SEG)]

    def osend(di, k):
        ref = oblk(k, x)
        return remote(ref, ref, osd, orv.at[di, k], g.xdev(DIRS[di]))

    def ofwd(k, di):
        d = DIRS[di]
        ref = oblk(k, mod4(x - d))
        return remote(ref, ref, ofs, ofr.at[k], g.xdev(d))

    def attend(k):
        for ch in range(2):
            cols = at128(k * SEG + ch * 128)
            qh, kh, vh = acts[3, :, cols], acts[4, :, cols], acts[2, :, cols]
            for i in range(4):
                n = (i + 1) * 128
                s = causal_scores(kh[:n], qh[i * 128:n], i, n)
                e = jnp.exp(s - jnp.max(s, axis=0, keepdims=True))
                p_all[0:n, pl.ds(i * 128, 128)] = (e * (1.0 / jnp.sum(e, axis=0, keepdims=True))).astype(BF16)
            o = lax.dot_general(p_all[...], vh, TN, preferred_element_type=F32).astype(BF16)
            o_full[:, at128(k * 1024 + x * SEG + ch * 128)] = o
        for di in range(2):
            osend(di, k).start()

    def o_pair(s):
        for k in range(4):
            cols = at256(k * 1024 + s * SEG)
            remote(o_full.at[:, cols], x_full.at[:, cols], ops, opr, g.partner).start()

    def cols_items(lo, hi):
        loop(lo, hi, lambda it: rings.item(cols_m, it // 4, lax.rem(it, 4)))

    def o_forward(base):
        for i in range(2):
            osend(i, base + i).wait_recv()
            ofwd(base + i, i).start()

    own_k, pair_k = 2 * c, 2 * (1 - c)

    rest = w.at[1, rings.my_rows, pl.ds(0, 768)]

    def groups(half):
        @pl.when(half == 1)
        def _():
            remote(rest, rest, sc2s, sc2r, g.partner).wait_recv()
            rings.pair_send(rows_m).start()
            rings.pair_done(2)
            w_store(2, True).start()
            loop(0, 2, lambda i: chunk(2, True, i))
            rings.first(rows_m, True)
        base = own_k + half * (pair_k - own_k)
        heads_prep(2 * base)

        def one(i):
            attend(base + i)

            @pl.when(half == 0)
            def _():
                @pl.when(i == 0)
                def _():
                    for u in range(3):
                        rings.second(cols_m, u, True)

            @pl.when(half == 1)
            def _():
                for r in range(2):
                    it = 2 * i + r
                    rings.item(cols_m, it // 4, lax.rem(it, 4))
        loop(0, 2, one)
    loop(0, 2, groups)
    cols_items(4, 8)
    o_forward(own_k)

    for u in range(3):
        rings.second(rows_m, u, True)
    cols_items(8, 12)
    o_forward(pair_k)
    rings.pair_done(cols_m)
    o_pair(x)

    def a_part(s, init=False):
        def step(i):
            cols = at256(i * SEG)
            acc = None
            for k in range(4):
                dot = jnp.dot(o_full[:, at256(k * 1024 + s * SEG)], w[0, at256(k * 1024 + s * SEG), cols], preferred_element_type=F32)
                acc = dot if acc is None else acc + dot
            a_acc[:, cols] = acc if init else a_acc[:, cols] + acc
        loop(0, 4, step)

    a_part(x, True)
    for k in range(4):
        osend(1 - k % 2, k).wait_recv()
    o_pair(mod4(x + 1))
    o_pair(mod4(x + 3))
    loop(0, 2, lambda i: a_part(mod4(x + 2 * i - 1)))
    rings.round(rows_m, 0)
    for k in range(4):
        ofwd(k, k % 2).wait_recv()
    a_part(mod4(x + 2))
    o_oth = x_full
    gy_mine, gy_rest = gyc.at[pl.ds(0, 128)], gyc.at[pl.ds(0, 384)]
    pltpu.make_async_copy(gy_mine, gy_mine, gls).wait()
    remote(gy_rest, gy_rest, gys, gyr, g.partner).wait()

    sq[...] = jnp.zeros((2, 512, 128), F32)

    def a_stats(h):
        cols = at128(h * 128)
        a = a_acc[:, cols].astype(BF16).astype(F32)
        gh = gyc[:, cols].astype(F32) * gains[2:3, cols]
        sq[0] = sq[0] + a * a
        sq[1] = sq[1] + gh * a
    loop(0, 8, a_stats)
    for i in range(2):
        stat2.put(i, sq[i])
    stat2.start()
    rings.round(rows_m, 1)
    total2 = stat2.total()
    inv_a = inv_column(total2, 0)
    sq[0] = jnp.broadcast_to(inv_a, (512, 128))
    sq[1] = jnp.broadcast_to(total2.T[:, 1:2] * inv_a / 4096.0, (512, 128))

    def gblk(k, s):
        return ga_all.at[s, :, pl.ds(k * SEG, SEG)]

    def gsend(di, k):
        ref = gblk(k, x)
        return remote(ref, ref, gsd, grv.at[di, k], g.xdev(DIRS[di]))

    def gsend_start(di, k):
        for i in range(4):
            ref = ga_all.at[x, pl.ds(i * 128, 128), at256(k * SEG)]
            remote(ref, ref, gsd, grv.at[di, k], g.xdev(DIRS[di])).start()

    def gfwd(k):
        d = DIRS[k % 2]
        ref = gblk(k, mod4(x - d))
        return remote(ref, ref, gfs, gfr.at[k], g.xdev(d))

    theirs = pl.ds(pl.multiple_of((1 - c) * 512, 512), 512)
    mine = pl.ds(pl.multiple_of(c * 512, 512), 512)
    ga_pair = remote(ga_all.at[x, :, theirs], gtw.at[pl.ds(512, 512)], gps, gpr, g.partner)

    def send_grad_a(k):
        def step(i):
            cols = at128(k * SEG + i * 128)
            scale = sq[0]
            a_hat = a_acc[:, cols].astype(BF16).astype(F32) * scale
            ga_all[x, :, cols] = (scale * (gyc[:, cols].astype(F32) * gains[2:3, cols] - a_hat * sq[1])).astype(BF16)
        loop(0, 2, step)
        for di in range(2):
            gsend_start(di, k)
    loop(0, 4, send_grad_a)
    ga_pair.start()
    o_pair(mod4(x + 2))
    gtw[0:512] = ga_all[x, :, mine]
    def finish_y(h):
        cols = at128(h * 128)
        a_hat = a_acc[:, cols].astype(BF16).astype(F32) * sq[0]
        xcv[:, cols] = (xcv[:, cols].astype(F32) + a_hat * gains[2:3, cols]).astype(BF16)
        post[0:1, cols] = jnp.sum(gyc[:, cols].astype(F32) * a_hat, axis=0, keepdims=True)
    loop(0, 8, finish_y)
    y_store.start()
    rings.round(rows_m, 2)
    remote(o_full, o_oth, ops, opr, g.partner).wait_recv()
    ga_pair.wait_recv()

    def slot(kk, t, jj):
        return wo_seg.at[kk, jj] if t == 2 else r1.at[kk, t, jj]

    def send1(t, kk, jj):
        src = s0.at[kk, jj] if t == 0 else r1.at[kk, t - 1, jj]
        rs = wor.at[jj] if t == 2 else s1r.at[t, jj]
        return remote(src, slot(kk, t, jj), s1s.at[t], rs, g.axis1(1 - 2 * kk))

    def tile(kk, tt, jj):
        d = 1 - 2 * kk
        cols = g.seg_rows(mod4(p1 - d * (1 + tt)), mod4(p2 - d * (1 + jj)))
        right = at256(kk * SEG)
        return (lax.dot_general(o_full[:, cols], gtw[0:512, right], TN, preferred_element_type=F32)
                + lax.dot_general(o_oth[:, cols], gtw[512:1024, right], TN, preferred_element_type=F32))

    def start_item(jj):
        def color(kk):
            s0[kk, jj] = tile(kk, 0, jj)
            send1(0, kk, jj).start()
        loop(0, 2, color)

    def ring_item(t, jj):
        ref = s0.at[0, pl.ds(0, 2)]
        remote(ref, ref, s1s.at[t], s1r.at[t, jj], g.partner).wait_recv()

        def color(kk):
            dst = r1.at[kk, t, jj]
            dst[...] = dst[...] + tile(kk, t + 1, jj)
            send1(t + 1, kk, jj).start()
        loop(0, 2, color)

    def last_tiles(jj):
        def color(kk):
            wo_add[kk, jj] = tile(kk, 3, jj)
        loop(0, 2, color)

    def g_forward(lo):
        for k in (lo, lo + 1):
            gsend(k % 2, k).wait_recv()
            gfwd(k).start()

    loop(0, 4, start_item)
    g_forward(0)
    loop(0, 2, lambda jj: ring_item(0, jj))
    g_forward(2)
    loop(2, 4, lambda jj: ring_item(0, jj))
    rings.pair_done(rows_m)

    def go_part(s, init=False):
        def step(zi):
            cols = at256(zi * SEG)
            acc = None
            for k in range(4):
                dot = lax.dot_general(ga_all[s, :, k * SEG:(k + 1) * SEG], w[1, at256(zi * 1024 + k * SEG), at256(s * SEG)],
                                      NT, preferred_element_type=F32)
                acc = dot if acc is None else acc + dot
            a_acc[:, cols] = acc if init else a_acc[:, cols] + acc
        loop(0, 4, step)

    go_part(x, True)
    loop(0, 4, lambda jj: ring_item(1, jj))
    for k in range(4):
        gsend(1 - k % 2, k).wait_recv()
    loop(0, 2, lambda i: go_part(mod4(x + 2 * i - 1)))
    remote(s0, s0, s1s.at[0], opr, g.partner).wait_send()
    loop(0, 4, last_tiles)
    @pl.when(y == x)
    def _():
        remote(gain_rest, gain_rest, g1s, g1r, g.partner).wait_send()
    remote(tmp3, tmp3, sc1s, sc1r, g.partner).wait_send()
    remote(rest, rest, sc2s, sc2r, g.partner).wait_send()
    for b in range(4):
        if b >= 2:
            xt_pair(b).wait_send()
            xt_store(b).wait()
        xt_pair(b).wait_recv()
    w_store(2, False).wait()
    w_store(2, True).wait()
    y_store.wait()
    remote(o_full, o_oth, ops, opr, g.partner).wait_send()
    ga_pair.wait_send()
    both = ga_all.at[pl.ds(0, 2)]
    one = ga_all.at[0]
    remote(both, both, osd, opr, g.partner).wait_send()
    remote(both, both, gsd, opr, g.partner).wait_send()
    remote(one, one, ofs, opr, g.partner).wait_send()
    for m in (2, cols_m, rows_m):
        rings.drain(m)
    for k in range(4):
        gfwd(k).wait_recv()
    go_part(mod4(x + 2))

    def keep_grad_o(h):
        cols = at128(h * 128)
        acts[5, :, cols] = a_acc[:, cols].astype(BF16)
    loop(0, 8, keep_grad_o)

    remote(one, one, gfs, opr, g.partner).wait_send()
    for t in (1, 2):
        remote(s0, s0, s1s.at[t], opr, g.partner).wait_send()


FORWARD_SCRATCH = [
    pltpu.VMEM((3, 4096, 1024), BF16),
    pltpu.VMEM((512, 4096), BF16),
    pltpu.VMEM((2, 1024, 512), BF16),
    pltpu.VMEM((512, 1024), BF16),
    pltpu.VMEM((512, 1024), BF16),
    pltpu.VMEM((8, 128), F32),
    pltpu.VMEM((512, 1024), F32),
    pltpu.VMEM((512, 4096), BF16),
    pltpu.VMEM((4, 512, 1024), BF16),
    pltpu.VMEM((1024, 512), BF16),
    pltpu.VMEM((2, 512, 128), F32),
    pltpu.VMEM((4, 8, 512), F32),
    pltpu.VMEM((4, 8, 512), F32),
    pltpu.VMEM((2, 2, 4, SEG, SEG), F32),
    pltpu.VMEM((512, 512), BF16),
    pltpu.VMEM((4, 128, SEG), BF16),
    DMA((4,)), DMA(()), DMA(()), DMA((2, 4)), DMA(()), DMA((4,)),
    DMA(()), DMA(()), DMA(()), DMA((3,)), DMA((3,)), DMA((3,)), DMA((3,)),
    DMA((3, 2)), DMA((4,)), DMA((4,)), DMA((4,)), DMA(()),
    DMA(()), DMA(()), DMA(()), DMA(()), DMA(()), DMA(()), pltpu.SemaphoreType.REGULAR(()),
    DMA(()), DMA(()), DMA(()), DMA(()), DMA(()), DMA(()), DMA((2, 4)), DMA(()), DMA((4,)), DMA(()), DMA(()),
    DMA(()), DMA((2, 4)), DMA(()), DMA((4,)), DMA(()), DMA(()),
    DMA((3,)), DMA((2, 4)),
] + ring_sems(3)


NU = 4
WO = 4


def backward_phase(io, keep, r1, r1h, r2, r2h, rg, buf, dall, rt, lt, gxc, p_all, ds_all, lanes, st, ge, gy, gxo,
            s1s, s1t, s1r, s2s, s2r, ags, agr, agx, d2s, d2r, fws, fwr, lws, lts, gs, gr, gls, wls, gxs, gyl, dps, dpr, sts, strv,
            e1s, e1r, e2s, e2r, e3s, e3r, e4s):
    gy_in, cos_tab, sin_tab, wq, wk, wv, x_t, y_cols, dwv, dwk, dwq, dwo, y_out, gx_part, gx_out, gain_out = io
    acts, gains, stats, post, wo_seg, wo_add, wor, inside, ysd, yrv, yst, e4r = keep
    s0 = wo_add
    outs = (dwv, dwk, dwq, dwq, dwo)
    widths = (SEG, SEG, 128, 128, SEG)
    shifts = (0, 0, 0, 128, 0)
    weights = (wv, wk, wq)
    g = Torus()
    x, z, y, c, p1, p2 = g.x, g.z, g.y, g.c, g.p1, g.p2
    peers = ([(x, mod4(z + d), y, c) for d in (1, 2, 3)] + [(x, z, mod4(y + d), c) for d in (1, 2, 3)]
             + [g.partner, g.xdev(2)] + [g.xdev(d, h) for d in DIRS for h in (0, 1)])
    for peer in peers:
        pl.semaphore_signal(inside, inc=1, device_id=peer, device_id_type=MESH_ID)

    def block(kk, tt, jj):
        d = 1 - 2 * kk
        return g.seg_rows(mod4(p1 - d * (1 + tt)), mod4(p2 - d * (1 + jj)))

    def aload(n, kk):
        par = lax.rem(n, 2)
        return pltpu.make_async_copy(x_t.at[block(kk, 1 + n // 4, lax.rem(n, 4))], lt.at[0, par, kk], lts.at[0, par])

    def bload(jj, kk):
        par = lax.rem(jj, 2)
        return pltpu.make_async_copy(x_t.at[block(kk, 0, jj)], lt.at[1, par, kk], lts.at[1, par])

    def load_wait(kind, par):
        pltpu.make_async_copy(lt.at[kind, par], lt.at[kind, par], lts.at[kind, par]).wait()

    def tile(kind, m, par, kk):
        cols = pl.ds(pl.multiple_of(kk * SEG + shifts[m], 128), widths[m])
        return jnp.dot(lt[kind, par, kk], rt[min(m, 2), :, cols], preferred_element_type=F32)

    def slot(m, kk, t, jj):
        if m == WO:
            return wo_seg.at[kk, jj]
        return r1.at[m, kk, t, jj] if m < 2 else r1h.at[m - 2, kk, t, jj]

    def slot2(m, kk, u):
        return r2h.at[m - 2, kk, u] if m in (2, 3) else r2.at[min(m, 2), kk, u]

    def first_slot(m, kk, jj):
        return s0.at[kk, jj, :, pl.ds(shifts[m], widths[m])]

    def send1(m, t, kk, jj, first=False):
        src = first_slot(m, kk, jj) if first else slot(m, kk, t - 1, jj)
        ss = s1s.at[m, jj] if first and m < 2 else s1t.at[m]
        return remote(src, slot(m, kk, t, jj), ss, s1r.at[m, t, jj], g.axis1(1 - 2 * kk))

    def recv1(m, t, jj):
        ref = r1.at[0, 0, 0, pl.ds(0, 2)] if m < 2 else r1h.at[0, 0, 0, pl.ds(0, 2)]
        remote(ref, ref, s1t.at[0], s1r.at[m, t, jj], g.partner).wait_recv()

    def send2(m, u, kk):
        return remote(slot(m, kk, 2, u), slot2(m, kk, u), s2s.at[m], s2r.at[m, u], g.axis2(DIRS[kk]))

    def start_item(m, jj):
        load_wait(1, lax.rem(jj, 2))
        if m in (1, 2):
            ref = s0.at[0, pl.ds(0, 2)]
            remote(ref, ref, s1s.at[m - 1, jj], s2r.at[0, 0], g.partner).wait_send()

        def color(kk):
            first_slot(m, kk, jj)[...] = tile(1, m, lax.rem(jj, 2), kk)
            send1(m, 0, kk, jj, True).start()
        loop(0, 2, color)
        for kk in range(2):
            pl.when(jj < 2)(lambda: bload(jj + 2, kk).start())
            if m + 1 < NU:
                pl.when(jj >= 2)(lambda: bload(jj - 2, kk).start())

    def ring_item(m, n):
        t, jj = n // 4, lax.rem(n, 4)
        load_wait(0, lax.rem(n, 2))
        recv1(m, t, jj)

        def color(kk):
            ref = slot(m, kk, t, jj)
            ref[...] = ref[...] + tile(0, m, lax.rem(n, 2), kk)
            pl.when(t < 2)(lambda: send1(m, t + 1, kk, jj).start())
        loop(0, 2, color)
        for kk in range(2):
            pl.when(n < 10)(lambda: aload(n + 2, kk).start())
            if m + 1 < NU:
                pl.when(n >= 10)(lambda: aload(n - 10, kk).start())

    def wo_item(jj):
        ref = s0.at[0, pl.ds(0, 2)]
        remote(ref, ref, s1t.at[0], wor.at[jj], g.partner).wait_recv()

        def color(kk):
            wo_seg[kk, jj] = wo_seg[kk, jj] + wo_add[kk, jj]
        loop(0, 2, color)

    def out_cols(k, xs, m=0):
        return pl.ds(pl.multiple_of(k * 1024 + xs * SEG + shifts[m], 128), widths[m])

    def ag_send(m, kk, di, h):
        k = 2 * c + kk
        return remote(slot(m, kk, 2, 3).at[pl.ds(h * 128, 128)], outs[m].at[:, out_cols(k, x, m)], ags.at[m],
                      agr.at[m, di] if di == kk else agx.at[m],
                      g.xdev(DIRS[di], h))

    def pair_send(m, kk):
        src = slot(m, kk, 2, 3).at[at128((1 - c) * 128)]
        return remote(src, outs[m].at[:, out_cols(2 * c + kk, x, m)], d2s.at[m], d2r.at[m], g.partner)

    def own_store(m, kk):
        return pltpu.make_async_copy(slot(m, kk, 2, 3).at[at128(c * 128)], outs[m].at[:, out_cols(2 * c + kk, x, m)], lws.at[m])

    def forward(m, k):
        di = k % 2
        ref = outs[m].at[:, out_cols(k, mod4(x - DIRS[di]), m)]
        return remote(ref, ref, fws.at[m], fwr.at[m], g.xdev(DIRS[di]))

    def hand_out(m, kk):
        own_store(m, kk).start()
        for di in range(2):
            for h in range(2):
                ag_send(m, kk, di, h).start()
        pair_send(m, kk).start()

    def phase2(m, u):
        if u > 0:
            ref = r2h.at[0, 0, pl.ds(0, 2)] if m in (2, 3) else r2.at[0, 0, pl.ds(0, 2)]
            remote(ref, ref, s2s.at[m], s2r.at[m, u - 1], g.partner).wait_recv()
        for kk in range(2):
            if u > 0:
                ref = slot(m, kk, 2, u)
                ref[...] = ref[...] + slot2(m, kk, u - 1)[...]
            if u < 3:
                send2(m, u, kk).start()
            else:
                hand_out(m, kk)

    def direct2(m, u, kk):
        return remote(slot(m, kk, 2, u), slot2(m, kk, u), s2s.at[m], s2r.at[m, u], g.axis2(-(1 + u) * DIRS[kk]))

    def last_phase2(m):
        for u in range(3):
            ref = r2h.at[0, 0, pl.ds(0, 2)]
            remote(ref, ref, s2s.at[m], s2r.at[m, u], g.partner).wait_recv()
        for kk in range(2):
            ref = slot(m, kk, 2, 3)
            ref[...] = (ref[...] + slot2(m, kk, 0)[...]) + (slot2(m, kk, 1)[...] + slot2(m, kk, 2)[...])
            hand_out(m, kk)

    def do_forward(m):
        for di in range(2):
            ref = outs[m].at[:, pl.ds(0, 2 * widths[m])]
            remote(ref, ref, ags.at[m], agr.at[m, di], g.partner).wait_recv()
            for k in (di, di + 2):
                forward(m, k).start()

    def bytes_of(m, n, ss, rs):
        ref = outs[m].at[:, pl.ds(0, n * widths[m])]
        return remote(ref, ref, ss, rs, g.partner)

    def drain_slots(m):
        if m != WO:
            ref = r1.at[m, pl.ds(0, 2), pl.ds(0, 2)] if m < 2 else r1h.at[0]
            remote(ref, ref, s1t.at[m], d2r.at[m], g.partner).wait_send()
        bytes_of(m, 12, s2s.at[m], d2r.at[m]).wait_send()
        bytes_of(m, 8, ags.at[m], agx.at[m]).wait_send()
        bytes_of(m, 2, d2s.at[m], d2r.at[m]).wait_send()
        ref = outs[m].at[:, pl.ds(0, 2 * widths[m])]
        pltpu.make_async_copy(ref, ref, lws.at[m]).wait()

    def drain_unit(m):
        drain_slots(m)
        bytes_of(m, 4, ags.at[m], agx.at[m]).wait_recv()
        bytes_of(m, 2, d2s.at[m], d2r.at[m]).wait_recv()
        bytes_of(m, 4, fws.at[m], fwr.at[m]).wait()

    def gcols(kk, jj):
        return pl.ds(pl.multiple_of(kk * 2048 + jj * 512, 512), 512)

    def gsend(t, kk, jj):
        d = DIRS[kk]
        if t == 0:
            src = gx_part.at[at128(mod4(x - d) * 128), gcols(kk, jj)]
        else:
            src = rg.at[kk, t - 1, jj]
        return remote(src, rg.at[kk, t, jj], gs, gr.at[t, jj], g.xdev(d))

    def gbuf(t, kk, jj):
        return (t % 2, at128(jj * 128), pl.ds(kk * 512, 512))

    def gload(t, kk, jj):
        src = gx_part.at[at128(mod4(x - DIRS[kk] * (2 + t)) * 128), gcols(kk, jj)]
        return pltpu.make_async_copy(src, buf.at[gbuf(t, kk, jj)], gls.at[t % 2, jj])

    def gloads(t):
        each(lambda kk, jj: gload(t, kk, jj).start())

    def chunk_rows(e):
        return pl.ds(pl.multiple_of((lax.rem(e, 2) * 4 + e // 2) * 512, 512), 512)

    def wload(e, i):
        par = lax.rem(e, 2)
        return pltpu.make_async_copy(weights[i].at[chunk_rows(e)], acts.at[3 * par + i], wls.at[par])

    def gx_store(e):
        par = lax.rem(e, 2)
        return pltpu.make_async_copy(gxc.at[par], gx_part.at[:, chunk_rows(e)], gxs.at[par])

    def gx_ship(e, kk):
        gx_store(e).wait()
        gsend(0, kk, e // 2).start()

    def gx_chunk(e):
        par = lax.rem(e, 2)
        ref = acts.at[pl.ds(0, 3)]
        pltpu.make_async_copy(ref, ref, wls.at[par]).wait()

        def rows_half(r):
            rows = at256(r * SEG)
            acc = None
            for i in range(3):
                dot = lax.dot_general(dall[i, rows, :], acts[3 * par + i], NT, preferred_element_type=F32)
                acc = dot if acc is None else acc + dot
            gxc[par, rows, :] = acc
        loop(0, 2, rows_half)
        gx_store(e).start()

        @pl.when(e < 6)
        def _():
            for i in range(3):
                wload(e + 2, i).start()
        for kk in range(2):
            pl.when(jnp.logical_and(e > 0, lax.rem(e, 2) == 1 - kk))(lambda: gx_ship(e - 1, kk))

    gx_save = pltpu.make_async_copy(gxo, gx_out, gyl)

    def gx_item(t, jj):
        ref = rg.at[0, 0, pl.ds(0, 2)]
        remote(ref, ref, gs, gr.at[t, jj], g.partner).wait_recv()
        pltpu.make_async_copy(ref, ref, gls.at[t % 2, jj]).wait()
        for kk in range(2):
            total = rg[kk, t, jj] + buf[gbuf(t, kk, jj)]
            if t < 2:
                rg[kk, t, jj] = total
                gsend(t + 1, kk, jj).start()
            else:
                gxo[:, gcols(kk, jj)] = (total + gy[:, gcols(kk, jj)].astype(F32)).astype(BF16)

    def y_send(i, k):
        d = (1, -1, 2)[i]
        src = y_cols.at[at128(mod4(x + d) * 128), pl.ds(k * SEG, SEG)]
        return remote(src, y_out.at[:, out_cols(k, x)], ysd, yrv, g.xdev(d))

    def y_own(k):
        return pltpu.make_async_copy(y_cols.at[at128(x * 128), pl.ds(k * SEG, SEG)], y_out.at[:, out_cols(k, x)], yst)

    gain1 = remote(ge.at[0], ge.at[1], e1s, e1r, g.partner)

    def gain2(d):
        return remote(ge.at[8], ge.at[1 + d], e2s.at[d - 1], e2r.at[d - 1], (x, mod4(z + d), y, c))

    def gain3(d):
        return remote(ge.at[9], ge.at[4 + d], e3s.at[d - 1], e3r.at[d - 1], (x, z, mod4(y + d), c))

    my_head = at128(z * SEG + c * 128)

    def gain4(d):
        return remote(ge.at[10, :, my_head], gain_out, e4s.at[d - 1], e4r, g.xdev(d))

    gy_load = pltpu.make_async_copy(gy_in, gy, gyl)
    stat = StatExchange(g, st, sts, strv)
    theirs = pl.ds(pl.multiple_of((1 - c) * 512, 512), 512)
    mine = pl.ds(pl.multiple_of(c * 512, 512), 512)

    def swap(i):
        return remote(dall.at[i, :, theirs], rt.at[i, pl.ds(512, 512)], dps.at[i], dpr.at[i], g.partner)

    def share(i):
        rt[i, 0:512] = dall[i, :, mine]
        swap(i).start()

    gy_load.start()
    for k in range(4):
        for i in range(3):
            y_send(i, k).start()
        y_own(k).start()
    for kk in range(2):
        for jj in range(2):
            bload(jj, kk).start()
            aload(jj, kk).start()
    inv = [gxc.at[0, :, pl.ds(i * 128, 128)] for i in range(2)]
    proj = [gxc.at[1, :, pl.ds(i * 128, 128)] for i in range(2)]
    for i in range(2):
        inv[i][...] = jnp.broadcast_to(inv_column(stats[...], i), (512, 128))
    lanes[...] = jnp.zeros((2, 512, 128), F32)
    st[0] = jnp.zeros((8, 512), F32)
    ge[0] = jnp.zeros((8, 1024), F32)
    ge[0, 2:3] = post[...]

    p_all[...] = jnp.zeros((512, 512), BF16)
    ds_all[...] = jnp.zeros((512, 512), BF16)

    def norm_back(i, src_rows, cols, gn):
        hat = acts[i, src_rows, cols].astype(F32) * inv[i][src_rows, :]
        prod = gn * hat
        gain = gains[i:i + 1, cols]
        buf[i, src_rows, cols] = gn * gain
        lanes[i, src_rows] = lanes[i, src_rows] + prod * gain
        return jnp.sum(prod, axis=0, keepdims=True)

    def head(h):
        cols = at128(h * 128)
        vh, qh, kh, do = (acts[i, :, cols] for i in (2, 3, 4, 5))
        for i in range(4):
            n = (i + 1) * 128
            block_i = pl.ds(i * 128, 128)
            s = causal_scores(kh[:n], qh[i * 128:n], i, n)
            e = jnp.exp(s - jnp.max(s, axis=0, keepdims=True))
            p = e * (1.0 / jnp.sum(e, axis=0, keepdims=True))
            dp = lax.dot_general(vh[:n], do[i * 128:n], NT, preferred_element_type=F32)
            p_all[0:n, block_i] = p.astype(BF16)
            ds_all[0:n, block_i] = (p * (dp - jnp.sum(p * dp, axis=0, keepdims=True)) * SCALE).astype(BF16)
        dall[0, :, cols] = jnp.dot(p_all[...], do, preferred_element_type=F32).astype(BF16)
        dq = lax.dot_general(ds_all[...], kh, TN, preferred_element_type=F32)
        dk = jnp.dot(ds_all[...], qh, preferred_element_type=F32)
        for i, grad in ((0, dq), (1, dk)):
            ge[0, i:i + 1, cols] = norm_back(i, pl.ds(0, 512), cols, rope_turn(grad, cos_tab[...], -sin_tab[...]))

    def finish(i, m, column):
        proj[i][...] = jnp.broadcast_to(column, (512, 128))

        def step(h):
            cols = at128(h * 128)
            scale = inv[i][...]
            hat = acts[i, :, cols].astype(F32) * scale
            dall[m, :, cols] = (scale * (buf[i, :, cols] - hat * proj[i][...])).astype(BF16)
        loop(0, 8, step)

    def head_step(i):
        head(i)

        @pl.when(i == 1)
        def _():
            pl.semaphore_wait(inside, len(peers))
            wo_item(0)
            phase2(WO, 0)

        @pl.when(i == 3)
        def _():
            wo_item(1)
            phase2(WO, 1)

        @pl.when(i == 5)
        def _():
            wo_item(2)
            phase2(WO, 2)
    loop(0, 8, head_step)
    share(0)
    for i in range(2):
        stat.put(i, lanes[i])
    stat.start()
    gain1.start()
    wo_item(3)
    swap(0).wait_recv()
    loop(0, 4, lambda jj: start_item(0, jj))
    total = stat.total().T / 4096.0
    phase2(WO, 3)
    finish(1, 1, total[:, 1:2])
    share(1)
    finish(0, 2, total[:, 0:1])
    share(2)
    for e in range(2):
        for i in range(3):
            wload(e, i).start()
    gy_load.wait()

    for m in range(NU):
        def early(n, m=m):
            ring_item(m, n)
            if m > 0:
                pl.when(n == 0)(lambda: phase2(m - 1, 2))
                pl.when(n == 2)(lambda: phase2(m - 1, 3))
            if m == 0:
                gx_chunk(n)
            elif m == 1:
                pl.when(n >= 4)(lambda: gx_item(1, n - 4))

        loop(0, 8, early)
        if m == 0:
            gx_ship(7, 1)
            gloads(0)
            gloads(1)
            do_forward(WO)
            gain1.wait_recv()
            ge[8] = ge[0] + ge[1]
            for d in (1, 2, 3):
                gain2(d).start()
            swap(1).wait_recv()
            swap(2).wait_recv()
        if m == 1:
            for d in (1, 2, 3):
                gain2(d).wait_recv()
            ge[9] = (ge[8] + ge[2]) + (ge[3] + ge[4])
            for d in (1, 2, 3):
                gain3(d).start()
        if m == 3:
            gx_save.start()
            do_forward(1)
        if m == 2:
            for d in (1, 2, 3):
                gain3(d).wait_recv()
            ge[10] = (ge[9] + ge[5]) + (ge[6] + ge[7])

            @pl.when(y == x)
            def _():
                gain_out[...] = ge[10, :, my_head]
                for d in (1, 2, 3):
                    gain4(d).start()

        def late(n, m=m):
            if m + 1 < NU:
                start_item(m + 1, n - 8)
            ring_item(m, n)
            if m < 3:
                pl.when(n == 8)(lambda: phase2(m, 0))
                pl.when(n == 10)(lambda: phase2(m, 1))
            else:
                for u in range(3):
                    for kk in range(2):
                        pl.when(n == 8 + u)(lambda: direct2(m, u, kk).start())
            if m in (0, 2):
                gx_item(m, n - 8)

        loop(8, 12, late)
        if m == 0:
            gloads(2)
        if m == 1:
            do_forward(0)
        if m == 3:
            do_forward(2)
    last_phase2(NU - 1)
    do_forward(NU - 1)

    @pl.when(y == x)
    def _():
        for d in (1, 2, 3):
            gain4(d).wait_send()

    @pl.when(y != x)
    def _():
        gain4(1).wait_recv()
    gain1.wait_send()
    for d in (1, 2, 3):
        gain2(d).wait_send()
        gain3(d).wait_send()
    y_all, y_mine = y_out.at[:, pl.ds(0, 3072)], y_out.at[:, pl.ds(0, 1024)]
    remote(y_all, y_all, ysd, yrv, g.partner).wait()
    pltpu.make_async_copy(y_mine, y_mine, yst).wait()
    for m in range(NU + 1):
        drain_unit(m)
    most = gx_part.at[:, pl.ds(0, 3072)]
    remote(most, most, gs, gr.at[0, 0], g.partner).wait_send()
    for i in range(3):
        swap(i).wait_send()
    gx_save.wait()


BACKWARD_SCRATCH = [
    pltpu.VMEM((2, 2, 3, 4, SEG, SEG), F32),
    pltpu.VMEM((2, 2, 3, 4, SEG, 128), F32),
    pltpu.VMEM((3, 2, 3, SEG, SEG), F32),
    pltpu.VMEM((2, 2, 3, SEG, 128), F32),
    pltpu.VMEM((2, 3, 4, 128, 512), F32),
    pltpu.VMEM((2, 512, 1024), F32),
    pltpu.VMEM((3, 512, 1024), BF16),
    pltpu.VMEM((3, 1024, 512), BF16),
    pltpu.VMEM((2, 2, 2, SEG, 1024), BF16),
    pltpu.VMEM((2, 512, 512), F32),
    pltpu.VMEM((512, 512), BF16),
    pltpu.VMEM((512, 512), BF16),
    pltpu.VMEM((2, 512, 128), F32),
    pltpu.VMEM((4, 8, 512), F32),
    pltpu.VMEM((11, 8, 1024), F32),
    pltpu.VMEM((128, 4096), BF16),
    pltpu.VMEM((128, 4096), BF16),
    DMA((2, 4)), DMA((NU,)), DMA((NU, 3, 4)), DMA((NU + 1,)), DMA((NU + 1, 3)),
    DMA((NU + 1,)), DMA((NU + 1, 2)), DMA((NU + 1,)), DMA((NU + 1,)), DMA((NU + 1,)), DMA((NU + 1,)), DMA((NU + 1,)), DMA((NU + 1,)),
    DMA((2, 2)), DMA(()), DMA((3, 4)), DMA((2, 4)), DMA((2,)), DMA((2,)), DMA(()),
    DMA((3,)), DMA((3,)), DMA((3,)), DMA((3,)),
    DMA(()), DMA(()), DMA((3,)), DMA((3,)), DMA((3,)), DMA((3,)), DMA((3,)),
]


def layer_kernel(wq_in, wk_in, wv_in, wo_in, x_in, gy_in, gq_in, gk_in, gp_in, cos_tab, sin_tab,
                 dwv, dwk, dwq, dwo, y_out, gx_out, wq_out, wk_out, wv_out, x_t, y_cols, gx_part, gain_out,
                 acts, gains, stats, post, wo_seg, wo_add, wor, inside, ysd, yrv, yst, e4r):
    keep = (acts, gains, stats, post, wo_seg, wo_add, wor)
    first = (wq_in, wk_in, wv_in, wo_in, x_in, gy_in, gq_in, gk_in, gp_in, cos_tab, sin_tab, wq_out, wk_out, wv_out, x_t, y_cols)
    second = (gy_in, cos_tab, sin_tab, wq_out, wk_out, wv_out, x_t, y_cols, dwv, dwk, dwq, dwo, y_out, gx_part, gx_out, gain_out)
    pl.run_scoped(lambda *refs: forward_phase(first, keep, *refs), *FORWARD_SCRATCH)
    pl.run_scoped(lambda *refs: backward_phase(second, keep + (inside, ysd, yrv, yst, e4r), *refs), *BACKWARD_SCRATCH)


def layer(w_q, w_k, w_v, w_o, x_tok, gy_tok, gq, gk, gp, cos_tab, sin_tab):
    grad, tok, mat = SDS((128, 4096), F32), SDS((128, 4096), BF16), SDS((4096, 1024), BF16)
    return pl.pallas_call(
        layer_kernel,
        out_shape=[grad] * 4 + [tok] * 2 + [mat] * 4 + [SDS((512, 1024), BF16), SDS((512, 4096), F32), SDS((8, 128), F32)],
        in_specs=[IN_HBM] * 6 + [IN_VMEM] * 5,
        out_specs=[IN_HBM] * 12 + [IN_VMEM],
        scratch_shapes=[
            pltpu.VMEM((6, 512, 1024), BF16),
            pltpu.VMEM((8, 1024), F32),
            pltpu.VMEM((8, 512), F32),
            pltpu.VMEM((1, 1024), F32),
            pltpu.VMEM((2, 4, SEG, SEG), F32),
            pltpu.VMEM((2, 4, SEG, SEG), F32),
            DMA((4,)), pltpu.SemaphoreType.REGULAR, DMA(()), DMA(()), DMA(()), DMA(()),
        ],
        compiler_params=params(5, 63.9), cost_estimate=COST, name='layer',
    )(w_q, w_k, w_v, w_o, x_tok, gy_tok, gq, gk, gp, cos_tab, sin_tab)


def copy_kernel(*refs):
    n = (len(refs) - 7) // 5
    gain_src, gain_dst, gain_buf, gain_sems = refs[n], refs[2 * n + 1:2 * n + 4], refs[3 * n + 4], refs[5 * n + 5:]
    srcs, dsts, bufs = refs[:n], refs[n + 1:2 * n + 1], refs[2 * n + 4:3 * n + 4]
    loads, stores = refs[3 * n + 5:4 * n + 5], refs[4 * n + 5:5 * n + 5]
    parts = 4

    def rows(i, p):
        step = srcs[i].shape[0] // parts
        return pl.ds(p * step, step)

    def load(i, p):
        return pltpu.make_async_copy(srcs[i].at[rows(i, p)], bufs[i].at[rows(i, p)], loads[i].at[p])

    def store(i, p):
        return pltpu.make_async_copy(bufs[i].at[rows(i, p)], dsts[i].at[rows(i, p)], stores[i].at[p])

    gain_load = pltpu.make_async_copy(gain_src, gain_buf, gain_sems[0])
    gain_stores = [pltpu.make_async_copy(gain_buf.at[pl.ds(i, 1)], gain_dst[i], gain_sems[1].at[i]) for i in range(3)]
    order = [(i, p) for i in range(n) for p in range(parts)]
    gain_load.start()
    for i, p in order:
        load(i, p).start()
    gain_load.wait()
    for copy in gain_stores:
        copy.start()
    for i, p in order:
        load(i, p).wait()
        store(i, p).start()
    for i, p in order:
        store(i, p).wait()
    for copy in gain_stores:
        copy.wait()


def copy_out(gains, *arrays):
    n = len(arrays)
    return pl.pallas_call(
        copy_kernel,
        out_shape=[SDS(a.shape, a.dtype) for a in arrays] + [SDS((1, 128), F32)] * 3,
        in_specs=[IN_HBM] * (n + 1),
        out_specs=[IN_HBM] * (n + 3),
        scratch_shapes=[pltpu.VMEM(a.shape, a.dtype) for a in arrays] + [pltpu.VMEM((8, 128), F32)] + [DMA((4,))] * (2 * n) + [DMA(()), DMA((3,))],
        compiler_params=pltpu.CompilerParams(vmem_limit_bytes=63 * 1024 * 1024), cost_estimate=COST, name='copy_out',
    )(*arrays, gains)


def solution(mesh):
    mesh4 = Mesh(mesh.devices.reshape(4, 4, 4, 2), ('sp', 'z', 'y', 'c'))
    tok_spec = P(FS, 'sp', None)
    row_spec = P(FS, None)
    vec_spec = P(FS)

    def local_step(x, grad_y, wq_rows, wk_rows, wv_rows, wo_rows, gq_rows, gk_rows, gpost_rows):
        x_tok, gy_tok = x[0], grad_y[0]
        cos_tab, sin_tab = rope_tables(4 * x_tok.shape[0])
        dwv, dwk, dwq, dwo, y, grad_x, *_, gn = layer(
            wq_rows, wk_rows, wv_rows, wo_rows, x_tok, gy_tok, gq_rows[None], gk_rows[None], gpost_rows[None], cos_tab, sin_tab)
        dwv, dwk, dwq, dwo, y, grad_x, *gn = copy_out(gn, dwv, dwk, dwq, dwo, y, grad_x)
        return y[None], grad_x[None], dwq, dwk, dwv, dwo, gn[0][0], gn[1][0], gn[2][0]

    return jax.shard_map(local_step, mesh=mesh4,
                         in_specs=(tok_spec, tok_spec, row_spec, row_spec, row_spec, row_spec, vec_spec, vec_spec, vec_spec),
                         out_specs=(tok_spec, tok_spec, row_spec, row_spec, row_spec, row_spec, vec_spec, vec_spec, vec_spec),
                         check_vma=False)
```

```python
import jax
import jax.numpy as jnp
import numpy as np
from jax import lax
from jax.experimental import pallas as pl
from jax.experimental.pallas import tpu as pltpu
from jax.sharding import Mesh, PartitionSpec as P

HEAD_DIM = 128
RMS_EPSILON = 1e-6
ROPE_THETA = 500000.0
FS = ('z', 'y', 'c')
F32 = jnp.float32
BF16 = jnp.bfloat16
MESH_ID = pl.DeviceIdType.MESH
HBM = pl.ANY
SEG = 256


def rope_tables(seq_len):
    half_dim = HEAD_DIM // 2
    angles = np.arange(seq_len)[:, None] * ROPE_THETA ** (-np.arange(half_dim) * (2.0 / HEAD_DIM))[None, :]
    cos_half, sin_half = np.cos(angles), np.sin(angles)
    tables = np.concatenate([cos_half, cos_half], axis=1), np.concatenate([-sin_half, sin_half], axis=1)
    return tuple(jnp.asarray(t, F32) for t in tables)


def coords():
    return tuple(lax.axis_index(n) for n in ('sp', 'z', 'y', 'c'))


def mod4(v):
    return lax.rem(v + 8, 4)


def remote(src, dst, ss, rs, dev):
    return pltpu.make_async_remote_copy(src_ref=src, dst_ref=dst, send_sem=ss, recv_sem=rs, device_id=dev, device_id_type=MESH_ID)


def at256(v):
    return pl.ds(pl.multiple_of(v, SEG), SEG)


def at128(v):
    return pl.ds(pl.multiple_of(v, 128), 128)


def each(fn, n=4):
    def step(jj, carry):
        for kk in range(2):
            fn(kk, jj)
        return carry
    lax.fori_loop(0, n, step, 0)


def loop(lo, hi, fn):
    def step(n, carry):
        fn(n)
        return carry
    lax.fori_loop(lo, hi, step, 0)


def greet(peers):
    barrier = pltpu.get_barrier_semaphore()
    for peer in peers:
        pl.semaphore_signal(barrier, inc=1, device_id=peer, device_id_type=MESH_ID)
    return lambda: pl.semaphore_wait(barrier, len(peers))


class Torus:
    def __init__(self):
        self.x, self.z, self.y, self.c = x, z, y, c = coords()
        self.p1 = (1 - c) * y + c * z
        self.p2 = (1 - c) * z + c * y
        self.partner = (x, z, y, 1 - c)

    def axis1(self, d):
        return (self.x, mod4(self.z + d * self.c), mod4(self.y + d * (1 - self.c)), self.c)

    def axis2(self, d):
        return (self.x, mod4(self.z + d * (1 - self.c)), mod4(self.y + d * self.c), self.c)

    def xdev(self, d, core=None):
        return (mod4(self.x + d), self.z, self.y, self.c if core is None else core)

    def seg_rows(self, b, j):
        zz = (1 - self.c) * j + self.c * b
        yy = (1 - self.c) * b + self.c * j
        return at256(zz * 1024 + yy * SEG)


DIRS = (1, -1)
RING_SEMS = 8


def ring_sems(nw):
    dma = pltpu.SemaphoreType.DMA
    return [dma((nw,)), dma((nw,)), dma((nw,)), dma((nw, 3)), dma((nw,)), dma((nw, 3, 4)), dma((nw,)), dma((nw,))]


class WeightRings:
    def __init__(self, g, w, slots, sems):
        self.g, self.w, self.slots = g, w, slots
        self.d0s, self.d0r, self.a1s, self.a1r, self.a2s, self.a2r, self.f3s, self.f3r = sems
        self.my_rows = at128(g.z * 1024 + g.y * SEG + g.c * 128)

    def pair_send(self, m):
        ref = self.w.at[self.slots[m], self.my_rows]
        return remote(ref, ref, self.d0s.at[self.slots[m]], self.d0r.at[self.slots[m]], self.g.partner)

    def same(self, m, kk, rows, ss, rs, dev):
        ref = self.w.at[self.slots[m], rows, at256((2 * self.g.c + kk) * SEG)]
        return remote(ref, ref, ss, rs, dev)

    def bulk(self, m, n, ss, rs):
        ref = self.w.at[self.slots[m], pl.ds(0, n * 128), pl.ds(0, 512)]
        return remote(ref, ref, ss, rs, self.g.partner)

    def send1(self, m, u, kk):
        g, d = self.g, DIRS[kk]
        return self.same(m, kk, g.seg_rows(g.p1, mod4(g.p2 - d * u)), self.a1s.at[self.slots[m]], self.a1r.at[self.slots[m], u], g.axis2(d))

    def far1(self, m, e, kk):
        g = self.g
        rows = g.seg_rows(g.p1, g.p2)
        return self.same(m, kk, rows, self.a1s.at[self.slots[m]], self.a1r.at[self.slots[m], e - 1], g.axis2(DIRS[kk] * e))

    def fwd1(self, m, u, kk):
        g = self.g
        rows = g.seg_rows(g.p1, mod4(g.p2 - DIRS[kk] * (u + 1)))
        return self.same(m, kk, rows, self.f3s.at[self.slots[m]], self.f3r.at[self.slots[m]], g.partner)

    def send2(self, m, t, kk, jj):
        g, d = self.g, DIRS[kk]
        rows = g.seg_rows(mod4(g.p1 - d * t), mod4(g.p2 - d * jj))
        return self.same(m, kk, rows, self.a2s.at[self.slots[m]], self.a2r.at[self.slots[m], t, jj], g.axis1(d))

    def fwd2(self, m, t, kk, jj):
        g, d = self.g, DIRS[kk]
        rows = g.seg_rows(mod4(g.p1 - d * (t + 1)), mod4(g.p2 - d * jj))
        return self.same(m, kk, rows, self.f3s.at[self.slots[m]], self.f3r.at[self.slots[m]], g.partner)

    def first(self, m, far=False):
        self.pair_send(m).wait_recv()
        for kk in range(2):
            if far:
                for e in (1, 2, 3):
                    self.far1(m, e, kk).start()
            else:
                self.send1(m, 0, kk).start()
            self.send2(m, 0, kk, 0).start()

    def second(self, m, u, far=False):
        self.bulk(m, 2, self.a1s.at[self.slots[m]], self.a1r.at[self.slots[m], u]).wait_recv()
        for kk in range(2):
            if u < 2 and not far:
                self.send1(m, u + 1, kk).start()
            self.send2(m, 0, kk, u + 1).start()
            self.fwd1(m, u, kk).start()

    def item(self, m, t, jj):
        self.bulk(m, 2, self.a2s.at[self.slots[m]], self.a2r.at[self.slots[m], t, jj]).wait_recv()

        def pass_on():
            for kk in range(2):
                self.send2(m, t + 1, kk, jj).start()
        if isinstance(t, int):
            if t < 2:
                pass_on()
        else:
            pl.when(t < 2)(pass_on)
        for kk in range(2):
            self.fwd2(m, t, kk, jj).start()

    def round(self, m, t, extra=None):
        def step(jj):
            self.item(m, t, jj)
            if extra is not None:
                extra(jj)
        loop(0, 4, step)

    def pair_done(self, m):
        self.bulk(m, 30, self.f3s.at[self.slots[m]], self.f3r.at[self.slots[m]]).wait_recv()

    def drain(self, m):
        self.pair_send(m).wait_send()
        for sems, n in ((self.a1s, 6), (self.a2s, 24), (self.f3s, 30)):
            self.bulk(m, n, sems.at[self.slots[m]], self.f3r.at[self.slots[m]]).wait_send()


class StatExchange:
    def __init__(self, g, st, ss, rs):
        self.g, self.st, self.ss, self.rs = g, st, ss, rs

    def copy(self, i):
        return remote(self.st.at[0], self.st.at[1 + i], self.ss.at[i], self.rs.at[i], self.g.xdev((1, -1, 2)[i]))

    def put(self, i, lanes):
        self.st[0, i:i + 1] = jnp.sum(lanes.T, axis=0, keepdims=True)

    def start(self):
        for i in range(3):
            self.copy(i).start()

    def total(self):
        for i in range(3):
            self.copy(i).wait()
        return (self.st[0] + self.st[1]) + (self.st[2] + self.st[3])


def params(cid, vmem_mib=60.0):
    return pltpu.CompilerParams(collective_id=cid, has_side_effects=True, vmem_limit_bytes=int(vmem_mib * 1024 * 1024))


COST = pl.CostEstimate(flops=10 ** 11, bytes_accessed=10 ** 8, transcendentals=0)
DMA = pltpu.SemaphoreType.DMA
IN_VMEM = pl.BlockSpec(memory_space=pltpu.VMEM)
IN_HBM = pl.BlockSpec(memory_space=pl.ANY)
SDS = jax.ShapeDtypeStruct


SCALE = HEAD_DIM ** -0.5
TN = (((0,), (0,)), ((), ()))
NT = (((1,), (1,)), ((), ()))
W_SLOTS = (0, 1, 2, 0, 1)


def rope_turn(u, cos_tab, sin_tab):
    return u * cos_tab + pltpu.roll(u, 64, 1) * sin_tab


def causal_scores(keys, q_blk, i, n):
    s = lax.dot_general(keys, q_blk, NT, preferred_element_type=F32) * SCALE
    query = lax.broadcasted_iota(jnp.int32, (n, 128), 1) + i * 128
    return jnp.where(query >= lax.broadcasted_iota(jnp.int32, (n, 128), 0), s, -1e30)


def inv_column(total, i):
    return lax.rsqrt(total.T[:, i:i + 1] / 4096.0 + RMS_EPSILON)


def forward_phase(io, keep, w, x_full, xt, gyc, xcv, gains_in, a_acc, o_full, ga_all, gtw, sq, st, st2, r1, p_all, tmp,
            ld, xls, xs, xr, xfs, xfr, gls, gys, gyr, sts, strv, sts2, strv2, wos, xps, xpr, xst, yst,
            g1s, g1r, g2s, g2r, g3s, g3r, free,
            scl, sc1s, sc1r, sc2s, sc2r, osd, orv, ofs, ofr, ops, opr, gsd, grv, gfs, gfr, gps, gpr, s1s, s1r, *ring):
    (wq_in, wk_in, wv_in, wo_in, x_in, gy_in, gq_in, gk_in, gp_in, cos_tab, sin_tab, wq_out, wk_out, wv_out, x_t, y_cols) = io
    acts, gains, stats, post, wo_seg, wo_add, wo_mid, wor, wo_sent = keep
    s0 = wo_add
    w_in, w_out = (wq_in, wk_in, wv_in, wo_in), (wq_out, wk_out, wv_out)
    nw = 3
    cols_m, rows_m = 3, 4
    g = Torus()
    x, z, y, c, p1, p2 = g.x, g.z, g.y, g.c, g.p1, g.p2
    rings = WeightRings(g, w, W_SLOTS, ring)
    plane = [(x, mod4(z + d), y, c) for d in (1, 2, 3)] + [(x, z, mod4(y + d), c) for d in (1, 2, 3)] + [g.partner]
    everyone = plane + [g.xdev(1), g.xdev(-1), g.xdev(2)]
    ready = greet(everyone)

    def load(m, k):
        src = w_in[m].at[:, at256(k * 1024 + x * SEG)]
        return pltpu.make_async_copy(src, w.at[W_SLOTS[m], rings.my_rows, pl.ds(k * SEG, SEG)], ld.at[m])

    def rows_y(d):
        to = mod4(y + d)
        return remote(wo_in.at[:, at256(to * 1024 + x * SEG)], tmp.at[y], sc1s, sc1r, (x, z, to, c))

    def rows_x(d):
        return remote(tmp.at[mod4(x + d)], w.at[1, rings.my_rows, at256(x * SEG)], sc2s, sc2r, g.xdev(d))

    tmp_own = pltpu.make_async_copy(wo_in.at[:, at256(y * 1024 + x * SEG)], tmp.at[y], scl)
    tmp3 = tmp.at[pl.ds(0, 3)]

    def load_wait(m):
        ref = w.at[W_SLOTS[m], rings.my_rows]
        pltpu.make_async_copy(ref, ref, ld.at[m]).wait()

    def xseg(b, s):
        return x_full.at[at128(b * 128), pl.ds(s * 1024, 1024)]

    x_own = pltpu.make_async_copy(x_in, x_full.at[at128(x * 128)], xls)

    def xsend(di, s):
        ref = xseg(x, s)
        return remote(ref, ref, xs, xr.at[di, s], g.xdev(DIRS[di]))

    def xfwd(s):
        d = DIRS[s // 2]
        ref = xseg(mod4(x - d), s)
        return remote(ref, ref, xfs, xfr.at[s], g.xdev(d))

    gy_rows = at128(x * 128)

    def gy_own(k):
        return pltpu.make_async_copy(gy_in.at[:, at256(k * 1024 + x * SEG)], gyc.at[gy_rows, pl.ds(k * SEG, SEG)], gls)

    def gy_send(i, k):
        d = (1, -1, 2)[i]
        src = gy_in.at[:, at256(k * 1024 + mod4(x + d) * SEG)]
        return remote(src, gyc.at[gy_rows, pl.ds(k * SEG, SEG)], gys, gyr, g.xdev(d))

    def gblock(zh, ch):
        return gains.at[:, at128(zh * SEG + ch * 128)]

    def gain1(d):
        return remote(gains_in, gblock(z, c), g1s, g1r, (x, z, mod4(y + d), c))

    def gain2(d):
        ref = gblock(z, c)
        return remote(ref, ref, g2s, g2r, (x, mod4(z + d), y, c))

    def gain3(zh):
        ref = gblock(zh, c)
        return remote(ref, ref, g3s, g3r, g.partner)

    stat = StatExchange(g, st, sts, strv)
    stat2 = StatExchange(g, st2, sts2, strv2)

    def xt_pair(b):
        return remote(xt.at[lax.rem(b, 2)], x_t.at[pl.ds(pl.multiple_of(b * 1024, 1024), 1024), pl.ds(512, 512)], xps.at[b], xpr.at[b], g.partner)

    def xt_store(b):
        return pltpu.make_async_copy(xt.at[lax.rem(b, 2)], x_t.at[pl.ds(pl.multiple_of(b * 1024, 1024), 1024), pl.ds(0, 512)], xst.at[b])

    def turn(b):
        @pl.when(b >= 2)
        def _():
            xt_pair(b - 2).wait_send()
            xt_store(b - 2).wait()

        def step(i):
            xt[lax.rem(b, 2), at256(i * SEG), :] = x_full[:, at256(b * 1024 + i * SEG)].T
        loop(0, 4, step)
        xt_pair(b).start()
        xt_store(b).start()

    def w_store(m, theirs):
        cols = pl.ds(pl.multiple_of(((1 - c) if theirs else c) * 512, 512), 512)
        return pltpu.make_async_copy(w.at[m, :, cols], w_out[m].at[:, cols], wos.at[m, int(theirs)])

    y_store = pltpu.make_async_copy(xcv, y_cols, yst)

    st[0] = jnp.zeros((8, 512), F32)
    st2[0] = jnp.zeros((8, 512), F32)
    p_all[...] = jnp.zeros((512, 512), BF16)
    sq[...] = jnp.zeros((2, 512, 128), F32)
    gains_in[...] = jnp.concatenate([gq_in[...], gk_in[...], gp_in[...], jnp.zeros((5, 128), F32)], axis=0)
    for k in range(4):
        load(0, k).start()
    x_own.start()
    for m in range(1, nw):
        for k in range(4):
            load(m, k).start()
    for k in range(4):
        gy_own(k).start()
    ready()
    for m in range(nw):
        load_wait(m)
        rings.pair_send(m).start()
        if m == 0:
            x_own.wait()
            for s in range(4):
                for di in range(2):
                    xsend(di, (s + 2 * di) % 4).start()

    @pl.when(y == x)
    def _():
        gains[:, at128(z * SEG + c * 128)] = gains_in[...]
        for d in (1, 2, 3):
            gain1(d).start()

    def chunk(m, half, i):
        cols = at256((2 * (c + half * (1 - 2 * c)) + i) * SEG)
        acc_ref = a_acc.at[:, pl.ds(0, SEG)]

        def accumulate(kc):
            rows = pl.ds(pl.multiple_of(kc * 2048, 2048), 2048)
            acc_ref[...] = acc_ref[...] + jnp.dot(x_full[:, rows], w[m, rows, cols], preferred_element_type=F32)
        acc_ref[...] = jnp.zeros((512, SEG), F32)
        loop(0, 2, accumulate)
        acc = acc_ref[...].astype(BF16)
        acts[m, :, cols] = acc
        if m < 2:
            sqv = acc.astype(F32)
            sqv = sqv * sqv
            sq[m] = sq[m] + (sqv[:, :128] + sqv[:, 128:])

    def chunk_beside(m, half):
        return lambda jj: pl.when(lax.rem(jj, 2) == 1)(lambda: chunk(m, half, jj // 2))

    rings.first(0, True)
    rings.first(1)
    for u in range(3):
        rings.second(0, u, True)

    def prep_pair(jj):
        def step(i):
            cols = at128((2 * jj + i) * 128)
            for j in range(2):
                u = acts[j, :, cols].astype(F32) * sq[j] * gains[j:j + 1, cols]
                acts[3 + j, :, cols] = rope_turn(u, cos_tab[...], sin_tab[...]).astype(BF16)
        loop(0, 2, step)

    def tell(slot):
        for peer in everyone:
            pl.semaphore_signal(free.at[slot], inc=1, device_id=peer, device_id_type=MESH_ID)

    def beside(m, t):
        if (m, t) == (1, 1):
            own = chunk_beside(0, 0)

            def both(jj):
                turn(jj)
                own(jj)
            return both
        return {(1, 2): chunk_beside(0, 1), (2, 0): lambda jj: chunk(1, jj // 2, lax.rem(jj, 2)), (2, 2): prep_pair}.get((m, t))

    for m in range(nw):
        for t in range(3):
            if (m, t) == (2, 0):
                rings.pair_done(1)
                w_store(1, True).start()
            rings.round(m, t, beside(m, t))
            if m + 1 < nw:
                rings.second(m + 1, t)
            if (m, t) == (0, 0):
                @pl.when(y != x)
                def _():
                    remote(gains_in, gblock(z, c), g1s, g1r, g.partner).wait_recv()
                for d in (1, 2, 3):
                    gain2(d).start()
            if (m, t) == (0, 1):
                rings.first(2)
                for s in range(4):
                    xsend(s // 2, s).wait_recv()
                    xfwd(s).start()
                for k in range(4):
                    for i in range(3):
                        gy_send(i, k).start()
            if (m, t) == (0, 2):
                w_store(0, False).start()
                gain_rest = gains.at[:, pl.ds(0, 384)]
                remote(gain_rest, gain_rest, g2s, g2r, g.partner).wait()
                for zh in range(4):
                    gain3(zh).start()
            if (m, t) == (1, 0):
                rings.pair_done(0)
                w_store(0, True).start()
                for s in range(4):
                    xsend(1 - s // 2, s).wait_recv()
                    xfwd(s).wait_recv()
            if (m, t) == (1, 2):
                w_store(1, False).start()
                for k in range(4):
                    xcv[:, pl.ds(k * SEG, SEG)] = x_full[:, at256(k * 1024 + x * SEG)]
                rings.drain(0)
                w_store(0, False).wait()
                w_store(0, True).wait()
                tell(0)
                for k in range(4):
                    load(cols_m, k).start()
            if (m, t) == (2, 0):
                for i in range(2):
                    stat.put(i, sq[i])
                stat.start()
                load_wait(cols_m)
                pl.semaphore_wait(free.at[0], len(everyone))
                rings.pair_send(cols_m).start()
            if (m, t) == (2, 1):
                rings.drain(1)
                w_store(1, False).wait()
                w_store(1, True).wait()
                half_x, quarter_x = x_full.at[:, pl.ds(0, 2048)], x_full.at[:, pl.ds(0, 1024)]
                remote(half_x, half_x, xs, xr.at[0, 0], g.partner).wait_send()
                remote(quarter_x, quarter_x, xfs, xr.at[0, 0], g.partner).wait_send()
                tmp_own.start()
                for d in (1, 2, 3):
                    rows_y(d).start()
                tell(1)
                gain_half = gains.at[:, pl.ds(0, 512)]
                remote(gain_half, gain_half, g3s, g3r, g.partner).wait()
                total = stat.total()
                stats[...] = total
                for i in range(2):
                    sq[i] = jnp.broadcast_to(inv_column(total, i), (512, 128))

    rings.first(cols_m, True)
    remote(tmp3, tmp3, sc1s, sc1r, g.partner).wait_recv()
    tmp_own.wait()
    pl.semaphore_wait(free.at[1], len(everyone))
    for d in (1, -1, 2):
        rows_x(d).start()
    w[1, rings.my_rows, at256(x * SEG)] = tmp[x]
    w_store(2, False).start()
    def oblk(k, s):
        return o_full.at[:, at256(k * 1024 + s * SEG)]

    def osend(di, k):
        ref = oblk(k, x)
        return remote(ref, ref, osd, orv.at[di, k], g.xdev(DIRS[di]))

    def ofwd(k, di):
        d = DIRS[di]
        ref = oblk(k, mod4(x - d))
        return remote(ref, ref, ofs, ofr.at[k], g.xdev(d))

    def attend(k):
        for ch in range(2):
            cols = at128(k * SEG + ch * 128)
            qh, kh, vh = acts[3, :, cols], acts[4, :, cols], acts[2, :, cols]
            for i in range(4):
                n = (i + 1) * 128
                s = causal_scores(kh[:n], qh[i * 128:n], i, n)
                e = jnp.exp(s - jnp.max(s, axis=0, keepdims=True))
                p_all[0:n, pl.ds(i * 128, 128)] = (e * (1.0 / jnp.sum(e, axis=0, keepdims=True))).astype(BF16)
            o = lax.dot_general(p_all[...], vh, TN, preferred_element_type=F32).astype(BF16)
            o_full[:, at128(k * 1024 + x * SEG + ch * 128)] = o
        for di in range(2):
            osend(di, k).start()

    def o_pair(s):
        for k in range(4):
            cols = at256(k * 1024 + s * SEG)
            remote(o_full.at[:, cols], x_full.at[:, cols], ops, opr, g.partner).start()

    def cols_items(lo, hi):
        loop(lo, hi, lambda it: rings.item(cols_m, it // 4, lax.rem(it, 4)))

    def o_forward(base):
        for i in range(2):
            osend(i, base + i).wait_recv()
            ofwd(base + i, i).start()

    own_k, pair_k = 2 * c, 2 * (1 - c)

    rest = w.at[1, rings.my_rows, pl.ds(0, 768)]

    def groups(half):
        @pl.when(half == 1)
        def _():
            remote(rest, rest, sc2s, sc2r, g.partner).wait_recv()
            rings.pair_send(rows_m).start()
            rings.pair_done(2)
            w_store(2, True).start()
        base = own_k + half * (pair_k - own_k)

        def one(i):
            chunk(2, half, i)
            attend(base + i)
            pl.when(jnp.logical_and(half == 1, i == 0))(lambda: rings.first(rows_m, True))

            @pl.when(half == 0)
            def _():
                @pl.when(i == 0)
                def _():
                    for u in range(3):
                        rings.second(cols_m, u, True)

            @pl.when(half == 1)
            def _():
                for r in range(2):
                    it = 2 * i + r
                    rings.item(cols_m, it // 4, lax.rem(it, 4))
        loop(0, 2, one)
    loop(0, 2, groups)
    cols_items(4, 8)
    o_forward(own_k)

    for u in range(3):
        rings.second(rows_m, u, True)
    cols_items(8, 12)
    o_forward(pair_k)
    rings.pair_done(cols_m)
    o_pair(x)

    def a_part(s, init=False):
        def step(i):
            cols = at256(i * SEG)
            acc = None
            for k in range(4):
                dot = jnp.dot(o_full[:, at256(k * 1024 + s * SEG)], w[0, at256(k * 1024 + s * SEG), cols], preferred_element_type=F32)
                acc = dot if acc is None else acc + dot
            a_acc[:, cols] = acc if init else a_acc[:, cols] + acc
        loop(0, 4, step)

    a_part(x, True)
    for k in range(4):
        osend(1 - k % 2, k).wait_recv()
    o_pair(mod4(x + 1))
    o_pair(mod4(x + 3))
    loop(0, 2, lambda i: a_part(mod4(x + 2 * i - 1)))
    rings.round(rows_m, 0)
    for k in range(4):
        ofwd(k, k % 2).wait_recv()
    a_part(mod4(x + 2))
    o_oth = x_full
    gy_mine, gy_rest = gyc.at[pl.ds(0, 128)], gyc.at[pl.ds(0, 384)]
    pltpu.make_async_copy(gy_mine, gy_mine, gls).wait()
    remote(gy_rest, gy_rest, gys, gyr, g.partner).wait()

    sq[...] = jnp.zeros((2, 512, 128), F32)

    def a_stats(h):
        cols = at128(h * 128)
        a = a_acc[:, cols].astype(BF16).astype(F32)
        gh = gyc[:, cols].astype(F32) * gains[2:3, cols]
        sq[0] = sq[0] + a * a
        sq[1] = sq[1] + gh * a
    loop(0, 8, a_stats)
    for i in range(2):
        stat2.put(i, sq[i])
    stat2.start()
    total2 = stat2.total()
    inv_a = inv_column(total2, 0)
    sq[0] = jnp.broadcast_to(inv_a, (512, 128))
    sq[1] = jnp.broadcast_to(total2.T[:, 1:2] * inv_a / 4096.0, (512, 128))

    def gblk(k, s):
        return ga_all.at[s, :, pl.ds(k * SEG, SEG)]

    def gsend(di, k):
        ref = gblk(k, x)
        return remote(ref, ref, gsd, grv.at[di, k], g.xdev(DIRS[di]))

    def gsend_start(di, k):
        for i in range(4):
            ref = ga_all.at[x, pl.ds(i * 128, 128), at256(k * SEG)]
            remote(ref, ref, gsd, grv.at[di, k], g.xdev(DIRS[di])).start()

    def gfwd(k):
        d = DIRS[k % 2]
        ref = gblk(k, mod4(x - d))
        return remote(ref, ref, gfs, gfr.at[k], g.xdev(d))

    theirs = pl.ds(pl.multiple_of((1 - c) * 512, 512), 512)
    mine = pl.ds(pl.multiple_of(c * 512, 512), 512)
    ga_pair = remote(ga_all.at[x, :, theirs], gtw.at[pl.ds(512, 512)], gps, gpr, g.partner)

    def send_grad_a(k):
        def step(i):
            cols = at128(k * SEG + i * 128)
            scale = sq[0]
            a_hat = a_acc[:, cols].astype(BF16).astype(F32) * scale
            ga_all[x, :, cols] = (scale * (gyc[:, cols].astype(F32) * gains[2:3, cols] - a_hat * sq[1])).astype(BF16)
        loop(0, 2, step)
        for di in range(2):
            gsend_start(di, k)
    loop(0, 4, send_grad_a)
    ga_pair.start()
    o_pair(mod4(x + 2))
    gtw[0:512] = ga_all[x, :, mine]
    def finish_y(h):
        cols = at128(h * 128)
        a_hat = a_acc[:, cols].astype(BF16).astype(F32) * sq[0]
        xcv[:, cols] = (xcv[:, cols].astype(F32) + a_hat * gains[2:3, cols]).astype(BF16)
        post[0:1, cols] = jnp.sum(gyc[:, cols].astype(F32) * a_hat, axis=0, keepdims=True)
    loop(0, 8, finish_y)
    y_store.start()
    remote(o_full, o_oth, ops, opr, g.partner).wait_recv()
    ga_pair.wait_recv()

    def slot(kk, t, jj):
        return (r1, wo_mid, wo_seg)[t].at[kk, jj]

    def send1(t, kk, jj):
        src = s0.at[kk, jj] if t == 0 else slot(kk, t - 1, jj)
        ss, rs = (wo_sent, wor.at[jj]) if t == 2 else (s1s.at[t], s1r.at[t, jj])
        return remote(src, slot(kk, t, jj), ss, rs, g.axis1(1 - 2 * kk))

    def tile(kk, tt, jj):
        d = 1 - 2 * kk
        cols = g.seg_rows(mod4(p1 - d * (1 + tt)), mod4(p2 - d * (1 + jj)))
        right = at256(kk * SEG)
        return (lax.dot_general(o_full[:, cols], gtw[0:512, right], TN, preferred_element_type=F32)
                + lax.dot_general(o_oth[:, cols], gtw[512:1024, right], TN, preferred_element_type=F32))

    def start_item(jj):
        def color(kk):
            s0[kk, jj] = tile(kk, 0, jj)
            send1(0, kk, jj).start()
        loop(0, 2, color)

    def ring_item(t, jj):
        ref = s0.at[0, pl.ds(0, 2)]
        remote(ref, ref, s1s.at[t], s1r.at[t, jj], g.partner).wait_recv()

        def color(kk):
            dst = slot(kk, t, jj)
            dst[...] = dst[...] + tile(kk, t + 1, jj)
            send1(t + 1, kk, jj).start()
        loop(0, 2, color)

    def last_tiles(jj):
        def color(kk):
            wo_add[kk, jj] = tile(kk, 3, jj)
        loop(0, 2, color)

    def g_forward(lo):
        for k in (lo, lo + 1):
            gsend(k % 2, k).wait_recv()
            gfwd(k).start()

    loop(0, 4, start_item)
    rings.round(rows_m, 1)
    rings.round(rows_m, 2)
    g_forward(0)
    loop(0, 2, lambda jj: ring_item(0, jj))
    g_forward(2)
    loop(2, 4, lambda jj: ring_item(0, jj))
    rings.pair_done(rows_m)

    def go_part(s, init=False):
        def step(zi):
            cols = at256(zi * SEG)
            acc = None
            for k in range(4):
                dot = lax.dot_general(ga_all[s, :, k * SEG:(k + 1) * SEG], w[1, at256(zi * 1024 + k * SEG), at256(s * SEG)],
                                      NT, preferred_element_type=F32)
                acc = dot if acc is None else acc + dot
            a_acc[:, cols] = acc if init else a_acc[:, cols] + acc
        loop(0, 4, step)

    go_part(x, True)
    for k in range(4):
        gsend(1 - k % 2, k).wait_recv()
    loop(0, 2, lambda i: go_part(mod4(x + 2 * i - 1)))
    remote(s0, s0, s1s.at[0], opr, g.partner).wait_send()
    loop(0, 4, last_tiles)
    loop(0, 4, lambda jj: ring_item(1, jj))

    @pl.when(y == x)
    def _():
        remote(gain_rest, gain_rest, g1s, g1r, g.partner).wait_send()
    remote(tmp3, tmp3, sc1s, sc1r, g.partner).wait_send()
    remote(rest, rest, sc2s, sc2r, g.partner).wait_send()
    for b in range(4):
        if b >= 2:
            xt_pair(b).wait_send()
            xt_store(b).wait()
        xt_pair(b).wait_recv()
    w_store(2, False).wait()
    w_store(2, True).wait()
    y_store.wait()
    remote(o_full, o_oth, ops, opr, g.partner).wait_send()
    ga_pair.wait_send()
    both = ga_all.at[pl.ds(0, 2)]
    one = ga_all.at[0]
    remote(both, both, osd, opr, g.partner).wait_send()
    remote(both, both, gsd, opr, g.partner).wait_send()
    remote(one, one, ofs, opr, g.partner).wait_send()
    for m in (2, cols_m, rows_m):
        rings.drain(m)
    for k in range(4):
        gfwd(k).wait_recv()
    go_part(mod4(x + 2))

    def keep_grad_o(h):
        cols = at128(h * 128)
        acts[5, :, cols] = a_acc[:, cols].astype(BF16)
    loop(0, 8, keep_grad_o)

    remote(one, one, gfs, opr, g.partner).wait_send()
    remote(s0, s0, s1s.at[1], opr, g.partner).wait_send()


FORWARD_SCRATCH = [
    pltpu.VMEM((3, 4096, 1024), BF16),
    pltpu.VMEM((512, 4096), BF16),
    pltpu.VMEM((2, 1024, 512), BF16),
    pltpu.VMEM((512, 1024), BF16),
    pltpu.VMEM((512, 1024), BF16),
    pltpu.VMEM((8, 128), F32),
    pltpu.VMEM((512, 1024), F32),
    pltpu.VMEM((512, 4096), BF16),
    pltpu.VMEM((4, 512, 1024), BF16),
    pltpu.VMEM((1024, 512), BF16),
    pltpu.VMEM((2, 512, 128), F32),
    pltpu.VMEM((4, 8, 512), F32),
    pltpu.VMEM((4, 8, 512), F32),
    pltpu.VMEM((2, 4, SEG, SEG), F32),
    pltpu.VMEM((512, 512), BF16),
    pltpu.VMEM((4, 128, SEG), BF16),
    DMA((4,)), DMA(()), DMA(()), DMA((2, 4)), DMA(()), DMA((4,)),
    DMA(()), DMA(()), DMA(()), DMA((3,)), DMA((3,)), DMA((3,)), DMA((3,)),
    DMA((3, 2)), DMA((4,)), DMA((4,)), DMA((4,)), DMA(()),
    DMA(()), DMA(()), DMA(()), DMA(()), DMA(()), DMA(()), pltpu.SemaphoreType.REGULAR((2,)),
    DMA(()), DMA(()), DMA(()), DMA(()), DMA(()), DMA(()), DMA((2, 4)), DMA(()), DMA((4,)), DMA(()), DMA(()),
    DMA(()), DMA((2, 4)), DMA(()), DMA((4,)), DMA(()), DMA(()),
    DMA((2,)), DMA((2, 4)),
] + ring_sems(3)


NU = 4
WO = 4


def backward_phase(io, keep, r1, r1h, r2, r2h, rg, buf, dall, rt, lt, gxc, p_all, ds_all, lanes, st, ge, gy, gxo,
            s1s, s1t, s1r, s2s, s2r, ags, agr, agx, d2s, d2r, fws, fwr, lws, lts, gs, gr, gls, wls, gxs, gyl, dps, dpr, sts, strv,
            e1s, e1r, e2s, e2r, e3s, e3r, e4s):
    gy_in, cos_tab, sin_tab, wq, wk, wv, x_t, y_cols, dwv, dwk, dwq, dwo, y_out, gx_part, gx_out, gain_out = io
    acts, gains, stats, post, wo_seg, wo_add, wo_mid, wor, wo_sent, inside, ysd, yrv, yst, e4r = keep
    s0 = wo_add
    outs = (dwv, dwk, dwq, dwq, dwo)
    widths = (SEG, SEG, 128, 128, SEG)
    shifts = (0, 0, 0, 128, 0)
    weights = (wv, wk, wq)
    g = Torus()
    x, z, y, c, p1, p2 = g.x, g.z, g.y, g.c, g.p1, g.p2
    peers = ([(x, mod4(z + d), y, c) for d in (1, 2, 3)] + [(x, z, mod4(y + d), c) for d in (1, 2, 3)]
             + [g.partner, g.xdev(2)] + [g.xdev(d, h) for d in DIRS for h in (0, 1)])
    for peer in peers:
        pl.semaphore_signal(inside, inc=1, device_id=peer, device_id_type=MESH_ID)

    def block(kk, tt, jj):
        d = 1 - 2 * kk
        return g.seg_rows(mod4(p1 - d * (1 + tt)), mod4(p2 - d * (1 + jj)))

    def aload(n, kk):
        par = lax.rem(n, 2)
        return pltpu.make_async_copy(x_t.at[block(kk, 1 + n // 4, lax.rem(n, 4))], lt.at[0, par, kk], lts.at[0, par])

    def bload(jj, kk):
        par = lax.rem(jj, 2)
        return pltpu.make_async_copy(x_t.at[block(kk, 0, jj)], lt.at[1, par, kk], lts.at[1, par])

    def load_wait(kind, par):
        pltpu.make_async_copy(lt.at[kind, par], lt.at[kind, par], lts.at[kind, par]).wait()

    def tile(kind, m, par, kk):
        cols = pl.ds(pl.multiple_of(kk * SEG + shifts[m], 128), widths[m])
        return jnp.dot(lt[kind, par, kk], rt[min(m, 2), :, cols], preferred_element_type=F32)

    def slot(m, kk, t, jj):
        if m == WO:
            return wo_seg.at[kk, jj]
        return r1.at[m, kk, t, jj] if m < 2 else r1h.at[m - 2, kk, t, jj]

    def slot2(m, kk, u):
        return r2h.at[m - 2, kk, u] if m in (2, 3) else r2.at[min(m, 2), kk, u]

    def first_slot(m, kk, jj):
        return s0.at[kk, jj, :, pl.ds(shifts[m], widths[m])]

    def send1(m, t, kk, jj, first=False):
        src = first_slot(m, kk, jj) if first else slot(m, kk, t - 1, jj)
        ss = s1s.at[m, jj] if first and m < 2 else s1t.at[m]
        return remote(src, slot(m, kk, t, jj), ss, s1r.at[m, t, jj], g.axis1(1 - 2 * kk))

    def recv1(m, t, jj):
        ref = r1.at[0, 0, 0, pl.ds(0, 2)] if m < 2 else r1h.at[0, 0, 0, pl.ds(0, 2)]
        remote(ref, ref, s1t.at[0], s1r.at[m, t, jj], g.partner).wait_recv()

    def send2(m, u, kk):
        return remote(slot(m, kk, 2, u), slot2(m, kk, u), s2s.at[m], s2r.at[m, u], g.axis2(DIRS[kk]))

    def start_item(m, jj):
        load_wait(1, lax.rem(jj, 2))
        if m in (1, 2):
            ref = s0.at[0, pl.ds(0, 2)]
            remote(ref, ref, s1s.at[m - 1, jj], s2r.at[0, 0], g.partner).wait_send()

        def color(kk):
            first_slot(m, kk, jj)[...] = tile(1, m, lax.rem(jj, 2), kk)
            send1(m, 0, kk, jj, True).start()
        loop(0, 2, color)
        for kk in range(2):
            pl.when(jj < 2)(lambda: bload(jj + 2, kk).start())
            if m + 1 < NU:
                pl.when(jj >= 2)(lambda: bload(jj - 2, kk).start())

    def ring_item(m, n):
        t, jj = n // 4, lax.rem(n, 4)
        load_wait(0, lax.rem(n, 2))
        recv1(m, t, jj)

        def color(kk):
            ref = slot(m, kk, t, jj)
            ref[...] = ref[...] + tile(0, m, lax.rem(n, 2), kk)
            pl.when(t < 2)(lambda: send1(m, t + 1, kk, jj).start())
        loop(0, 2, color)
        for kk in range(2):
            pl.when(n < 10)(lambda: aload(n + 2, kk).start())
            if m + 1 < NU:
                pl.when(n >= 10)(lambda: aload(n - 10, kk).start())

    def wo_item(jj):
        ref = s0.at[0, pl.ds(0, 2)]
        remote(ref, ref, s1t.at[0], wor.at[jj], g.partner).wait_recv()

        def color(kk):
            wo_seg[kk, jj] = wo_seg[kk, jj] + wo_add[kk, jj]
        loop(0, 2, color)

    def out_cols(k, xs, m=0):
        return pl.ds(pl.multiple_of(k * 1024 + xs * SEG + shifts[m], 128), widths[m])

    def ag_send(m, kk, di, h):
        k = 2 * c + kk
        return remote(slot(m, kk, 2, 3).at[pl.ds(h * 128, 128)], outs[m].at[:, out_cols(k, x, m)], ags.at[m],
                      agr.at[m, di] if di == kk else agx.at[m],
                      g.xdev(DIRS[di], h))

    def pair_send(m, kk):
        src = slot(m, kk, 2, 3).at[at128((1 - c) * 128)]
        return remote(src, outs[m].at[:, out_cols(2 * c + kk, x, m)], d2s.at[m], d2r.at[m], g.partner)

    def own_store(m, kk):
        return pltpu.make_async_copy(slot(m, kk, 2, 3).at[at128(c * 128)], outs[m].at[:, out_cols(2 * c + kk, x, m)], lws.at[m])

    def forward(m, k):
        di = k % 2
        ref = outs[m].at[:, out_cols(k, mod4(x - DIRS[di]), m)]
        return remote(ref, ref, fws.at[m], fwr.at[m], g.xdev(DIRS[di]))

    def hand_out(m, kk):
        own_store(m, kk).start()
        for di in range(2):
            for h in range(2):
                ag_send(m, kk, di, h).start()
        pair_send(m, kk).start()

    def phase2(m, u):
        if u > 0:
            ref = r2h.at[0, 0, pl.ds(0, 2)] if m in (2, 3) else r2.at[0, 0, pl.ds(0, 2)]
            remote(ref, ref, s2s.at[m], s2r.at[m, u - 1], g.partner).wait_recv()
        for kk in range(2):
            if u > 0:
                ref = slot(m, kk, 2, u)
                ref[...] = ref[...] + slot2(m, kk, u - 1)[...]
            if u < 3:
                send2(m, u, kk).start()
            else:
                hand_out(m, kk)

    def direct2(m, u, kk):
        return remote(slot(m, kk, 2, u), slot2(m, kk, u), s2s.at[m], s2r.at[m, u], g.axis2(-(1 + u) * DIRS[kk]))

    def last_phase2(m):
        for u in range(3):
            ref = r2h.at[0, 0, pl.ds(0, 2)]
            remote(ref, ref, s2s.at[m], s2r.at[m, u], g.partner).wait_recv()
        for kk in range(2):
            ref = slot(m, kk, 2, 3)
            ref[...] = (ref[...] + slot2(m, kk, 0)[...]) + (slot2(m, kk, 1)[...] + slot2(m, kk, 2)[...])
            hand_out(m, kk)

    def do_forward(m):
        for di in range(2):
            ref = outs[m].at[:, pl.ds(0, 2 * widths[m])]
            remote(ref, ref, ags.at[m], agr.at[m, di], g.partner).wait_recv()
            for k in (di, di + 2):
                forward(m, k).start()

    def bytes_of(m, n, ss, rs):
        ref = outs[m].at[:, pl.ds(0, n * widths[m])]
        return remote(ref, ref, ss, rs, g.partner)

    def drain_slots(m):
        if m != WO:
            ref = r1.at[m, pl.ds(0, 2), pl.ds(0, 2)] if m < 2 else r1h.at[0]
            remote(ref, ref, s1t.at[m], d2r.at[m], g.partner).wait_send()
        bytes_of(m, 12, s2s.at[m], d2r.at[m]).wait_send()
        bytes_of(m, 8, ags.at[m], agx.at[m]).wait_send()
        bytes_of(m, 2, d2s.at[m], d2r.at[m]).wait_send()
        ref = outs[m].at[:, pl.ds(0, 2 * widths[m])]
        pltpu.make_async_copy(ref, ref, lws.at[m]).wait()

    def drain_unit(m):
        drain_slots(m)
        bytes_of(m, 4, ags.at[m], agx.at[m]).wait_recv()
        bytes_of(m, 2, d2s.at[m], d2r.at[m]).wait_recv()
        bytes_of(m, 4, fws.at[m], fwr.at[m]).wait()

    def gcols(kk, jj):
        return pl.ds(pl.multiple_of(kk * 2048 + jj * 512, 512), 512)

    def gsend(t, kk, jj):
        d = DIRS[kk]
        if t == 0:
            src = gx_part.at[at128(mod4(x - d) * 128), gcols(kk, jj)]
        else:
            src = rg.at[kk, t - 1, jj]
        return remote(src, rg.at[kk, t, jj], gs, gr.at[t, jj], g.xdev(d))

    def gbuf(t, kk, jj):
        return (t % 2, at128(jj * 128), pl.ds(kk * 512, 512))

    def gload(t, kk, jj):
        src = gx_part.at[at128(mod4(x - DIRS[kk] * (2 + t)) * 128), gcols(kk, jj)]
        return pltpu.make_async_copy(src, buf.at[gbuf(t, kk, jj)], gls.at[t % 2, jj])

    def gloads(t):
        each(lambda kk, jj: gload(t, kk, jj).start())

    def chunk_rows(e):
        return pl.ds(pl.multiple_of((lax.rem(e, 2) * 4 + e // 2) * 512, 512), 512)

    def wload(e, i):
        par = lax.rem(e, 2)
        return pltpu.make_async_copy(weights[i].at[chunk_rows(e)], acts.at[3 * par + i], wls.at[par])

    def gx_store(e):
        par = lax.rem(e, 2)
        return pltpu.make_async_copy(gxc.at[par], gx_part.at[:, chunk_rows(e)], gxs.at[par])

    def gx_ship(e, kk):
        gx_store(e).wait()
        gsend(0, kk, e // 2).start()

    def gx_chunk(e):
        par = lax.rem(e, 2)
        ref = acts.at[pl.ds(0, 3)]
        pltpu.make_async_copy(ref, ref, wls.at[par]).wait()

        def rows_half(r):
            rows = at256(r * SEG)
            acc = None
            for i in range(3):
                dot = lax.dot_general(dall[i, rows, :], acts[3 * par + i], NT, preferred_element_type=F32)
                acc = dot if acc is None else acc + dot
            gxc[par, rows, :] = acc
        loop(0, 2, rows_half)
        gx_store(e).start()

        @pl.when(e < 6)
        def _():
            for i in range(3):
                wload(e + 2, i).start()
        for kk in range(2):
            pl.when(jnp.logical_and(e > 0, lax.rem(e, 2) == 1 - kk))(lambda: gx_ship(e - 1, kk))

    gx_save = pltpu.make_async_copy(gxo, gx_out, gyl)

    def gx_item(t, jj):
        ref = rg.at[0, 0, pl.ds(0, 2)]
        remote(ref, ref, gs, gr.at[t, jj], g.partner).wait_recv()
        pltpu.make_async_copy(ref, ref, gls.at[t % 2, jj]).wait()
        for kk in range(2):
            total = rg[kk, t, jj] + buf[gbuf(t, kk, jj)]
            if t < 2:
                rg[kk, t, jj] = total
                gsend(t + 1, kk, jj).start()
            else:
                gxo[:, gcols(kk, jj)] = (total + gy[:, gcols(kk, jj)].astype(F32)).astype(BF16)

    def y_send(i, k):
        d = (1, -1, 2)[i]
        src = y_cols.at[at128(mod4(x + d) * 128), pl.ds(k * SEG, SEG)]
        return remote(src, y_out.at[:, out_cols(k, x)], ysd, yrv, g.xdev(d))

    def y_own(k):
        return pltpu.make_async_copy(y_cols.at[at128(x * 128), pl.ds(k * SEG, SEG)], y_out.at[:, out_cols(k, x)], yst)

    gain1 = remote(ge.at[0], ge.at[1], e1s, e1r, g.partner)

    def gain2(d):
        return remote(ge.at[8], ge.at[1 + d], e2s.at[d - 1], e2r.at[d - 1], (x, mod4(z + d), y, c))

    def gain3(d):
        return remote(ge.at[9], ge.at[4 + d], e3s.at[d - 1], e3r.at[d - 1], (x, z, mod4(y + d), c))

    my_head = at128(z * SEG + c * 128)

    def gain4(d):
        return remote(ge.at[10, :, my_head], gain_out, e4s.at[d - 1], e4r, g.xdev(d))

    gy_load = pltpu.make_async_copy(gy_in, gy, gyl)
    stat = StatExchange(g, st, sts, strv)
    theirs = pl.ds(pl.multiple_of((1 - c) * 512, 512), 512)
    mine = pl.ds(pl.multiple_of(c * 512, 512), 512)

    def swap(i):
        return remote(dall.at[i, :, theirs], rt.at[i, pl.ds(512, 512)], dps.at[i], dpr.at[i], g.partner)

    def share(i):
        rt[i, 0:512] = dall[i, :, mine]
        swap(i).start()

    gy_load.start()
    for k in range(4):
        for i in range(3):
            y_send(i, k).start()
        y_own(k).start()
    for kk in range(2):
        for jj in range(2):
            bload(jj, kk).start()
            aload(jj, kk).start()
    inv = [gxc.at[0, :, pl.ds(i * 128, 128)] for i in range(2)]
    proj = [gxc.at[1, :, pl.ds(i * 128, 128)] for i in range(2)]
    for i in range(2):
        inv[i][...] = jnp.broadcast_to(inv_column(stats[...], i), (512, 128))
    lanes[...] = jnp.zeros((2, 512, 128), F32)
    st[0] = jnp.zeros((8, 512), F32)
    ge[0] = jnp.zeros((8, 1024), F32)
    ge[0, 2:3] = post[...]

    p_all[...] = jnp.zeros((512, 512), BF16)
    ds_all[...] = jnp.zeros((512, 512), BF16)

    def norm_back(i, src_rows, cols, gn):
        hat = acts[i, src_rows, cols].astype(F32) * inv[i][src_rows, :]
        prod = gn * hat
        gain = gains[i:i + 1, cols]
        buf[i, src_rows, cols] = gn * gain
        lanes[i, src_rows] = lanes[i, src_rows] + prod * gain
        return jnp.sum(prod, axis=0, keepdims=True)

    def head(h):
        cols = at128(h * 128)
        vh, qh, kh, do = (acts[i, :, cols] for i in (2, 3, 4, 5))
        for i in range(4):
            n = (i + 1) * 128
            block_i = pl.ds(i * 128, 128)
            s = causal_scores(kh[:n], qh[i * 128:n], i, n)
            e = jnp.exp(s - jnp.max(s, axis=0, keepdims=True))
            p = e * (1.0 / jnp.sum(e, axis=0, keepdims=True))
            dp = lax.dot_general(vh[:n], do[i * 128:n], NT, preferred_element_type=F32)
            p_all[0:n, block_i] = p.astype(BF16)
            ds_all[0:n, block_i] = (p * (dp - jnp.sum(p * dp, axis=0, keepdims=True)) * SCALE).astype(BF16)
        dall[0, :, cols] = jnp.dot(p_all[...], do, preferred_element_type=F32).astype(BF16)
        dq = lax.dot_general(ds_all[...], kh, TN, preferred_element_type=F32)
        dk = jnp.dot(ds_all[...], qh, preferred_element_type=F32)
        for i, grad in ((0, dq), (1, dk)):
            ge[0, i:i + 1, cols] = norm_back(i, pl.ds(0, 512), cols, rope_turn(grad, cos_tab[...], -sin_tab[...]))

    def finish(i, m, column):
        proj[i][...] = jnp.broadcast_to(column, (512, 128))

        def step(h):
            cols = at128(h * 128)
            scale = inv[i][...]
            hat = acts[i, :, cols].astype(F32) * scale
            dall[m, :, cols] = (scale * (buf[i, :, cols] - hat * proj[i][...])).astype(BF16)
        loop(0, 8, step)

    def head_step(i):
        head(i)

        @pl.when(i == 2)
        def _():
            pl.semaphore_wait(inside, len(peers))
            wo_item(0)
            phase2(WO, 0)

        @pl.when(i == 4)
        def _():
            wo_item(1)
            phase2(WO, 1)

        @pl.when(i == 7)
        def _():
            wo_item(2)
            phase2(WO, 2)
    loop(0, 8, head_step)
    share(0)
    for i in range(2):
        stat.put(i, lanes[i])
    stat.start()
    gain1.start()
    wo_item(3)
    swap(0).wait_recv()
    loop(0, 4, lambda jj: start_item(0, jj))
    total = stat.total().T / 4096.0
    finish(1, 1, total[:, 1:2])
    share(1)
    finish(0, 2, total[:, 0:1])
    share(2)
    for e in range(2):
        for i in range(3):
            wload(e, i).start()
    phase2(WO, 3)
    gy_load.wait()

    for m in range(NU):
        def early(n, m=m):
            ring_item(m, n)
            if m > 0:
                pl.when(n == 0)(lambda: phase2(m - 1, 2))
                pl.when(n == 2)(lambda: phase2(m - 1, 3))
            if m == 0:
                gx_chunk(n)
            elif m == 1:
                pl.when(n >= 4)(lambda: gx_item(1, n - 4))

        loop(0, 8, early)
        if m == 0:
            gx_ship(7, 1)
            gloads(0)
            gloads(1)
            do_forward(WO)
            gain1.wait_recv()
            ge[8] = ge[0] + ge[1]
            for d in (1, 2, 3):
                gain2(d).start()
            swap(1).wait_recv()
            swap(2).wait_recv()
        if m == 1:
            for d in (1, 2, 3):
                gain2(d).wait_recv()
            ge[9] = (ge[8] + ge[2]) + (ge[3] + ge[4])
            for d in (1, 2, 3):
                gain3(d).start()
        if m == 3:
            gx_save.start()
            do_forward(1)
        if m == 2:
            for d in (1, 2, 3):
                gain3(d).wait_recv()
            ge[10] = (ge[9] + ge[5]) + (ge[6] + ge[7])

            @pl.when(y == x)
            def _():
                gain_out[...] = ge[10, :, my_head]
                for d in (1, 2, 3):
                    gain4(d).start()

        def late(n, m=m):
            if m + 1 < NU:
                start_item(m + 1, n - 8)
            ring_item(m, n)
            if m < 3:
                pl.when(n == 8)(lambda: phase2(m, 0))
                pl.when(n == 10)(lambda: phase2(m, 1))
            else:
                for u in range(3):
                    for kk in range(2):
                        pl.when(n == 8 + u)(lambda: direct2(m, u, kk).start())
            if m in (0, 2):
                gx_item(m, n - 8)

        loop(8, 12, late)
        if m == 0:
            gloads(2)
        if m == 1:
            do_forward(0)
        if m == 3:
            do_forward(2)
    last_phase2(NU - 1)
    do_forward(NU - 1)

    remote(wo_mid, wo_mid, wo_sent, yrv, g.partner).wait_send()
    @pl.when(y == x)
    def _():
        for d in (1, 2, 3):
            gain4(d).wait_send()

    @pl.when(y != x)
    def _():
        gain4(1).wait_recv()
    gain1.wait_send()
    for d in (1, 2, 3):
        gain2(d).wait_send()
        gain3(d).wait_send()
    y_all, y_mine = y_out.at[:, pl.ds(0, 3072)], y_out.at[:, pl.ds(0, 1024)]
    remote(y_all, y_all, ysd, yrv, g.partner).wait()
    pltpu.make_async_copy(y_mine, y_mine, yst).wait()
    for m in range(NU + 1):
        drain_unit(m)
    most = gx_part.at[:, pl.ds(0, 3072)]
    remote(most, most, gs, gr.at[0, 0], g.partner).wait_send()
    for i in range(3):
        swap(i).wait_send()
    gx_save.wait()


BACKWARD_SCRATCH = [
    pltpu.VMEM((2, 2, 3, 4, SEG, SEG), F32),
    pltpu.VMEM((2, 2, 3, 4, SEG, 128), F32),
    pltpu.VMEM((3, 2, 3, SEG, SEG), F32),
    pltpu.VMEM((2, 2, 3, SEG, 128), F32),
    pltpu.VMEM((2, 3, 4, 128, 512), F32),
    pltpu.VMEM((2, 512, 1024), F32),
    pltpu.VMEM((3, 512, 1024), BF16),
    pltpu.VMEM((3, 1024, 512), BF16),
    pltpu.VMEM((2, 2, 2, SEG, 1024), BF16),
    pltpu.VMEM((2, 512, 512), F32),
    pltpu.VMEM((512, 512), BF16),
    pltpu.VMEM((512, 512), BF16),
    pltpu.VMEM((2, 512, 128), F32),
    pltpu.VMEM((4, 8, 512), F32),
    pltpu.VMEM((11, 8, 1024), F32),
    pltpu.VMEM((128, 4096), BF16),
    pltpu.VMEM((128, 4096), BF16),
    DMA((2, 4)), DMA((NU,)), DMA((NU, 3, 4)), DMA((NU + 1,)), DMA((NU + 1, 3)),
    DMA((NU + 1,)), DMA((NU + 1, 2)), DMA((NU + 1,)), DMA((NU + 1,)), DMA((NU + 1,)), DMA((NU + 1,)), DMA((NU + 1,)), DMA((NU + 1,)),
    DMA((2, 2)), DMA(()), DMA((3, 4)), DMA((2, 4)), DMA((2,)), DMA((2,)), DMA(()),
    DMA((3,)), DMA((3,)), DMA((3,)), DMA((3,)),
    DMA(()), DMA(()), DMA((3,)), DMA((3,)), DMA((3,)), DMA((3,)), DMA((3,)),
]


def layer_kernel(wq_in, wk_in, wv_in, wo_in, x_in, gy_in, gq_in, gk_in, gp_in, cos_tab, sin_tab,
                 dwv, dwk, dwq, dwo, y_out, gx_out, wq_out, wk_out, wv_out, x_t, y_cols, gx_part, gain_out,
                 acts, gains, stats, post, wo_seg, wo_add, wo_mid, wor, wo_sent, inside, ysd, yrv, yst, e4r):
    keep = (acts, gains, stats, post, wo_seg, wo_add, wo_mid, wor, wo_sent)
    first = (wq_in, wk_in, wv_in, wo_in, x_in, gy_in, gq_in, gk_in, gp_in, cos_tab, sin_tab, wq_out, wk_out, wv_out, x_t, y_cols)
    second = (gy_in, cos_tab, sin_tab, wq_out, wk_out, wv_out, x_t, y_cols, dwv, dwk, dwq, dwo, y_out, gx_part, gx_out, gain_out)
    pl.run_scoped(lambda *refs: forward_phase(first, keep, *refs), *FORWARD_SCRATCH)
    pl.run_scoped(lambda *refs: backward_phase(second, keep + (inside, ysd, yrv, yst, e4r), *refs), *BACKWARD_SCRATCH)


def layer(w_q, w_k, w_v, w_o, x_tok, gy_tok, gq, gk, gp, cos_tab, sin_tab):
    grad, tok, mat = SDS((128, 4096), F32), SDS((128, 4096), BF16), SDS((4096, 1024), BF16)
    return pl.pallas_call(
        layer_kernel,
        out_shape=[grad] * 4 + [tok] * 2 + [mat] * 4 + [SDS((512, 1024), BF16), SDS((512, 4096), F32), SDS((8, 128), F32)],
        in_specs=[IN_HBM] * 6 + [IN_VMEM] * 5,
        out_specs=[IN_HBM] * 12 + [IN_VMEM],
        scratch_shapes=[
            pltpu.VMEM((6, 512, 1024), BF16),
            pltpu.VMEM((8, 1024), F32),
            pltpu.VMEM((8, 512), F32),
            pltpu.VMEM((1, 1024), F32),
            pltpu.VMEM((2, 4, SEG, SEG), F32),
            pltpu.VMEM((2, 4, SEG, SEG), F32),
            pltpu.VMEM((2, 4, SEG, SEG), F32),
            DMA((4,)), DMA(()), pltpu.SemaphoreType.REGULAR, DMA(()), DMA(()), DMA(()), DMA(()),
        ],
        compiler_params=params(5, 63.9), cost_estimate=COST, name='layer',
    )(w_q, w_k, w_v, w_o, x_tok, gy_tok, gq, gk, gp, cos_tab, sin_tab)


def copy_kernel(*refs):
    n = (len(refs) - 7) // 5
    gain_src, gain_dst, gain_buf, gain_sems = refs[n], refs[2 * n + 1:2 * n + 4], refs[3 * n + 4], refs[5 * n + 5:]
    srcs, dsts, bufs = refs[:n], refs[n + 1:2 * n + 1], refs[2 * n + 4:3 * n + 4]
    loads, stores = refs[3 * n + 5:4 * n + 5], refs[4 * n + 5:5 * n + 5]
    parts = 4

    def rows(i, p):
        step = srcs[i].shape[0] // parts
        return pl.ds(p * step, step)

    def load(i, p):
        return pltpu.make_async_copy(srcs[i].at[rows(i, p)], bufs[i].at[rows(i, p)], loads[i].at[p])

    def store(i, p):
        return pltpu.make_async_copy(bufs[i].at[rows(i, p)], dsts[i].at[rows(i, p)], stores[i].at[p])

    gain_load = pltpu.make_async_copy(gain_src, gain_buf, gain_sems[0])
    gain_stores = [pltpu.make_async_copy(gain_buf.at[pl.ds(i, 1)], gain_dst[i], gain_sems[1].at[i]) for i in range(3)]
    order = [(i, p) for i in range(n) for p in range(parts)]
    gain_load.start()
    for i, p in order:
        load(i, p).start()
    gain_load.wait()
    for copy in gain_stores:
        copy.start()
    for i, p in order:
        load(i, p).wait()
        store(i, p).start()
    for i, p in order:
        store(i, p).wait()
    for copy in gain_stores:
        copy.wait()


def copy_out(gains, *arrays):
    n = len(arrays)
    return pl.pallas_call(
        copy_kernel,
        out_shape=[SDS(a.shape, a.dtype) for a in arrays] + [SDS((1, 128), F32)] * 3,
        in_specs=[IN_HBM] * (n + 1),
        out_specs=[IN_HBM] * (n + 3),
        scratch_shapes=[pltpu.VMEM(a.shape, a.dtype) for a in arrays] + [pltpu.VMEM((8, 128), F32)] + [DMA((4,))] * (2 * n) + [DMA(()), DMA((3,))],
        compiler_params=pltpu.CompilerParams(vmem_limit_bytes=63 * 1024 * 1024), cost_estimate=COST, name='copy_out',
    )(*arrays, gains)


def solution(mesh):
    mesh4 = Mesh(mesh.devices.reshape(4, 4, 4, 2), ('sp', 'z', 'y', 'c'))
    tok_spec = P(FS, 'sp', None)
    row_spec = P(FS, None)
    vec_spec = P(FS)

    def local_step(x, grad_y, wq_rows, wk_rows, wv_rows, wo_rows, gq_rows, gk_rows, gpost_rows):
        x_tok, gy_tok = x[0], grad_y[0]
        cos_tab, sin_tab = rope_tables(4 * x_tok.shape[0])
        dwv, dwk, dwq, dwo, y, grad_x, *_, gn = layer(
            wq_rows, wk_rows, wv_rows, wo_rows, x_tok, gy_tok, gq_rows[None], gk_rows[None], gpost_rows[None], cos_tab, sin_tab)
        dwv, dwk, dwq, dwo, y, grad_x, *gn = copy_out(gn, dwv, dwk, dwq, dwo, y, grad_x)
        return y[None], grad_x[None], dwq, dwk, dwv, dwo, gn[0][0], gn[1][0], gn[2][0]

    return jax.shard_map(local_step, mesh=mesh4,
                         in_specs=(tok_spec, tok_spec, row_spec, row_spec, row_spec, row_spec, vec_spec, vec_spec, vec_spec),
                         out_specs=(tok_spec, tok_spec, row_spec, row_spec, row_spec, row_spec, vec_spec, vec_spec, vec_spec),
                         check_vma=False)
```

```python
import jax
import jax.numpy as jnp
import numpy as np
from jax import lax
from jax.experimental import pallas as pl
from jax.experimental.pallas import tpu as pltpu
from jax.sharding import Mesh, PartitionSpec as P

HEAD_DIM = 128
RMS_EPSILON = 1e-6
ROPE_THETA = 500000.0
FS = ('z', 'y', 'c')
F32 = jnp.float32
BF16 = jnp.bfloat16
MESH_ID = pl.DeviceIdType.MESH
HBM = pl.ANY
SEG = 256


def rope_tables(seq_len):
    half_dim = HEAD_DIM // 2
    angles = np.arange(seq_len)[:, None] * ROPE_THETA ** (-np.arange(half_dim) * (2.0 / HEAD_DIM))[None, :]
    cos_half, sin_half = np.cos(angles), np.sin(angles)
    tables = np.concatenate([cos_half, cos_half], axis=1), np.concatenate([-sin_half, sin_half], axis=1)
    return tuple(jnp.asarray(t, F32) for t in tables)


def coords():
    return tuple(lax.axis_index(n) for n in ('sp', 'z', 'y', 'c'))


def mod4(v):
    return lax.rem(v + 8, 4)


def remote(src, dst, ss, rs, dev):
    return pltpu.make_async_remote_copy(src_ref=src, dst_ref=dst, send_sem=ss, recv_sem=rs, device_id=dev, device_id_type=MESH_ID)


def at256(v):
    return pl.ds(pl.multiple_of(v, SEG), SEG)


def at128(v):
    return pl.ds(pl.multiple_of(v, 128), 128)


def each(fn, n=4):
    def step(jj, carry):
        for kk in range(2):
            fn(kk, jj)
        return carry
    lax.fori_loop(0, n, step, 0)


def loop(lo, hi, fn):
    def step(n, carry):
        fn(n)
        return carry
    lax.fori_loop(lo, hi, step, 0)


def greet(peers):
    barrier = pltpu.get_barrier_semaphore()
    for peer in peers:
        pl.semaphore_signal(barrier, inc=1, device_id=peer, device_id_type=MESH_ID)
    return lambda: pl.semaphore_wait(barrier, len(peers))


class Torus:
    def __init__(self):
        self.x, self.z, self.y, self.c = x, z, y, c = coords()
        self.p1 = (1 - c) * y + c * z
        self.p2 = (1 - c) * z + c * y
        self.partner = (x, z, y, 1 - c)

    def axis1(self, d):
        return (self.x, mod4(self.z + d * self.c), mod4(self.y + d * (1 - self.c)), self.c)

    def axis2(self, d):
        return (self.x, mod4(self.z + d * (1 - self.c)), mod4(self.y + d * self.c), self.c)

    def xdev(self, d, core=None):
        return (mod4(self.x + d), self.z, self.y, self.c if core is None else core)

    def seg_rows(self, b, j):
        zz = (1 - self.c) * j + self.c * b
        yy = (1 - self.c) * b + self.c * j
        return at256(zz * 1024 + yy * SEG)


DIRS = (1, -1)
RING_SEMS = 8


def ring_sems(nw):
    dma = pltpu.SemaphoreType.DMA
    return [dma((nw,)), dma((nw,)), dma((nw,)), dma((nw, 3)), dma((nw,)), dma((nw, 3, 4)), dma((nw,)), dma((nw,))]


class WeightRings:
    def __init__(self, g, w, slots, sems):
        self.g, self.w, self.slots = g, w, slots
        self.d0s, self.d0r, self.a1s, self.a1r, self.a2s, self.a2r, self.f3s, self.f3r = sems
        self.my_rows = at128(g.z * 1024 + g.y * SEG + g.c * 128)

    def pair_send(self, m):
        ref = self.w.at[self.slots[m], self.my_rows]
        return remote(ref, ref, self.d0s.at[self.slots[m]], self.d0r.at[self.slots[m]], self.g.partner)

    def same(self, m, kk, rows, ss, rs, dev):
        ref = self.w.at[self.slots[m], rows, at256((2 * self.g.c + kk) * SEG)]
        return remote(ref, ref, ss, rs, dev)

    def bulk(self, m, n, ss, rs):
        ref = self.w.at[self.slots[m], pl.ds(0, n * 128), pl.ds(0, 512)]
        return remote(ref, ref, ss, rs, self.g.partner)

    def send1(self, m, u, kk):
        g, d = self.g, DIRS[kk]
        return self.same(m, kk, g.seg_rows(g.p1, mod4(g.p2 - d * u)), self.a1s.at[self.slots[m]], self.a1r.at[self.slots[m], u], g.axis2(d))

    def far1(self, m, e, kk):
        g = self.g
        rows = g.seg_rows(g.p1, g.p2)
        return self.same(m, kk, rows, self.a1s.at[self.slots[m]], self.a1r.at[self.slots[m], e - 1], g.axis2(DIRS[kk] * e))

    def fwd1(self, m, u, kk):
        g = self.g
        rows = g.seg_rows(g.p1, mod4(g.p2 - DIRS[kk] * (u + 1)))
        return self.same(m, kk, rows, self.f3s.at[self.slots[m]], self.f3r.at[self.slots[m]], g.partner)

    def send2(self, m, t, kk, jj):
        g, d = self.g, DIRS[kk]
        rows = g.seg_rows(mod4(g.p1 - d * t), mod4(g.p2 - d * jj))
        return self.same(m, kk, rows, self.a2s.at[self.slots[m]], self.a2r.at[self.slots[m], t, jj], g.axis1(d))

    def fwd2(self, m, t, kk, jj):
        g, d = self.g, DIRS[kk]
        rows = g.seg_rows(mod4(g.p1 - d * (t + 1)), mod4(g.p2 - d * jj))
        return self.same(m, kk, rows, self.f3s.at[self.slots[m]], self.f3r.at[self.slots[m]], g.partner)

    def first(self, m, far=False):
        self.pair_send(m).wait_recv()
        for kk in range(2):
            if far:
                for e in (1, 2, 3):
                    self.far1(m, e, kk).start()
            else:
                self.send1(m, 0, kk).start()
            self.send2(m, 0, kk, 0).start()

    def second(self, m, u, far=False):
        self.bulk(m, 2, self.a1s.at[self.slots[m]], self.a1r.at[self.slots[m], u]).wait_recv()
        for kk in range(2):
            if u < 2 and not far:
                self.send1(m, u + 1, kk).start()
            self.send2(m, 0, kk, u + 1).start()
            self.fwd1(m, u, kk).start()

    def item(self, m, t, jj):
        self.bulk(m, 2, self.a2s.at[self.slots[m]], self.a2r.at[self.slots[m], t, jj]).wait_recv()

        def pass_on():
            for kk in range(2):
                self.send2(m, t + 1, kk, jj).start()
        if isinstance(t, int):
            if t < 2:
                pass_on()
        else:
            pl.when(t < 2)(pass_on)
        for kk in range(2):
            self.fwd2(m, t, kk, jj).start()

    def round(self, m, t, extra=None):
        def step(jj):
            self.item(m, t, jj)
            if extra is not None:
                extra(jj)
        loop(0, 4, step)

    def pair_done(self, m):
        self.bulk(m, 30, self.f3s.at[self.slots[m]], self.f3r.at[self.slots[m]]).wait_recv()

    def drain(self, m):
        self.pair_send(m).wait_send()
        for sems, n in ((self.a1s, 6), (self.a2s, 24), (self.f3s, 30)):
            self.bulk(m, n, sems.at[self.slots[m]], self.f3r.at[self.slots[m]]).wait_send()


class StatExchange:
    def __init__(self, g, st, ss, rs):
        self.g, self.st, self.ss, self.rs = g, st, ss, rs

    def copy(self, i):
        return remote(self.st.at[0], self.st.at[1 + i], self.ss.at[i], self.rs.at[i], self.g.xdev((1, -1, 2)[i]))

    def put(self, i, lanes):
        self.st[0, i:i + 1] = jnp.sum(lanes.T, axis=0, keepdims=True)

    def start(self):
        for i in range(3):
            self.copy(i).start()

    def total(self):
        for i in range(3):
            self.copy(i).wait()
        return (self.st[0] + self.st[1]) + (self.st[2] + self.st[3])


def params(cid, vmem_mib=60.0):
    return pltpu.CompilerParams(collective_id=cid, has_side_effects=True, vmem_limit_bytes=int(vmem_mib * 1024 * 1024))


COST = pl.CostEstimate(flops=10 ** 11, bytes_accessed=10 ** 8, transcendentals=0)
DMA = pltpu.SemaphoreType.DMA
IN_VMEM = pl.BlockSpec(memory_space=pltpu.VMEM)
IN_HBM = pl.BlockSpec(memory_space=pl.ANY)
SDS = jax.ShapeDtypeStruct


SCALE = HEAD_DIM ** -0.5
TN = (((0,), (0,)), ((), ()))
NT = (((1,), (1,)), ((), ()))
W_SLOTS = (0, 1, 2, 0, 1)


def rope_turn(u, cos_tab, sin_tab):
    return u * cos_tab + pltpu.roll(u, 64, 1) * sin_tab


def causal_scores(keys, q_blk, i, n):
    s = lax.dot_general(keys, q_blk, NT, preferred_element_type=F32) * SCALE
    query = lax.broadcasted_iota(jnp.int32, (n, 128), 1) + i * 128
    return jnp.where(query >= lax.broadcasted_iota(jnp.int32, (n, 128), 0), s, -1e30)


def inv_column(total, i):
    return lax.rsqrt(total.T[:, i:i + 1] / 4096.0 + RMS_EPSILON)


def forward_phase(io, keep, w, x_full, xt, gyc, xcv, gains_in, a_acc, o_full, ga_all, gtw, sq, st, st2, r1, p_all, tmp,
            ld, xls, xs, xr, xfs, xfr, gls, gys, gyr, sts, strv, sts2, strv2, wos, xps, xpr, xst, yst,
            g1s, g1r, g2s, g2r, g3s, g3r, free,
            scl, sc1s, sc1r, sc2s, sc2r, osd, orv, ofs, ofr, ops, opr, gsd, grv, gfs, gfr, gps, gpr, s1s, s1r, *ring):
    (wq_in, wk_in, wv_in, wo_in, x_in, gy_in, gq_in, gk_in, gp_in, cos_tab, sin_tab, wq_out, wk_out, wv_out, x_t, y_cols) = io
    acts, gains, stats, post, wo_seg, wo_add, wo_mid, wor, wo_sent = keep
    s0 = wo_add
    w_in, w_out = (wq_in, wk_in, wv_in, wo_in), (wq_out, wk_out, wv_out)
    nw = 3
    cols_m, rows_m = 3, 4
    g = Torus()
    x, z, y, c, p1, p2 = g.x, g.z, g.y, g.c, g.p1, g.p2
    rings = WeightRings(g, w, W_SLOTS, ring)
    plane = [(x, mod4(z + d), y, c) for d in (1, 2, 3)] + [(x, z, mod4(y + d), c) for d in (1, 2, 3)] + [g.partner]
    everyone = plane + [g.xdev(1), g.xdev(-1), g.xdev(2)]
    ready = greet(everyone)

    def load(m, k):
        src = w_in[m].at[:, at256(k * 1024 + x * SEG)]
        return pltpu.make_async_copy(src, w.at[W_SLOTS[m], rings.my_rows, pl.ds(k * SEG, SEG)], ld.at[m])

    def rows_y(d):
        to = mod4(y + d)
        return remote(wo_in.at[:, at256(to * 1024 + x * SEG)], tmp.at[y], sc1s, sc1r, (x, z, to, c))

    def rows_x(d):
        return remote(tmp.at[mod4(x + d)], w.at[1, rings.my_rows, at256(x * SEG)], sc2s, sc2r, g.xdev(d))

    tmp_own = pltpu.make_async_copy(wo_in.at[:, at256(y * 1024 + x * SEG)], tmp.at[y], scl)
    tmp3 = tmp.at[pl.ds(0, 3)]

    def load_wait(m):
        ref = w.at[W_SLOTS[m], rings.my_rows]
        pltpu.make_async_copy(ref, ref, ld.at[m]).wait()

    def xseg(b, s):
        return x_full.at[at128(b * 128), pl.ds(s * 1024, 1024)]

    x_own = pltpu.make_async_copy(x_in, x_full.at[at128(x * 128)], xls)

    def xsend(di, s):
        ref = xseg(x, s)
        return remote(ref, ref, xs, xr.at[di, s], g.xdev(DIRS[di]))

    def xfwd(s):
        d = DIRS[s // 2]
        ref = xseg(mod4(x - d), s)
        return remote(ref, ref, xfs, xfr.at[s], g.xdev(d))

    gy_rows = at128(x * 128)

    def gy_own(k):
        return pltpu.make_async_copy(gy_in.at[:, at256(k * 1024 + x * SEG)], gyc.at[gy_rows, pl.ds(k * SEG, SEG)], gls)

    def gy_send(i, k):
        d = (1, -1, 2)[i]
        src = gy_in.at[:, at256(k * 1024 + mod4(x + d) * SEG)]
        return remote(src, gyc.at[gy_rows, pl.ds(k * SEG, SEG)], gys, gyr, g.xdev(d))

    def gblock(zh, ch):
        return gains.at[:, at128(zh * SEG + ch * 128)]

    def gain1(d):
        return remote(gains_in, gblock(z, c), g1s, g1r, (x, z, mod4(y + d), c))

    def gain2(d):
        ref = gblock(z, c)
        return remote(ref, ref, g2s, g2r, (x, mod4(z + d), y, c))

    def gain3(zh):
        ref = gblock(zh, c)
        return remote(ref, ref, g3s, g3r, g.partner)

    stat = StatExchange(g, st, sts, strv)
    stat2 = StatExchange(g, st2, sts2, strv2)

    def xt_pair(b):
        return remote(xt.at[lax.rem(b, 2)], x_t.at[pl.ds(pl.multiple_of(b * 1024, 1024), 1024), pl.ds(512, 512)], xps.at[b], xpr.at[b], g.partner)

    def xt_store(b):
        return pltpu.make_async_copy(xt.at[lax.rem(b, 2)], x_t.at[pl.ds(pl.multiple_of(b * 1024, 1024), 1024), pl.ds(0, 512)], xst.at[b])

    def turn(b):
        @pl.when(b >= 2)
        def _():
            xt_pair(b - 2).wait_send()
            xt_store(b - 2).wait()

        def step(i):
            xt[lax.rem(b, 2), at256(i * SEG), :] = x_full[:, at256(b * 1024 + i * SEG)].T
        loop(0, 4, step)
        xt_pair(b).start()
        xt_store(b).start()

    def w_store(m, theirs):
        cols = pl.ds(pl.multiple_of(((1 - c) if theirs else c) * 512, 512), 512)
        return pltpu.make_async_copy(w.at[m, :, cols], w_out[m].at[:, cols], wos.at[m, int(theirs)])

    y_store = pltpu.make_async_copy(xcv, y_cols, yst)

    st[0] = jnp.zeros((8, 512), F32)
    st2[0] = jnp.zeros((8, 512), F32)
    p_all[...] = jnp.zeros((512, 512), BF16)
    sq[...] = jnp.zeros((2, 512, 128), F32)
    gains_in[...] = jnp.concatenate([gq_in[...], gk_in[...], gp_in[...], jnp.zeros((5, 128), F32)], axis=0)
    for k in range(4):
        load(0, k).start()
    x_own.start()
    for m in range(1, nw):
        for k in range(4):
            load(m, k).start()
    for k in range(4):
        gy_own(k).start()
    ready()
    for m in range(nw):
        load_wait(m)
        rings.pair_send(m).start()
        if m == 0:
            x_own.wait()
            for s in range(4):
                for di in range(2):
                    xsend(di, (s + 2 * di) % 4).start()

    @pl.when(y == x)
    def _():
        gains[:, at128(z * SEG + c * 128)] = gains_in[...]
        for d in (1, 2, 3):
            gain1(d).start()

    def chunk(m, half, i):
        cols = at256((2 * (c + half * (1 - 2 * c)) + i) * SEG)
        acc_ref = a_acc.at[:, pl.ds(0, SEG)]

        def accumulate(kc):
            rows = pl.ds(pl.multiple_of(kc * 2048, 2048), 2048)
            acc_ref[...] = acc_ref[...] + jnp.dot(x_full[:, rows], w[m, rows, cols], preferred_element_type=F32)
        acc_ref[...] = jnp.zeros((512, SEG), F32)
        loop(0, 2, accumulate)
        acc = acc_ref[...].astype(BF16)
        acts[m, :, cols] = acc
        if m < 2:
            sqv = acc.astype(F32)
            sqv = sqv * sqv
            sq[m] = sq[m] + (sqv[:, :128] + sqv[:, 128:])

    def chunk_beside(m, half):
        return lambda jj: pl.when(lax.rem(jj, 2) == 1)(lambda: chunk(m, half, jj // 2))

    rings.first(0, True)
    rings.first(1)
    for u in range(3):
        rings.second(0, u, True)

    def prep_pair(jj):
        def step(i):
            cols = at128((2 * jj + i) * 128)
            for j in range(2):
                u = acts[j, :, cols].astype(F32) * sq[j] * gains[j:j + 1, cols]
                acts[3 + j, :, cols] = rope_turn(u, cos_tab[...], sin_tab[...]).astype(BF16)
        loop(0, 2, step)

    def tell(slot):
        for peer in everyone:
            pl.semaphore_signal(free.at[slot], inc=1, device_id=peer, device_id_type=MESH_ID)

    def beside(m, t):
        if (m, t) == (1, 1):
            own = chunk_beside(0, 0)

            def both(jj):
                turn(jj)
                own(jj)
            return both
        return {(1, 2): chunk_beside(0, 1), (2, 0): lambda jj: chunk(1, jj // 2, lax.rem(jj, 2)), (2, 2): prep_pair}.get((m, t))

    for m in range(nw):
        for t in range(3):
            if (m, t) == (2, 0):
                rings.pair_done(1)
                w_store(1, True).start()
            rings.round(m, t, beside(m, t))
            if m + 1 < nw:
                rings.second(m + 1, t)
            if (m, t) == (0, 0):
                @pl.when(y != x)
                def _():
                    remote(gains_in, gblock(z, c), g1s, g1r, g.partner).wait_recv()
                for d in (1, 2, 3):
                    gain2(d).start()
            if (m, t) == (0, 1):
                rings.first(2)
                for s in range(4):
                    xsend(s // 2, s).wait_recv()
                    xfwd(s).start()
                for k in range(4):
                    for i in range(3):
                        gy_send(i, k).start()
            if (m, t) == (0, 2):
                w_store(0, False).start()
                gain_rest = gains.at[:, pl.ds(0, 384)]
                remote(gain_rest, gain_rest, g2s, g2r, g.partner).wait()
                for zh in range(4):
                    gain3(zh).start()
            if (m, t) == (1, 0):
                rings.pair_done(0)
                w_store(0, True).start()
                for s in range(4):
                    xsend(1 - s // 2, s).wait_recv()
                    xfwd(s).wait_recv()
            if (m, t) == (1, 2):
                w_store(1, False).start()
                for k in range(4):
                    xcv[:, pl.ds(k * SEG, SEG)] = x_full[:, at256(k * 1024 + x * SEG)]
                rings.drain(0)
                w_store(0, False).wait()
                w_store(0, True).wait()
                tell(0)
                for k in range(4):
                    load(cols_m, k).start()
            if (m, t) == (2, 0):
                for i in range(2):
                    stat.put(i, sq[i])
                stat.start()
                load_wait(cols_m)
                pl.semaphore_wait(free.at[0], len(everyone))
                rings.pair_send(cols_m).start()
            if (m, t) == (2, 1):
                rings.drain(1)
                w_store(1, False).wait()
                w_store(1, True).wait()
                half_x, quarter_x = x_full.at[:, pl.ds(0, 2048)], x_full.at[:, pl.ds(0, 1024)]
                remote(half_x, half_x, xs, xr.at[0, 0], g.partner).wait_send()
                remote(quarter_x, quarter_x, xfs, xr.at[0, 0], g.partner).wait_send()
                tmp_own.start()
                for d in (1, 2, 3):
                    rows_y(d).start()
                tell(1)
                gain_half = gains.at[:, pl.ds(0, 512)]
                remote(gain_half, gain_half, g3s, g3r, g.partner).wait()
                total = stat.total()
                stats[...] = total
                for i in range(2):
                    sq[i] = jnp.broadcast_to(inv_column(total, i), (512, 128))

    rings.first(cols_m, True)
    remote(tmp3, tmp3, sc1s, sc1r, g.partner).wait_recv()
    tmp_own.wait()
    pl.semaphore_wait(free.at[1], len(everyone))
    for d in (1, -1, 2):
        rows_x(d).start()
    w[1, rings.my_rows, at256(x * SEG)] = tmp[x]
    w_store(2, False).start()
    def oblk(k, s):
        return o_full.at[:, at256(k * 1024 + s * SEG)]

    def osend(di, k):
        ref = oblk(k, x)
        return remote(ref, ref, osd, orv.at[di, k], g.xdev(DIRS[di]))

    def ofwd(k, di):
        d = DIRS[di]
        ref = oblk(k, mod4(x - d))
        return remote(ref, ref, ofs, ofr.at[k], g.xdev(d))

    def attend(k):
        for ch in range(2):
            cols = at128(k * SEG + ch * 128)
            qh, kh, vh = acts[3, :, cols], acts[4, :, cols], acts[2, :, cols]
            for i in range(4):
                n = (i + 1) * 128
                s = causal_scores(kh[:n], qh[i * 128:n], i, n)
                e = jnp.exp(s - jnp.max(s, axis=0, keepdims=True))
                p_all[0:n, pl.ds(i * 128, 128)] = (e * (1.0 / jnp.sum(e, axis=0, keepdims=True))).astype(BF16)
            o = lax.dot_general(p_all[...], vh, TN, preferred_element_type=F32).astype(BF16)
            o_full[:, at128(k * 1024 + x * SEG + ch * 128)] = o
        for di in range(2):
            osend(di, k).start()

    def o_pair(s):
        for k in range(4):
            cols = at256(k * 1024 + s * SEG)
            remote(o_full.at[:, cols], x_full.at[:, cols], ops, opr, g.partner).start()

    def cols_items(lo, hi):
        loop(lo, hi, lambda it: rings.item(cols_m, it // 4, lax.rem(it, 4)))

    def o_forward(base):
        for i in range(2):
            osend(i, base + i).wait_recv()
            ofwd(base + i, i).start()

    own_k, pair_k = 2 * c, 2 * (1 - c)

    rest = w.at[1, rings.my_rows, pl.ds(0, 768)]

    def groups(half):
        @pl.when(half == 1)
        def _():
            remote(rest, rest, sc2s, sc2r, g.partner).wait_recv()
            rings.pair_send(rows_m).start()
            rings.pair_done(2)
            w_store(2, True).start()
        base = own_k + half * (pair_k - own_k)

        def one(i):
            chunk(2, half, i)
            attend(base + i)
            pl.when(jnp.logical_and(half == 1, i == 0))(lambda: rings.first(rows_m, True))

            @pl.when(half == 0)
            def _():
                @pl.when(i == 0)
                def _():
                    for u in range(3):
                        rings.second(cols_m, u, True)

            @pl.when(half == 1)
            def _():
                for r in range(2):
                    it = 2 * i + r
                    rings.item(cols_m, it // 4, lax.rem(it, 4))
        loop(0, 2, one)
    loop(0, 2, groups)
    cols_items(4, 8)
    o_forward(own_k)

    for u in range(3):
        rings.second(rows_m, u, True)
    cols_items(8, 12)
    o_forward(pair_k)
    rings.pair_done(cols_m)
    o_pair(x)

    def a_part(s, init=False):
        def step(i):
            cols = pl.ds(pl.multiple_of(i * 512, 512), 512)
            acc = None
            for k in range(4):
                dot = jnp.dot(o_full[:, at256(k * 1024 + s * SEG)], w[0, at256(k * 1024 + s * SEG), cols], preferred_element_type=F32)
                acc = dot if acc is None else acc + dot
            a_acc[:, cols] = acc if init else a_acc[:, cols] + acc
        loop(0, 2, step)

    a_part(x, True)
    for k in range(4):
        osend(1 - k % 2, k).wait_recv()
    o_pair(mod4(x + 1))
    o_pair(mod4(x + 3))
    loop(0, 2, lambda i: a_part(mod4(x + 2 * i - 1)))
    rings.round(rows_m, 0)
    for k in range(4):
        ofwd(k, k % 2).wait_recv()
    a_part(mod4(x + 2))
    o_oth = x_full
    gy_mine, gy_rest = gyc.at[pl.ds(0, 128)], gyc.at[pl.ds(0, 384)]
    pltpu.make_async_copy(gy_mine, gy_mine, gls).wait()
    remote(gy_rest, gy_rest, gys, gyr, g.partner).wait()

    sq[...] = jnp.zeros((2, 512, 128), F32)

    def a_stats(h):
        cols = at128(h * 128)
        a = a_acc[:, cols].astype(BF16).astype(F32)
        gh = gyc[:, cols].astype(F32) * gains[2:3, cols]
        sq[0] = sq[0] + a * a
        sq[1] = sq[1] + gh * a
    loop(0, 8, a_stats)
    for i in range(2):
        stat2.put(i, sq[i])
    stat2.start()
    total2 = stat2.total()
    inv_a = inv_column(total2, 0)
    sq[0] = jnp.broadcast_to(inv_a, (512, 128))
    sq[1] = jnp.broadcast_to(total2.T[:, 1:2] * inv_a / 4096.0, (512, 128))

    def gblk(k, s):
        return ga_all.at[s, :, pl.ds(k * SEG, SEG)]

    def gsend(di, k):
        ref = gblk(k, x)
        return remote(ref, ref, gsd, grv.at[di, k], g.xdev(DIRS[di]))

    def gsend_start(di, k):
        for i in range(4):
            ref = ga_all.at[x, pl.ds(i * 128, 128), at256(k * SEG)]
            remote(ref, ref, gsd, grv.at[di, k], g.xdev(DIRS[di])).start()

    def gfwd(k):
        d = DIRS[k % 2]
        ref = gblk(k, mod4(x - d))
        return remote(ref, ref, gfs, gfr.at[k], g.xdev(d))

    theirs = pl.ds(pl.multiple_of((1 - c) * 512, 512), 512)
    mine = pl.ds(pl.multiple_of(c * 512, 512), 512)
    ga_pair = remote(ga_all.at[x, :, theirs], gtw.at[pl.ds(512, 512)], gps, gpr, g.partner)

    def send_grad_a(k):
        def step(i):
            cols = at128(k * SEG + i * 128)
            scale = sq[0]
            a_hat = a_acc[:, cols].astype(BF16).astype(F32) * scale
            ga_all[x, :, cols] = (scale * (gyc[:, cols].astype(F32) * gains[2:3, cols] - a_hat * sq[1])).astype(BF16)
        loop(0, 2, step)
        for di in range(2):
            gsend_start(di, k)
    loop(0, 4, send_grad_a)
    ga_pair.start()
    o_pair(mod4(x + 2))
    gtw[0:512] = ga_all[x, :, mine]
    def finish_y(h):
        cols = at128(h * 128)
        a_hat = a_acc[:, cols].astype(BF16).astype(F32) * sq[0]
        xcv[:, cols] = (xcv[:, cols].astype(F32) + a_hat * gains[2:3, cols]).astype(BF16)
        post[0:1, cols] = jnp.sum(gyc[:, cols].astype(F32) * a_hat, axis=0, keepdims=True)
    loop(0, 8, finish_y)
    y_store.start()
    remote(o_full, o_oth, ops, opr, g.partner).wait_recv()
    ga_pair.wait_recv()

    def slot(kk, t, jj):
        return (r1, wo_mid, wo_seg)[t].at[kk, jj]

    def send1(t, kk, jj):
        src = s0.at[kk, jj] if t == 0 else slot(kk, t - 1, jj)
        ss, rs = (wo_sent, wor.at[jj]) if t == 2 else (s1s.at[t], s1r.at[t, jj])
        return remote(src, slot(kk, t, jj), ss, rs, g.axis1(1 - 2 * kk))

    def tile(kk, tt, jj):
        d = 1 - 2 * kk
        cols = g.seg_rows(mod4(p1 - d * (1 + tt)), mod4(p2 - d * (1 + jj)))
        right = at256(kk * SEG)
        return (lax.dot_general(o_full[:, cols], gtw[0:512, right], TN, preferred_element_type=F32)
                + lax.dot_general(o_oth[:, cols], gtw[512:1024, right], TN, preferred_element_type=F32))

    def start_item(jj):
        def color(kk):
            s0[kk, jj] = tile(kk, 0, jj)
            send1(0, kk, jj).start()
        loop(0, 2, color)

    def ring_item(t, jj):
        ref = s0.at[0, pl.ds(0, 2)]
        remote(ref, ref, s1s.at[t], s1r.at[t, jj], g.partner).wait_recv()

        def color(kk):
            dst = slot(kk, t, jj)
            dst[...] = dst[...] + tile(kk, t + 1, jj)
            send1(t + 1, kk, jj).start()
        loop(0, 2, color)

    def last_tiles(jj):
        def color(kk):
            wo_add[kk, jj] = tile(kk, 3, jj)
        loop(0, 2, color)

    def g_forward(lo):
        for k in (lo, lo + 1):
            gsend(k % 2, k).wait_recv()
            gfwd(k).start()

    loop(0, 4, start_item)
    rings.round(rows_m, 1)
    rings.round(rows_m, 2)
    g_forward(0)
    loop(0, 2, lambda jj: ring_item(0, jj))
    g_forward(2)
    loop(2, 4, lambda jj: ring_item(0, jj))
    rings.pair_done(rows_m)

    def go_part(s, init=False):
        def step(zi):
            cols = at256(zi * SEG)
            acc = None
            for k in range(4):
                dot = lax.dot_general(ga_all[s, :, k * SEG:(k + 1) * SEG], w[1, at256(zi * 1024 + k * SEG), at256(s * SEG)],
                                      NT, preferred_element_type=F32)
                acc = dot if acc is None else acc + dot
            a_acc[:, cols] = acc if init else a_acc[:, cols] + acc
        loop(0, 4, step)

    go_part(x, True)
    for k in range(4):
        gsend(1 - k % 2, k).wait_recv()
    loop(0, 2, lambda i: go_part(mod4(x + 2 * i - 1)))
    remote(s0, s0, s1s.at[0], opr, g.partner).wait_send()
    loop(0, 4, last_tiles)
    loop(0, 4, lambda jj: ring_item(1, jj))

    @pl.when(y == x)
    def _():
        remote(gain_rest, gain_rest, g1s, g1r, g.partner).wait_send()
    remote(tmp3, tmp3, sc1s, sc1r, g.partner).wait_send()
    remote(rest, rest, sc2s, sc2r, g.partner).wait_send()
    for b in range(4):
        if b >= 2:
            xt_pair(b).wait_send()
            xt_store(b).wait()
        xt_pair(b).wait_recv()
    w_store(2, False).wait()
    w_store(2, True).wait()
    y_store.wait()
    remote(o_full, o_oth, ops, opr, g.partner).wait_send()
    ga_pair.wait_send()
    both = ga_all.at[pl.ds(0, 2)]
    one = ga_all.at[0]
    remote(both, both, osd, opr, g.partner).wait_send()
    remote(both, both, gsd, opr, g.partner).wait_send()
    remote(one, one, ofs, opr, g.partner).wait_send()
    for m in (2, cols_m, rows_m):
        rings.drain(m)
    for k in range(4):
        gfwd(k).wait_recv()
    go_part(mod4(x + 2))

    def keep_grad_o(h):
        cols = at128(h * 128)
        acts[5, :, cols] = a_acc[:, cols].astype(BF16)
    loop(0, 8, keep_grad_o)

    remote(one, one, gfs, opr, g.partner).wait_send()
    remote(s0, s0, s1s.at[1], opr, g.partner).wait_send()


FORWARD_SCRATCH = [
    pltpu.VMEM((3, 4096, 1024), BF16),
    pltpu.VMEM((512, 4096), BF16),
    pltpu.VMEM((2, 1024, 512), BF16),
    pltpu.VMEM((512, 1024), BF16),
    pltpu.VMEM((512, 1024), BF16),
    pltpu.VMEM((8, 128), F32),
    pltpu.VMEM((512, 1024), F32),
    pltpu.VMEM((512, 4096), BF16),
    pltpu.VMEM((4, 512, 1024), BF16),
    pltpu.VMEM((1024, 512), BF16),
    pltpu.VMEM((2, 512, 128), F32),
    pltpu.VMEM((4, 8, 512), F32),
    pltpu.VMEM((4, 8, 512), F32),
    pltpu.VMEM((2, 4, SEG, SEG), F32),
    pltpu.VMEM((512, 512), BF16),
    pltpu.VMEM((4, 128, SEG), BF16),
    DMA((4,)), DMA(()), DMA(()), DMA((2, 4)), DMA(()), DMA((4,)),
    DMA(()), DMA(()), DMA(()), DMA((3,)), DMA((3,)), DMA((3,)), DMA((3,)),
    DMA((3, 2)), DMA((4,)), DMA((4,)), DMA((4,)), DMA(()),
    DMA(()), DMA(()), DMA(()), DMA(()), DMA(()), DMA(()), pltpu.SemaphoreType.REGULAR((2,)),
    DMA(()), DMA(()), DMA(()), DMA(()), DMA(()), DMA(()), DMA((2, 4)), DMA(()), DMA((4,)), DMA(()), DMA(()),
    DMA(()), DMA((2, 4)), DMA(()), DMA((4,)), DMA(()), DMA(()),
    DMA((2,)), DMA((2, 4)),
] + ring_sems(3)


NU = 4
WO = 4


def backward_phase(io, keep, r1, r1h, r2, r2h, rg, buf, dall, rt, lt, gxc, p_all, ds_all, lanes, st, ge, gy, gxo,
            s1s, s1t, s1r, s2s, s2r, ags, agr, agx, d2s, d2r, fws, fwr, lws, lts, gs, gr, gls, wls, gxs, gyl, dps, dpr, sts, strv,
            e1s, e1r, e2s, e2r, e3s, e3r, e4s):
    gy_in, cos_tab, sin_tab, wq, wk, wv, x_t, y_cols, dwv, dwk, dwq, dwo, y_out, gx_part, gx_out, gain_out = io
    acts, gains, stats, post, wo_seg, wo_add, wo_mid, wor, wo_sent, inside, ysd, yrv, yst, e4r = keep
    s0 = wo_add
    outs = (dwv, dwk, dwq, dwq, dwo)
    widths = (SEG, SEG, 128, 128, SEG)
    shifts = (0, 0, 0, 128, 0)
    weights = (wv, wk, wq)
    g = Torus()
    x, z, y, c, p1, p2 = g.x, g.z, g.y, g.c, g.p1, g.p2
    peers = ([(x, mod4(z + d), y, c) for d in (1, 2, 3)] + [(x, z, mod4(y + d), c) for d in (1, 2, 3)]
             + [g.partner, g.xdev(2)] + [g.xdev(d, h) for d in DIRS for h in (0, 1)])
    for peer in peers:
        pl.semaphore_signal(inside, inc=1, device_id=peer, device_id_type=MESH_ID)

    def block(kk, tt, jj):
        d = 1 - 2 * kk
        return g.seg_rows(mod4(p1 - d * (1 + tt)), mod4(p2 - d * (1 + jj)))

    def aload(n, kk):
        par = lax.rem(n, 2)
        return pltpu.make_async_copy(x_t.at[block(kk, 1 + n // 4, lax.rem(n, 4))], lt.at[0, par, kk], lts.at[0, par])

    def bload(jj, kk):
        par = lax.rem(jj, 2)
        return pltpu.make_async_copy(x_t.at[block(kk, 0, jj)], lt.at[1, par, kk], lts.at[1, par])

    def load_wait(kind, par):
        pltpu.make_async_copy(lt.at[kind, par], lt.at[kind, par], lts.at[kind, par]).wait()

    def tile(kind, m, par, kk):
        cols = pl.ds(pl.multiple_of(kk * SEG + shifts[m], 128), widths[m])
        return jnp.dot(lt[kind, par, kk], rt[min(m, 2), :, cols], preferred_element_type=F32)

    def slot(m, kk, t, jj):
        if m == WO:
            return wo_seg.at[kk, jj]
        return r1.at[m, kk, t, jj] if m < 2 else r1h.at[m - 2, kk, t, jj]

    def slot2(m, kk, u):
        return r2h.at[m - 2, kk, u] if m in (2, 3) else r2.at[min(m, 2), kk, u]

    def first_slot(m, kk, jj):
        return s0.at[kk, jj, :, pl.ds(shifts[m], widths[m])]

    def send1(m, t, kk, jj, first=False):
        src = first_slot(m, kk, jj) if first else slot(m, kk, t - 1, jj)
        ss = s1s.at[m, jj] if first and m < 2 else s1t.at[m]
        return remote(src, slot(m, kk, t, jj), ss, s1r.at[m, t, jj], g.axis1(1 - 2 * kk))

    def recv1(m, t, jj):
        ref = r1.at[0, 0, 0, pl.ds(0, 2)] if m < 2 else r1h.at[0, 0, 0, pl.ds(0, 2)]
        remote(ref, ref, s1t.at[0], s1r.at[m, t, jj], g.partner).wait_recv()

    def send2(m, u, kk):
        return remote(slot(m, kk, 2, u), slot2(m, kk, u), s2s.at[m], s2r.at[m, u], g.axis2(DIRS[kk]))

    def start_item(m, jj):
        load_wait(1, lax.rem(jj, 2))
        if m in (1, 2):
            ref = s0.at[0, pl.ds(0, 2)]
            remote(ref, ref, s1s.at[m - 1, jj], s2r.at[0, 0], g.partner).wait_send()

        def color(kk):
            first_slot(m, kk, jj)[...] = tile(1, m, lax.rem(jj, 2), kk)
            send1(m, 0, kk, jj, True).start()
        loop(0, 2, color)
        for kk in range(2):
            pl.when(jj < 2)(lambda: bload(jj + 2, kk).start())
            if m + 1 < NU:
                pl.when(jj >= 2)(lambda: bload(jj - 2, kk).start())

    def ring_item(m, n):
        t, jj = n // 4, lax.rem(n, 4)
        load_wait(0, lax.rem(n, 2))
        recv1(m, t, jj)

        def color(kk):
            ref = slot(m, kk, t, jj)
            ref[...] = ref[...] + tile(0, m, lax.rem(n, 2), kk)
            pl.when(t < 2)(lambda: send1(m, t + 1, kk, jj).start())
        loop(0, 2, color)
        for kk in range(2):
            pl.when(n < 10)(lambda: aload(n + 2, kk).start())
            if m + 1 < NU:
                pl.when(n >= 10)(lambda: aload(n - 10, kk).start())

    def wo_item(jj):
        ref = s0.at[0, pl.ds(0, 2)]
        remote(ref, ref, s1t.at[0], wor.at[jj], g.partner).wait_recv()

        def color(kk):
            wo_seg[kk, jj] = wo_seg[kk, jj] + wo_add[kk, jj]
        loop(0, 2, color)

    def out_cols(k, xs, m=0):
        return pl.ds(pl.multiple_of(k * 1024 + xs * SEG + shifts[m], 128), widths[m])

    def ag_send(m, kk, di, h):
        k = 2 * c + kk
        return remote(slot(m, kk, 2, 3).at[pl.ds(h * 128, 128)], outs[m].at[:, out_cols(k, x, m)], ags.at[m],
                      agr.at[m, di] if di == kk else agx.at[m],
                      g.xdev(DIRS[di], h))

    def pair_send(m, kk):
        src = slot(m, kk, 2, 3).at[at128((1 - c) * 128)]
        return remote(src, outs[m].at[:, out_cols(2 * c + kk, x, m)], d2s.at[m], d2r.at[m], g.partner)

    def own_store(m, kk):
        return pltpu.make_async_copy(slot(m, kk, 2, 3).at[at128(c * 128)], outs[m].at[:, out_cols(2 * c + kk, x, m)], lws.at[m])

    def forward(m, k):
        di = k % 2
        ref = outs[m].at[:, out_cols(k, mod4(x - DIRS[di]), m)]
        return remote(ref, ref, fws.at[m], fwr.at[m], g.xdev(DIRS[di]))

    def hand_out(m, kk):
        own_store(m, kk).start()
        for di in range(2):
            for h in range(2):
                ag_send(m, kk, di, h).start()
        pair_send(m, kk).start()

    def phase2(m, u):
        if u > 0:
            ref = r2h.at[0, 0, pl.ds(0, 2)] if m in (2, 3) else r2.at[0, 0, pl.ds(0, 2)]
            remote(ref, ref, s2s.at[m], s2r.at[m, u - 1], g.partner).wait_recv()
        for kk in range(2):
            if u > 0:
                ref = slot(m, kk, 2, u)
                ref[...] = ref[...] + slot2(m, kk, u - 1)[...]
            if u < 3:
                send2(m, u, kk).start()
            else:
                hand_out(m, kk)

    def direct2(m, u, kk):
        return remote(slot(m, kk, 2, u), slot2(m, kk, u), s2s.at[m], s2r.at[m, u], g.axis2(-(1 + u) * DIRS[kk]))

    def last_phase2(m):
        for u in range(3):
            ref = r2h.at[0, 0, pl.ds(0, 2)]
            remote(ref, ref, s2s.at[m], s2r.at[m, u], g.partner).wait_recv()
        for kk in range(2):
            ref = slot(m, kk, 2, 3)
            ref[...] = (ref[...] + slot2(m, kk, 0)[...]) + (slot2(m, kk, 1)[...] + slot2(m, kk, 2)[...])
            hand_out(m, kk)

    def do_forward(m):
        for di in range(2):
            ref = outs[m].at[:, pl.ds(0, 2 * widths[m])]
            remote(ref, ref, ags.at[m], agr.at[m, di], g.partner).wait_recv()
            for k in (di, di + 2):
                forward(m, k).start()

    def bytes_of(m, n, ss, rs):
        ref = outs[m].at[:, pl.ds(0, n * widths[m])]
        return remote(ref, ref, ss, rs, g.partner)

    def drain_slots(m):
        if m != WO:
            ref = r1.at[m, pl.ds(0, 2), pl.ds(0, 2)] if m < 2 else r1h.at[0]
            remote(ref, ref, s1t.at[m], d2r.at[m], g.partner).wait_send()
        bytes_of(m, 12, s2s.at[m], d2r.at[m]).wait_send()
        bytes_of(m, 8, ags.at[m], agx.at[m]).wait_send()
        bytes_of(m, 2, d2s.at[m], d2r.at[m]).wait_send()
        ref = outs[m].at[:, pl.ds(0, 2 * widths[m])]
        pltpu.make_async_copy(ref, ref, lws.at[m]).wait()

    def drain_unit(m):
        drain_slots(m)
        bytes_of(m, 4, ags.at[m], agx.at[m]).wait_recv()
        bytes_of(m, 2, d2s.at[m], d2r.at[m]).wait_recv()
        bytes_of(m, 4, fws.at[m], fwr.at[m]).wait()

    def gcols(kk, jj):
        return pl.ds(pl.multiple_of(kk * 2048 + jj * 512, 512), 512)

    def gsend(t, kk, jj):
        d = DIRS[kk]
        if t == 0:
            src = gx_part.at[at128(mod4(x - d) * 128), gcols(kk, jj)]
        else:
            src = rg.at[kk, t - 1, jj]
        return remote(src, rg.at[kk, t, jj], gs, gr.at[t, jj], g.xdev(d))

    def gbuf(t, kk, jj):
        return (t % 2, at128(jj * 128), pl.ds(kk * 512, 512))

    def gload(t, kk, jj):
        src = gx_part.at[at128(mod4(x - DIRS[kk] * (2 + t)) * 128), gcols(kk, jj)]
        return pltpu.make_async_copy(src, buf.at[gbuf(t, kk, jj)], gls.at[t % 2, jj])

    def gloads(t):
        each(lambda kk, jj: gload(t, kk, jj).start())

    def chunk_rows(e):
        return pl.ds(pl.multiple_of((lax.rem(e, 2) * 4 + e // 2) * 512, 512), 512)

    def wload(e, i):
        par = lax.rem(e + 1, 2)
        return pltpu.make_async_copy(weights[i].at[chunk_rows(e)], acts.at[3 * par + i], wls.at[par])

    def gx_store(e):
        par = lax.rem(e, 2)
        return pltpu.make_async_copy(gxc.at[par], gx_part.at[:, chunk_rows(e)], gxs.at[par])

    def gx_ship(e, kk):
        gx_store(e).wait()
        gsend(0, kk, e // 2).start()

    def gx_chunk(e):
        par, wpar = lax.rem(e, 2), lax.rem(e + 1, 2)
        ref = acts.at[pl.ds(0, 3)]
        pltpu.make_async_copy(ref, ref, wls.at[wpar]).wait()

        def rows_half(r):
            rows = at256(r * SEG)
            acc = None
            for i in range(3):
                dot = lax.dot_general(dall[i, rows, :], acts[3 * wpar + i], NT, preferred_element_type=F32)
                acc = dot if acc is None else acc + dot
            gxc[par, rows, :] = acc
        loop(0, 2, rows_half)
        gx_store(e).start()

        @pl.when(e < 6)
        def _():
            for i in range(3):
                wload(e + 2, i).start()
        for kk in range(2):
            pl.when(jnp.logical_and(e > 0, lax.rem(e, 2) == 1 - kk))(lambda: gx_ship(e - 1, kk))

    gx_save = pltpu.make_async_copy(gxo, gx_out, gyl)

    def gx_item(t, jj):
        ref = rg.at[0, 0, pl.ds(0, 2)]
        remote(ref, ref, gs, gr.at[t, jj], g.partner).wait_recv()
        pltpu.make_async_copy(ref, ref, gls.at[t % 2, jj]).wait()
        for kk in range(2):
            total = rg[kk, t, jj] + buf[gbuf(t, kk, jj)]
            if t < 2:
                rg[kk, t, jj] = total
                gsend(t + 1, kk, jj).start()
            else:
                gxo[:, gcols(kk, jj)] = (total + gy[:, gcols(kk, jj)].astype(F32)).astype(BF16)

    def y_send(i, k):
        d = (1, -1, 2)[i]
        src = y_cols.at[at128(mod4(x + d) * 128), pl.ds(k * SEG, SEG)]
        return remote(src, y_out.at[:, out_cols(k, x)], ysd, yrv, g.xdev(d))

    def y_own(k):
        return pltpu.make_async_copy(y_cols.at[at128(x * 128), pl.ds(k * SEG, SEG)], y_out.at[:, out_cols(k, x)], yst)

    gain1 = remote(ge.at[0], ge.at[1], e1s, e1r, g.partner)

    def gain2(d):
        return remote(ge.at[8], ge.at[1 + d], e2s.at[d - 1], e2r.at[d - 1], (x, mod4(z + d), y, c))

    def gain3(d):
        return remote(ge.at[9], ge.at[4 + d], e3s.at[d - 1], e3r.at[d - 1], (x, z, mod4(y + d), c))

    my_head = at128(z * SEG + c * 128)

    def gain4(d):
        return remote(ge.at[10, :, my_head], gain_out, e4s.at[d - 1], e4r, g.xdev(d))

    gy_load = pltpu.make_async_copy(gy_in, gy, gyl)
    stat = StatExchange(g, st, sts, strv)
    theirs = pl.ds(pl.multiple_of((1 - c) * 512, 512), 512)
    mine = pl.ds(pl.multiple_of(c * 512, 512), 512)

    def swap(i):
        return remote(dall.at[i, :, theirs], rt.at[i, pl.ds(512, 512)], dps.at[i], dpr.at[i], g.partner)

    def share(i):
        rt[i, 0:512] = dall[i, :, mine]
        swap(i).start()

    gy_load.start()
    for k in range(4):
        for i in range(3):
            y_send(i, k).start()
        y_own(k).start()
    for kk in range(2):
        for jj in range(2):
            bload(jj, kk).start()
            aload(jj, kk).start()
    inv = [gxc.at[0, :, pl.ds(i * 128, 128)] for i in range(2)]
    proj = [gxc.at[1, :, pl.ds(i * 128, 128)] for i in range(2)]
    for i in range(2):
        inv[i][...] = jnp.broadcast_to(inv_column(stats[...], i), (512, 128))
    lanes[...] = jnp.zeros((2, 512, 128), F32)
    st[0] = jnp.zeros((8, 512), F32)
    ge[0] = jnp.zeros((8, 1024), F32)
    ge[0, 2:3] = post[...]

    p_all[...] = jnp.zeros((512, 512), BF16)
    ds_all[...] = jnp.zeros((512, 512), BF16)

    def norm_back(i, src_rows, cols, gn):
        hat = acts[i, src_rows, cols].astype(F32) * inv[i][src_rows, :]
        prod = gn * hat
        gain = gains[i:i + 1, cols]
        buf[i, src_rows, cols] = gn * gain
        lanes[i, src_rows] = lanes[i, src_rows] + prod * gain
        return jnp.sum(prod, axis=0, keepdims=True)

    def head(h):
        cols = at128(h * 128)
        vh, qh, kh, do = (acts[i, :, cols] for i in (2, 3, 4, 5))
        for i in range(4):
            n = (i + 1) * 128
            block_i = pl.ds(i * 128, 128)
            s = causal_scores(kh[:n], qh[i * 128:n], i, n)
            e = jnp.exp(s - jnp.max(s, axis=0, keepdims=True))
            p = e * (1.0 / jnp.sum(e, axis=0, keepdims=True))
            dp = lax.dot_general(vh[:n], do[i * 128:n], NT, preferred_element_type=F32)
            p_all[0:n, block_i] = p.astype(BF16)
            ds_all[0:n, block_i] = (p * (dp - jnp.sum(p * dp, axis=0, keepdims=True)) * SCALE).astype(BF16)
        dall[0, :, cols] = jnp.dot(p_all[...], do, preferred_element_type=F32).astype(BF16)
        dq = lax.dot_general(ds_all[...], kh, TN, preferred_element_type=F32)
        dk = jnp.dot(ds_all[...], qh, preferred_element_type=F32)
        for i, grad in ((0, dq), (1, dk)):
            ge[0, i:i + 1, cols] = norm_back(i, pl.ds(0, 512), cols, rope_turn(grad, cos_tab[...], -sin_tab[...]))

    def finish(i, m, column):
        proj[i][...] = jnp.broadcast_to(column, (512, 128))

        def step(h):
            cols = at128(h * 128)
            scale = inv[i][...]
            hat = acts[i, :, cols].astype(F32) * scale
            dall[m, :, cols] = (scale * (buf[i, :, cols] - hat * proj[i][...])).astype(BF16)
        loop(0, 8, step)

    def head_step(i):
        head(i)

        @pl.when(i == 2)
        def _():
            pl.semaphore_wait(inside, len(peers))
            wo_item(0)
            phase2(WO, 0)

        @pl.when(i == 4)
        def _():
            wo_item(1)
            phase2(WO, 1)

        @pl.when(i == 7)
        def _():
            wo_item(2)
            phase2(WO, 2)
    loop(0, 8, head_step)
    share(0)
    for i in range(2):
        stat.put(i, lanes[i])
    stat.start()
    gain1.start()
    for i in range(3):
        wload(0, i).start()
    wo_item(3)
    swap(0).wait_recv()
    loop(0, 4, lambda jj: start_item(0, jj))
    total = stat.total().T / 4096.0
    finish(1, 1, total[:, 1:2])
    share(1)
    finish(0, 2, total[:, 0:1])
    share(2)
    for i in range(3):
        wload(1, i).start()
    phase2(WO, 3)
    gy_load.wait()

    for m in range(NU):
        def early(n, m=m):
            ring_item(m, n)
            if m > 0:
                pl.when(n == 0)(lambda: phase2(m - 1, 2))
                pl.when(n == 2)(lambda: phase2(m - 1, 3))
            if m == 0:
                gx_chunk(n)
            elif m == 1:
                pl.when(n >= 4)(lambda: gx_item(1, n - 4))

        loop(0, 8, early)
        if m == 0:
            gx_ship(7, 1)
            gloads(0)
            gloads(1)
            do_forward(WO)
            gain1.wait_recv()
            ge[8] = ge[0] + ge[1]
            for d in (1, 2, 3):
                gain2(d).start()
            swap(1).wait_recv()
            swap(2).wait_recv()
        if m == 1:
            for d in (1, 2, 3):
                gain2(d).wait_recv()
            ge[9] = (ge[8] + ge[2]) + (ge[3] + ge[4])
            for d in (1, 2, 3):
                gain3(d).start()
        if m == 3:
            gx_save.start()
            do_forward(1)
        if m == 2:
            for d in (1, 2, 3):
                gain3(d).wait_recv()
            ge[10] = (ge[9] + ge[5]) + (ge[6] + ge[7])

            @pl.when(y == x)
            def _():
                gain_out[...] = ge[10, :, my_head]
                for d in (1, 2, 3):
                    gain4(d).start()

        def late(n, m=m):
            if m + 1 < NU:
                start_item(m + 1, n - 8)
            ring_item(m, n)
            if m < 3:
                pl.when(n == 8)(lambda: phase2(m, 0))
                pl.when(n == 10)(lambda: phase2(m, 1))
            else:
                for u in range(3):
                    for kk in range(2):
                        pl.when(n == 8 + u)(lambda: direct2(m, u, kk).start())
            if m in (0, 2):
                gx_item(m, n - 8)

        loop(8, 12, late)
        if m == 0:
            gloads(2)
        if m == 1:
            do_forward(0)
        if m == 3:
            do_forward(2)
    last_phase2(NU - 1)
    do_forward(NU - 1)

    remote(wo_mid, wo_mid, wo_sent, yrv, g.partner).wait_send()
    @pl.when(y == x)
    def _():
        for d in (1, 2, 3):
            gain4(d).wait_send()

    @pl.when(y != x)
    def _():
        gain4(1).wait_recv()
    gain1.wait_send()
    for d in (1, 2, 3):
        gain2(d).wait_send()
        gain3(d).wait_send()
    y_all, y_mine = y_out.at[:, pl.ds(0, 3072)], y_out.at[:, pl.ds(0, 1024)]
    remote(y_all, y_all, ysd, yrv, g.partner).wait()
    pltpu.make_async_copy(y_mine, y_mine, yst).wait()
    for m in range(NU + 1):
        drain_unit(m)
    most = gx_part.at[:, pl.ds(0, 3072)]
    remote(most, most, gs, gr.at[0, 0], g.partner).wait_send()
    for i in range(3):
        swap(i).wait_send()
    gx_save.wait()


BACKWARD_SCRATCH = [
    pltpu.VMEM((2, 2, 3, 4, SEG, SEG), F32),
    pltpu.VMEM((2, 2, 3, 4, SEG, 128), F32),
    pltpu.VMEM((3, 2, 3, SEG, SEG), F32),
    pltpu.VMEM((2, 2, 3, SEG, 128), F32),
    pltpu.VMEM((2, 3, 4, 128, 512), F32),
    pltpu.VMEM((2, 512, 1024), F32),
    pltpu.VMEM((3, 512, 1024), BF16),
    pltpu.VMEM((3, 1024, 512), BF16),
    pltpu.VMEM((2, 2, 2, SEG, 1024), BF16),
    pltpu.VMEM((2, 512, 512), F32),
    pltpu.VMEM((512, 512), BF16),
    pltpu.VMEM((512, 512), BF16),
    pltpu.VMEM((2, 512, 128), F32),
    pltpu.VMEM((4, 8, 512), F32),
    pltpu.VMEM((11, 8, 1024), F32),
    pltpu.VMEM((128, 4096), BF16),
    pltpu.VMEM((128, 4096), BF16),
    DMA((2, 4)), DMA((NU,)), DMA((NU, 3, 4)), DMA((NU + 1,)), DMA((NU + 1, 3)),
    DMA((NU + 1,)), DMA((NU + 1, 2)), DMA((NU + 1,)), DMA((NU + 1,)), DMA((NU + 1,)), DMA((NU + 1,)), DMA((NU + 1,)), DMA((NU + 1,)),
    DMA((2, 2)), DMA(()), DMA((3, 4)), DMA((2, 4)), DMA((2,)), DMA((2,)), DMA(()),
    DMA((3,)), DMA((3,)), DMA((3,)), DMA((3,)),
    DMA(()), DMA(()), DMA((3,)), DMA((3,)), DMA((3,)), DMA((3,)), DMA((3,)),
]


def layer_kernel(wq_in, wk_in, wv_in, wo_in, x_in, gy_in, gq_in, gk_in, gp_in, cos_tab, sin_tab,
                 dwv, dwk, dwq, dwo, y_out, gx_out, wq_out, wk_out, wv_out, x_t, y_cols, gx_part, gain_out,
                 acts, gains, stats, post, wo_seg, wo_add, wo_mid, wor, wo_sent, inside, ysd, yrv, yst, e4r):
    keep = (acts, gains, stats, post, wo_seg, wo_add, wo_mid, wor, wo_sent)
    first = (wq_in, wk_in, wv_in, wo_in, x_in, gy_in, gq_in, gk_in, gp_in, cos_tab, sin_tab, wq_out, wk_out, wv_out, x_t, y_cols)
    second = (gy_in, cos_tab, sin_tab, wq_out, wk_out, wv_out, x_t, y_cols, dwv, dwk, dwq, dwo, y_out, gx_part, gx_out, gain_out)
    pl.run_scoped(lambda *refs: forward_phase(first, keep, *refs), *FORWARD_SCRATCH)
    pl.run_scoped(lambda *refs: backward_phase(second, keep + (inside, ysd, yrv, yst, e4r), *refs), *BACKWARD_SCRATCH)


def layer(w_q, w_k, w_v, w_o, x_tok, gy_tok, gq, gk, gp, cos_tab, sin_tab):
    grad, tok, mat = SDS((128, 4096), F32), SDS((128, 4096), BF16), SDS((4096, 1024), BF16)
    return pl.pallas_call(
        layer_kernel,
        out_shape=[grad] * 4 + [tok] * 2 + [mat] * 4 + [SDS((512, 1024), BF16), SDS((512, 4096), F32), SDS((8, 128), F32)],
        in_specs=[IN_HBM] * 6 + [IN_VMEM] * 5,
        out_specs=[IN_HBM] * 12 + [IN_VMEM],
        scratch_shapes=[
            pltpu.VMEM((6, 512, 1024), BF16),
            pltpu.VMEM((8, 1024), F32),
            pltpu.VMEM((8, 512), F32),
            pltpu.VMEM((1, 1024), F32),
            pltpu.VMEM((2, 4, SEG, SEG), F32),
            pltpu.VMEM((2, 4, SEG, SEG), F32),
            pltpu.VMEM((2, 4, SEG, SEG), F32),
            DMA((4,)), DMA(()), pltpu.SemaphoreType.REGULAR, DMA(()), DMA(()), DMA(()), DMA(()),
        ],
        compiler_params=params(5, 63.9), cost_estimate=COST, name='layer',
    )(w_q, w_k, w_v, w_o, x_tok, gy_tok, gq, gk, gp, cos_tab, sin_tab)


def copy_kernel(*refs):
    n = (len(refs) - 7) // 5
    gain_src, gain_dst, gain_buf, gain_sems = refs[n], refs[2 * n + 1:2 * n + 4], refs[3 * n + 4], refs[5 * n + 5:]
    srcs, dsts, bufs = refs[:n], refs[n + 1:2 * n + 1], refs[2 * n + 4:3 * n + 4]
    loads, stores = refs[3 * n + 5:4 * n + 5], refs[4 * n + 5:5 * n + 5]
    parts = 4

    def rows(i, p):
        step = srcs[i].shape[0] // parts
        return pl.ds(p * step, step)

    def load(i, p):
        return pltpu.make_async_copy(srcs[i].at[rows(i, p)], bufs[i].at[rows(i, p)], loads[i].at[p])

    def store(i, p):
        return pltpu.make_async_copy(bufs[i].at[rows(i, p)], dsts[i].at[rows(i, p)], stores[i].at[p])

    gain_load = pltpu.make_async_copy(gain_src, gain_buf, gain_sems[0])
    gain_stores = [pltpu.make_async_copy(gain_buf.at[pl.ds(i, 1)], gain_dst[i], gain_sems[1].at[i]) for i in range(3)]
    order = [(i, p) for i in range(n) for p in range(parts)]
    gain_load.start()
    for i, p in order:
        load(i, p).start()
    gain_load.wait()
    for copy in gain_stores:
        copy.start()
    for i, p in order:
        load(i, p).wait()
        store(i, p).start()
    for i, p in order:
        store(i, p).wait()
    for copy in gain_stores:
        copy.wait()


def copy_out(gains, *arrays):
    n = len(arrays)
    return pl.pallas_call(
        copy_kernel,
        out_shape=[SDS(a.shape, a.dtype) for a in arrays] + [SDS((1, 128), F32)] * 3,
        in_specs=[IN_HBM] * (n + 1),
        out_specs=[IN_HBM] * (n + 3),
        scratch_shapes=[pltpu.VMEM(a.shape, a.dtype) for a in arrays] + [pltpu.VMEM((8, 128), F32)] + [DMA((4,))] * (2 * n) + [DMA(()), DMA((3,))],
        compiler_params=pltpu.CompilerParams(vmem_limit_bytes=63 * 1024 * 1024), cost_estimate=COST, name='copy_out',
    )(*arrays, gains)


def solution(mesh):
    mesh4 = Mesh(mesh.devices.reshape(4, 4, 4, 2), ('sp', 'z', 'y', 'c'))
    tok_spec = P(FS, 'sp', None)
    row_spec = P(FS, None)
    vec_spec = P(FS)

    def local_step(x, grad_y, wq_rows, wk_rows, wv_rows, wo_rows, gq_rows, gk_rows, gpost_rows):
        x_tok, gy_tok = x[0], grad_y[0]
        cos_tab, sin_tab = rope_tables(4 * x_tok.shape[0])
        dwv, dwk, dwq, dwo, y, grad_x, *_, gn = layer(
            wq_rows, wk_rows, wv_rows, wo_rows, x_tok, gy_tok, gq_rows[None], gk_rows[None], gpost_rows[None], cos_tab, sin_tab)
        dwv, dwk, dwq, dwo, y, grad_x, *gn = copy_out(gn, dwv, dwk, dwq, dwo, y, grad_x)
        return y[None], grad_x[None], dwq, dwk, dwv, dwo, gn[0][0], gn[1][0], gn[2][0]

    return jax.shard_map(local_step, mesh=mesh4,
                         in_specs=(tok_spec, tok_spec, row_spec, row_spec, row_spec, row_spec, vec_spec, vec_spec, vec_spec),
                         out_specs=(tok_spec, tok_spec, row_spec, row_spec, row_spec, row_spec, vec_spec, vec_spec, vec_spec),
                         check_vma=False)
```
